32 devices in a mesh: ty: 4 (over x, core), tx: 8 (over z, y).
Axes of the slice: x: 2, y: 2, z: 4, core: 2. Of those that a mesh axis runs over, the one named last changes fastest.
Arguments:
- velocity: float32 [2, 3, 512, 1024], P(None, None, 'ty', 'tx'), may hold values from -6 to 6
- start_position: float32 [2, 16384], P(None, ('ty', 'tx')), may hold values from 0 to 128, as said below
- cells: int32 [2, 4, 2, 16384], P(None, None, None, ('ty', 'tx')), may hold values from -1 to 127, as said below
- history: float32 [2, 71, 16384], P(None, None, ('ty', 'tx')), may hold values from -6 to 6
- leavers: int32 [1, 8], replicated, may hold values from 1 to 16, as said below
- owner: int32 [16384, 1], P(('ty', 'tx')), may hold values from 0 to 31; in each aligned block of 512 rows (0 to 511, 512 to 1023, ...) at most 64 rows name the same one
- filter_matrix: float32 [73, 73], replicated, may hold values from -0.75 to 0.75
Outputs:
- filtered: float32 [2, 73, 65536], P(None, None, ('ty', 'tx'))
The draws below stay inside these ranges and needn't reach their ends.
Inputs may be any that keep to these rules, and one draw needn't show every extreme that they name: `start_position`: coordinates in cell units of the particle's tile. First coordinate cells lie in -1 .. 127 and second in -1 .. 127. Each move has one direction with exactly 16 leavers. Among the 512 slots of one tile no owner appears more than 64 times.
All inputs are finite; a program needn't handle non-finite values.
Results may differ from the reference program's by a relative error of at most 0.0003.
Values sent between devices are 32-bit elements; how exact they have to be, the bound alone decides.
No kernel may reach another device: no remote copies, remote signals or barrier semaphores. Data moves between devices by JAX's collectives and lax.ppermute only.
A program may use at most 64 MiB of HBM per device.

```python
import math
import jax
import jax.numpy as jnp
import numpy as np
from jax import lax

CY = 128
CX = 128
P_SIZE = 512
STEPS = 2
SAMPLES = 73
HISTORY = 71
MOST = 16
TILES = 32
SEND = 64
NY = 512
NX = 1024
N_TY = 4
N_TX = 8


moves = ((-1, -1), (-1, 0), (-1, 1), (0, -1), (0, 1), (1, -1), (1, 0), (1, 1))


def plan_draw(key):
    base_key = jax.random.fold_in(key, 9117)
    key_count, key_pick, key_rows, key_cols, key_walk = jax.random.split(base_key, 5)
    counts = jax.random.randint(key_count, (STEPS - 1, 8), 1, MOST + 1)
    pick = jax.random.randint(key_pick, (STEPS - 1, 1), 0, 8)
    counts = jnp.where(jnp.arange(8)[None, :] == pick, MOST, counts).astype(jnp.int32)
    slot = jnp.arange(P_SIZE, dtype=jnp.int32)
    lanes = []
    for step in range(STEPS - 1):
        offsets = jnp.cumsum(counts[step]) - counts[step]
        relative = slot - step * 8 * MOST
        lanes.append([(relative >= offsets[j]) & (relative < offsets[j] + counts[step, j]) for j in range(8)])
    base_y = jax.random.randint(key_rows, (TILES, P_SIZE), 0, CY)
    base_x = jax.random.randint(key_cols, (TILES, P_SIZE), 0, CX)
    for step in range(STEPS - 1):
        for j in range(8):
            dy, dx = moves[j]
            if dy == 1:
                base_y = jnp.where(lanes[step][j], CY - 1, base_y)
            if dy == -1:
                base_y = jnp.where(lanes[step][j], 0, base_y)
            if dx == 1:
                base_x = jnp.where(lanes[step][j], CX - 1, base_x)
            if dx == -1:
                base_x = jnp.where(lanes[step][j], 0, base_x)
    current_y = base_y
    current_x = base_x
    cell_list = []
    for step in range(STEPS):
        section_list = []
        for section in range(4):
            rolls = jax.random.randint(jax.random.fold_in(key_walk, step * 4 + section), (2, TILES, P_SIZE), 0, 5)
            delta = (rolls == 4).astype(jnp.int32) - (rolls == 0).astype(jnp.int32)
            cell_y = jnp.clip(current_y + delta[0], -1, CY - 1)
            cell_x = jnp.clip(current_x + delta[1], -1, CX - 1)
            section_list.append(jnp.stack([cell_y.reshape(-1), cell_x.reshape(-1)]))
        cell_list.append(jnp.stack(section_list))
        if step < STEPS - 1:
            grid_y = current_y.reshape(N_TY, N_TX, P_SIZE)
            grid_x = current_x.reshape(N_TY, N_TX, P_SIZE)
            new_y = grid_y
            new_x = grid_x
            for j in range(8):
                dy, dx = moves[j]
                rolled_y = jnp.clip(jnp.roll(grid_y, (dy, dx), axis=(0, 1)) - dy * CY, -1, CY - 1)
                rolled_x = jnp.clip(jnp.roll(grid_x, (dy, dx), axis=(0, 1)) - dx * CX, -1, CX - 1)
                new_y = jnp.where(lanes[step][j], rolled_y, new_y)
                new_x = jnp.where(lanes[step][j], rolled_x, new_x)
            current_y = new_y.reshape(TILES, P_SIZE)
            current_x = new_x.reshape(TILES, P_SIZE)
    cell_array = jnp.stack(cell_list).astype(jnp.int32)
    return (counts, base_y, base_x, cell_array)


def draw_leavers(key, part):
    counts, base_y, base_x, cell_array = plan_draw(key)
    return counts


def draw_cells(key, part):
    counts, base_y, base_x, cell_array = plan_draw(key)
    return cell_array


def draw_start_position(key, part):
    counts, base_y, base_x, cell_array = plan_draw(key)
    uniform = jax.random.uniform(jax.random.fold_in(key, 4242), (2, TILES, P_SIZE), jnp.float32)
    fraction = 0.999 * uniform
    rows = base_y.astype(jnp.float32) + fraction[0]
    cols = base_x.astype(jnp.float32) + fraction[1]
    return jnp.stack([rows.reshape(-1), cols.reshape(-1)]).astype(jnp.float32)


def steps_of(stream_key, shape, shards, low, largest):
    def one(position, shards_of):
        steps = jax.random.uniform(jax.random.fold_in(jax.random.fold_in(stream_key, 6), position), (shards_of,), jnp.float32, low / len(shards), largest / len(shards))
        return jnp.repeat(jnp.exp(steps), shape[position] // shards_of).reshape((-1,) + (1,) * (len(shape) - position - 1))

    loudness = one(*shards[0])
    for cut in shards[1:]:
        loudness = loudness * one(*cut)
    return loudness


def shared_out(stream_key, own, number, rows, count, top, bound, skew):
    ranking = jax.random.permutation(stream_key, count)
    crowded, ordinary = portions_of(count, rows * top, bound, skew, True), portions_of(count, rows * top, bound, skew, False)
    places = jnp.arange(count)

    def named(sizes, offset_by):
        used = int((sizes > 0).sum())
        fixed = max(1, used // 4)
        moved = fixed + (places - fixed + offset_by * (used - fixed)) % max(1, count - fixed)
        return jnp.zeros((count,), jnp.int32).at[ranking[jnp.where(places < fixed, places, moved)]].set(jnp.asarray(sizes, jnp.int32))

    sizes = jnp.where(number % 4 == 0, named(crowded, number // 4), named(ordinary, number - number // 4 - 1))
    mixed = jax.random.permutation(jax.random.fold_in(own, 3), count)
    giver, taker = mixed[0:count // 2 * 2:2], mixed[1:count // 2 * 2:2]
    margin = jnp.minimum(sizes[giver] - 1, bound - sizes[taker]) // 2
    margin = jnp.where((giver == ranking[0]) | (taker == ranking[0]) | (sizes[taker] == 0), 0, jnp.maximum(margin, 0))
    moved = jax.random.randint(jax.random.fold_in(own, 4), (count // 2,), 0, 1 << 20) % (margin + 1)
    sizes = sizes.at[giver].add(-moved).at[taker].add(moved)
    members = jnp.searchsorted(jnp.cumsum(sizes), jnp.arange(rows * top), side="right").astype(jnp.int32)
    listing = members.reshape(top, rows).T
    listing = listing[jax.random.permutation(jax.random.fold_in(own, 1), rows)]
    offset_by = jax.random.randint(jax.random.fold_in(own, 2), (rows, 1), 0, top)
    return jnp.take_along_axis(listing, (jnp.arange(top)[None, :] + offset_by) % top, axis=1)


def portions_of(number_of, total, limit, slope, full):
    loads = [(1 << 20) // math.isqrt(rank ** slope) + 1 for rank in range(1, number_of + 1)]
    largest = limit if full else min(limit, max(-(-total // number_of), total * loads[0] // sum(loads)))
    least = 1 if total - largest >= number_of - 1 else 0
    given, surplus = [largest] + [least] * (number_of - 1), total - largest - least * (number_of - 1)
    while surplus > 0:
        free = [i for i in range(1, number_of) if given[i] < largest] or [i for i in range(1, number_of) if given[i] < limit]
        mass, remaining = sum([loads[i] for i in free]), surplus
        for i in free:
            addition = min(limit - given[i], max(1, remaining * loads[i] // mass), surplus)
            given[i] = given[i] + addition
            surplus = surplus - addition
    return np.array(given)


def noise(rng, extent, spread, bound, cuts=(), kind=jnp.bfloat16):
    values = jax.random.normal(rng, extent, jnp.float32) * spread
    if len(cuts) > 0:
        values = steps_of(rng, extent, cuts, -0.22, 0.18) * values
    return jnp.clip(values, min=-bound, max=bound).astype(kind)


def setup_inputs(seed: int = 0) -> dict:
    seeds = jax.random.split(jax.random.key(seed), 8)
    velocity = noise(seeds[0], (2, STEPS + 1, NY, NX), 1.0, 6.0, ((2, 4), (3, 8)), jnp.float32)
    start_position = draw_start_position(jax.random.fold_in(seeds[7], 71), 0)
    cells = draw_cells(jax.random.fold_in(seeds[7], 71), 0)
    history = noise(seeds[3], (2, HISTORY, TILES * P_SIZE), 1.0, 6.0, ((2, 32),), jnp.float32)
    leavers = draw_leavers(jax.random.fold_in(seeds[7], 71), 0)
    owner_keys = jax.random.split(jax.random.fold_in(seeds[5], 1), (TILES * P_SIZE) // P_SIZE)
    owner_turns = jax.random.permutation(jax.random.fold_in(seeds[5], 3), (TILES * P_SIZE) // P_SIZE)
    owner = jax.vmap(lambda own, number: shared_out(jax.random.fold_in(seeds[5], 2), own, number, P_SIZE, TILES, 1, SEND, 2))(owner_keys, owner_turns).reshape((TILES * P_SIZE, 1))
    filter_matrix = noise(seeds[6], (SAMPLES, SAMPLES), SAMPLES ** -0.5, 0.75, (), jnp.float32)
    return dict(velocity=velocity, start_position=start_position, cells=cells, history=history, leavers=leavers, owner=owner, filter_matrix=filter_matrix)


drift = 0.2
moves = ((-1, -1), (-1, 0), (-1, 1), (0, -1), (0, 1), (1, -1), (1, 0), (1, 1))


def bilinear(plane, point, cell, tile_y, tile_x):
    row = (tile_y * CY + cell[0]) % NY
    col = (tile_x * CX + cell[1]) % NX
    row_next = (row + 1) % NY
    col_next = (col + 1) % NX
    wy = point[0] - cell[0].astype(jnp.float32)
    wx = point[1] - cell[1].astype(jnp.float32)
    first = jnp.take(plane, row * NX + col, axis=1)
    second = jnp.take(plane, row * NX + col_next, axis=1)
    third = jnp.take(plane, row_next * NX + col, axis=1)
    fourth = jnp.take(plane, row_next * NX + col_next, axis=1)
    return (1.0 - wy) * ((1.0 - wx) * first + wx * second) + wy * ((1.0 - wx) * third + wx * fourth)


def rank_rows(owned):
    labels = jnp.arange(N_TY * N_TX, dtype=jnp.int32)[:, None]
    onehot = (owned[None, :] == labels).astype(jnp.int32)
    running = jnp.cumsum(onehot, axis=1)
    return jnp.sum(running * onehot, axis=0) - 1


def reference(velocity, start_position, cells, history, leavers, owner, filter_matrix):
    tiles = N_TY * N_TX
    tile = jnp.arange(tiles, dtype=jnp.int32)[:, None]
    tile_y = tile // N_TX
    tile_x = tile % N_TX
    planes = [velocity[:, a].reshape(2, NY * NX) for a in range(STEPS + 1)]
    point = start_position.reshape(2, tiles, P_SIZE)
    series = jnp.concatenate([history.reshape(2, HISTORY, tiles, P_SIZE), jnp.zeros((2, STEPS, tiles, P_SIZE), jnp.float32)], axis=1)
    slot = jnp.arange(P_SIZE, dtype=jnp.int32)
    for step in range(STEPS):
        section_cells = cells[step].reshape(4, 2, tiles, P_SIZE)
        k_one = bilinear(planes[step], point, section_cells[0], tile_y, tile_x)
        spot = point + (0.5 * drift) * k_one
        k_two = 0.5 * (bilinear(planes[step], spot, section_cells[1], tile_y, tile_x) + bilinear(planes[step + 1], spot, section_cells[1], tile_y, tile_x))
        spot = point + (0.5 * drift) * k_two
        k_three = 0.5 * (bilinear(planes[step], spot, section_cells[2], tile_y, tile_x) + bilinear(planes[step + 1], spot, section_cells[2], tile_y, tile_x))
        spot = point + drift * k_three
        k_four = bilinear(planes[step + 1], spot, section_cells[3], tile_y, tile_x)
        series = series.at[:, HISTORY + step].set(k_one)
        point = point + (drift / 6.0) * (k_one + 2.0 * k_two + 2.0 * k_three + k_four)
        if step < STEPS - 1:
            counts = leavers[step]
            offsets = jnp.cumsum(counts) - counts
            band = step * 8 * MOST
            grid_point = point.reshape(2, N_TY, N_TX, P_SIZE)
            grid_series = series.reshape(2, SAMPLES, N_TY, N_TX, P_SIZE)
            new_point = grid_point
            new_series = grid_series
            for j in range(8):
                dy, dx = moves[j]
                lane = (slot >= band + offsets[j]) & (slot < band + offsets[j] + counts[j])
                rolled = jnp.roll(grid_point, (dy, dx), axis=(1, 2))
                shift_vec = jnp.array([dy * CY, dx * CX], jnp.float32).reshape(2, 1, 1, 1)
                new_point = jnp.where(lane, rolled - shift_vec, new_point)
                new_series = jnp.where(lane, jnp.roll(grid_series, (dy, dx), axis=(2, 3)), new_series)
            point = new_point.reshape(2, tiles, P_SIZE)
            series = new_series.reshape(2, SAMPLES, tiles, P_SIZE)
    low = jnp.einsum("tj,cjn->ctn", filter_matrix, series.reshape(2, SAMPLES, tiles * P_SIZE), precision=lax.Precision.HIGHEST)
    owned = owner.reshape(tiles, P_SIZE)
    ranks = lax.map(rank_rows, owned)
    dest = owned * (4 * P_SIZE) + tile * SEND + ranks
    result = jnp.zeros((2, SAMPLES, tiles * 4 * P_SIZE), jnp.float32)
    return result.at[:, :, dest.reshape(-1)].set(low)
```

```python
import functools

import jax
import jax.numpy as jnp
from jax import lax
from jax.experimental import pallas as pl
from jax.experimental.pallas import tpu as pltpu
from jax.sharding import PartitionSpec as P

STEPS = 2
SAMPLES = 73
HISTORY = 71
MOST = 16


drift = 0.2
moves = ((-1, -1), (-1, 0), (-1, 1), (0, -1), (0, 1), (1, -1), (1, 0), (1, 1))
f32 = jnp.float32
bf16 = jnp.bfloat16
LANES = 128


def up(value, to):
    return -(-value // to) * to


def shifted(value, axis, by):
    peers = lax.axis_size(axis)
    return lax.ppermute(value, axis, [(i, (i + by) % peers) for i in range(peers)])


def halves(value):
    high = value.astype(bf16)
    return high, (value - high.astype(f32)).astype(bf16)


def picked(condition):
    return jnp.where(condition, 1.0, 0.0).astype(f32)


def iota(shape, dim):
    return lax.broadcasted_iota(jnp.int32, shape, dim)


def whole(count):
    return [pl.BlockSpec(memory_space=pltpu.VMEM) for _ in range(count)]


def build_table(table_ref, number, snapshots, weight, velocity_ref, north_ref, south_ref, west_ref, east_ref, columns):
    rows, cols = velocity_ref.shape[2], velocity_ref.shape[3]
    count = velocity_ref.shape[1]
    block = up(rows + 2, 16)
    lane = iota((16, cols), 1)
    sub = iota((16, cols), 0)
    for c in range(2):
        inner = None
        for a in snapshots:
            k = c * count + a
            body = velocity_ref[c, a]
            side = pltpu.roll(columns, (cols - k) % cols, 1)
            top, low = north_ref[c, a : a + 1], south_ref[c, a : a + 1]
            edge = jnp.where(sub == 0, top, jnp.where(sub == 1, low, 0.0))
            north_west, north_east = west_ref[1, c, a : a + 1, cols - 1 :], east_ref[1, c, a : a + 1, 0:1]
            south_west, south_east = west_ref[2, c, a : a + 1, cols - 1 :], east_ref[2, c, a : a + 1, 0:1]
            west = jnp.where(sub == 0, north_west, jnp.where(sub == 1, south_west, 0.0))
            east = jnp.where(sub == 0, north_east, jnp.where(sub == 1, south_east, 0.0))
            corner = jnp.where(lane == 0, west, jnp.where(lane == 8, east, 0.0))
            parts = (body, side, edge, corner)
            inner = parts if inner is None else tuple(p + q for p, q in zip(inner, parts))
        body, side, edge, corner = (weight * p if weight != 1.0 else p for p in inner)
        for split, (b, s, e, n) in enumerate(zip(halves(body), halves(side), halves(edge), halves(corner))):
            at = (split * 2 + c) * block
            table_ref[number, at : at + rows, 0:cols] = b
            table_ref[number, at : at + rows, cols : 2 * cols] = s
            table_ref[number, at + rows : at + block, 0:cols] = e
            table_ref[number, at + rows : at + block, cols : 2 * cols] = n


def read_corners(table_ref, number, cell, rows, cols):
    block = up(rows + 2, 16)
    slots = cell.shape[1]
    cy, cx = cell[0:1], cell[1:2]
    at = iota((2 * cols, slots), 0)
    left = picked(at == jnp.where(cx < 0, cols, cx)).astype(bf16)
    right = picked(at == jnp.where(cx + 1 >= cols, cols + 8, cx + 1)).astype(bf16)
    row = iota((block, slots), 0)
    upper = row == jnp.where(cy < 0, rows, cy)
    lower = row == jnp.where(cy + 1 >= rows, rows + 1, cy + 1)
    table = table_ref[number]
    values = {}
    for side, onehot in enumerate((left, right)):
        product = jnp.dot(table, onehot, preferred_element_type=f32)
        for c in range(2):
            column = product[c * block : (c + 1) * block] + product[(2 + c) * block : (3 + c) * block]
            values[0, side, c] = jnp.sum(jnp.where(upper, column, 0.0), axis=0, keepdims=True)
            values[1, side, c] = jnp.sum(jnp.where(lower, column, 0.0), axis=0, keepdims=True)
    return [[values[v, h, c] for c in range(2)] for v in range(2) for h in range(2)]


def bilinear(corners, point, cell):
    wy = point[0] - cell[0:1].astype(f32)
    wx = point[1] - cell[1:2].astype(f32)
    first, second, third, fourth = corners
    return [
        (1.0 - wy) * ((1.0 - wx) * first[c] + wx * second[c]) + wy * ((1.0 - wx) * third[c] + wx * fourth[c])
        for c in range(2)
    ]


def along(point, factor, speed):
    return [p + factor * s for p, s in zip(point, speed)]


def halo_columns(west_ref, east_ref, cols):
    count = west_ref.shape[1] * west_ref.shape[2]
    zeros = jnp.zeros((8 - count, cols), f32)
    west = [west_ref[0, c, a : a + 1] for c in range(west_ref.shape[1]) for a in range(west_ref.shape[2])]
    east = [east_ref[0, c, a : a + 1] for c in range(east_ref.shape[1]) for a in range(east_ref.shape[2])]
    flat = jnp.concatenate(west + [zeros] + east + [zeros, jnp.zeros((cols - 16, cols), f32)], axis=0)
    return flat.T


def step_kernel(step, following, velocity_ref, north_ref, south_ref, west_ref, east_ref, point_ref, first_ref, cells_ref, *rest):
    if following:
        record_ref, next_ref, table_ref = rest
    else:
        record_ref, table_ref = rest
    rows, cols = velocity_ref.shape[2], velocity_ref.shape[3]
    columns = halo_columns(west_ref, east_ref, cols)
    fields = (velocity_ref, north_ref, south_ref, west_ref, east_ref, columns)
    build_table(table_ref, 0, (step,), 1.0, *fields)
    build_table(table_ref, 1, (step, step + 1), 0.5, *fields)
    build_table(table_ref, 2, (step + 1,), 1.0, *fields)
    sections = [cells_ref[step, s] for s in range(4)]
    if step == 0:
        first = read_corners(table_ref, 0, sections[0], rows, cols)
    else:
        first = [[first_ref[2 * i + c : 2 * i + c + 1] for c in range(2)] for i in range(4)]
    second = read_corners(table_ref, 1, sections[1], rows, cols)
    third = read_corners(table_ref, 1, sections[2], rows, cols)
    fourth = read_corners(table_ref, 2, sections[3], rows, cols)
    point = [point_ref[0:1], point_ref[1:2]]
    k_one = bilinear(first, point, sections[0])
    k_two = bilinear(second, along(point, 0.5 * drift, k_one), sections[1])
    k_three = bilinear(third, along(point, 0.5 * drift, k_two), sections[2])
    k_four = bilinear(fourth, along(point, drift, k_three), sections[3])
    point = [
        p + drift / 6.0 * (a + 2.0 * b + 2.0 * c + d)
        for p, a, b, c, d in zip(point, k_one, k_two, k_three, k_four)
    ]
    blank = [jnp.zeros_like(point[0])] * 4
    record_ref[...] = jnp.concatenate(point + k_one + blank, axis=0)
    if following:
        ahead = read_corners(table_ref, 2, cells_ref[step + 1, 0], rows, cols)
        next_ref[...] = jnp.concatenate([value for corner in ahead for value in corner], axis=0)


def run_step(step, halo, point, first, cells):
    velocity = halo[0]
    slots = point.shape[1]
    following = step + 1 < STEPS
    rows, cols = velocity.shape[2], velocity.shape[3]
    shape = jax.ShapeDtypeStruct((8, slots), f32)
    block = up(rows + 2, 16)
    return pl.pallas_call(
        functools.partial(step_kernel, step, following),
        out_shape=[shape] * (2 if following else 1),
        in_specs=whole(8),
        out_specs=whole(2 if following else 1),
        scratch_shapes=[pltpu.VMEM((3, 4 * block, 2 * cols), bf16)],
        cost_estimate=pl.CostEstimate(flops=10 * 4 * block * 2 * cols * slots * 2, bytes_accessed=600000, transcendentals=0),
        name="sample_step",
    )(*halo, point, first, cells)


def paired_halves(first, second, width):
    lane = iota(first.shape, 1)
    left = jnp.where(lane < width, first, pltpu.roll(second, width, 1))
    right = jnp.where(lane < width, pltpu.roll(first, width, 1), second)
    return left, right


def place_history_kernel(width, paired, history_ref, arrived_ref, owner_ref, owner_row_ref, out_ref, target_ref):
    slots = owner_ref.shape[0]
    total = out_ref.shape[0] * width if paired else out_ref.shape[2]
    rows = up(HISTORY, 8)
    before = iota((slots, slots), 1) < iota((slots, slots), 0)
    same = owner_ref[...] == owner_row_ref[...]
    rank = jnp.sum(picked(same & before), axis=1, keepdims=True).astype(jnp.int32)
    target = owner_ref[...] * width + rank
    target_ref[...] = jnp.broadcast_to(target, target_ref.shape)
    moved = arrived_ref.shape[2]
    blank = jnp.zeros((rows - HISTORY, slots), f32)
    parts = []
    for c in range(2):
        parts.append(jnp.concatenate([arrived_ref[c], history_ref[c, :, moved:]], axis=1))
        parts.append(blank)
    high, low = halves(jnp.concatenate(parts, axis=0))
    both = jnp.concatenate([high, low], axis=0)
    chunk = 256
    for start in range(0, total, chunk):
        onehot = picked(target == start + iota((slots, chunk), 1)).astype(bf16)
        product = jnp.dot(both, onehot, preferred_element_type=f32)
        placed = product[: 2 * rows] + product[2 * rows :]
        if paired:
            for at in range(0, chunk, LANES):
                left, right = paired_halves(placed[:rows, at : at + LANES], placed[rows:, at : at + LANES], width)
                number = (start + at) // width
                out_ref[number, 0:rows] = left
                out_ref[number + 1, 0:rows] = right
        else:
            out_ref[0, 0:rows, start : start + chunk] = placed[:rows]
            out_ref[1, 0:rows, start : start + chunk] = placed[rows:]


def place_samples_kernel(width, paired, record_ref, moved_ref, next_ref, cells_ref, target_ref, _, out_ref):
    slots = record_ref.shape[1]
    moved = moved_ref.shape[1]
    total = out_ref.shape[0] * width if paired else out_ref.shape[2]
    record = jnp.concatenate([moved_ref[...], record_ref[:, moved:]], axis=1)
    corners = [[next_ref[2 * i + c : 2 * i + c + 1] for c in range(2)] for i in range(4)]
    last = bilinear(corners, [record[0:1], record[1:2]], cells_ref[STEPS - 1, 0])
    blank = jnp.zeros((6, slots), f32)
    columns = [record[2:3], last[0], blank, record[3:4], last[1], blank]
    high, low = halves(jnp.concatenate(columns, axis=0))
    both = jnp.concatenate([high, low], axis=0)
    target = target_ref[:, 0:1]
    chunk = 256
    for start in range(0, total, chunk):
        onehot = picked(target == start + iota((slots, chunk), 1)).astype(bf16)
        product = jnp.dot(both, onehot, preferred_element_type=f32)
        placed = product[:16] + product[16:]
        if paired:
            for at in range(0, chunk, LANES):
                left, right = paired_halves(placed[:8, at : at + LANES], placed[8:, at : at + LANES], width)
                number = (start + at) // width
                out_ref[number] = left
                out_ref[number + 1] = right
        else:
            out_ref[0, :, start : start + chunk] = placed[:8]
            out_ref[1, :, start : start + chunk] = placed[8:]


def filter_kernel(width, paired, matrix_ref, arrived_ref, out_ref):
    outs, depth = matrix_ref.shape
    high, low = halves(matrix_ref[...])
    left = jnp.concatenate([high, low, high], axis=1)
    total = out_ref.shape[2]
    chunk = 512
    for start in range(0, total, chunk):
        if paired:
            tiles = [
                paired_halves(arrived_ref[at // width], arrived_ref[at // width + 1], width)
                for at in range(start, start + chunk, LANES)
            ]
            columns = [jnp.concatenate([t[c] for t in tiles], axis=1) for c in range(2)]
        else:
            columns = [arrived_ref[c, :, start : start + chunk] for c in range(2)]
        for c in range(2):
            x_high, x_low = halves(columns[c])
            right = jnp.concatenate([x_high, x_high, x_low], axis=0)
            product = jnp.dot(left, right, preferred_element_type=f32)
            out_ref[c, :, start : start + chunk] = product[: out_ref.shape[1]]


def cost(flops, moved):
    return pl.CostEstimate(flops=flops, bytes_accessed=moved, transcendentals=0)


def sides_of(counts, axis):
    slot = iota((1, 8 * MOST), 1)
    offsets = jnp.cumsum(counts) - counts
    result = jnp.zeros((1, 8 * MOST), jnp.int32)
    for j in range(8):
        inside = (slot >= offsets[j]) & (slot < offsets[j] + counts[j])
        result = result + jnp.where(inside, moves[j][axis], 0)
    return result


def moved_along(value, side, axis):
    forward = shifted(value, axis, 1)
    backward = shifted(value, axis, -1)
    return jnp.where(side == 1, forward, jnp.where(side == -1, backward, value))


def per_device(velocity, start_position, cells, history, leavers, owner, filter_matrix):
    tile_rows = velocity.shape[2]
    tile_cols = velocity.shape[3]
    slots = start_position.shape[1]
    tile_count = lax.axis_size("ty") * lax.axis_size("tx")
    per_owner = 4 * slots // tile_count
    paired = 2 * per_owner == LANES
    north = shifted(velocity[:, :, tile_rows - 1], "ty", 1)
    south = shifted(velocity[:, :, 0], "ty", -1)
    west = shifted(jnp.stack([velocity[:, :, :, tile_cols - 1], north, south]), "tx", 1)
    east = shifted(jnp.stack([velocity[:, :, :, 0], north, south]), "tx", -1)
    halo = (velocity, north, south, west, east)
    point = start_position
    first = jnp.zeros((8, slots), f32)
    moved_history = history
    record = None
    for step in range(STEPS):
        if step == STEPS - 1:
            waiting = first
        results = run_step(step, halo, point, first, cells)
        if step == STEPS - 1:
            break
        record, first = results
        counts = leavers[step]
        band = step * 8 * MOST
        side_y, side_x = sides_of(counts, 0), sides_of(counts, 1)
        part = record[:, band : band + 8 * MOST]
        part = moved_along(moved_along(part, side_y, "ty"), side_x, "tx")
        lowered = jnp.concatenate([side_y * tile_rows, side_x * tile_cols, jnp.zeros((6, 8 * MOST), jnp.int32)], axis=0)
        part = part - lowered.astype(f32)
        past = history[:, :, band : band + 8 * MOST]
        past = moved_along(moved_along(past, side_y, "ty"), side_x, "tx")
        point = jnp.concatenate([part[0:2], record[0:2, 8 * MOST :]], axis=1)
    depth = up(HISTORY, 8) + 8
    shape = (tile_count, depth, LANES) if paired else (2, depth, tile_count * per_owner)
    placed, target = pl.pallas_call(
        functools.partial(place_history_kernel, per_owner, paired),
        out_shape=[jax.ShapeDtypeStruct(shape, f32), jax.ShapeDtypeStruct((slots, LANES), jnp.int32)],
        in_specs=whole(4),
        out_specs=whole(2),
        cost_estimate=cost(2 * 4 * 80 * slots * 4 * slots, 3000000),
        name="place_history",
    )(history, past, owner, owner.reshape(1, slots))
    blocks = (tile_count, 8, LANES) if paired else (2, 8, tile_count * per_owner)
    placed = pl.pallas_call(
        functools.partial(place_samples_kernel, per_owner, paired),
        out_shape=jax.ShapeDtypeStruct(shape, f32),
        grid=(1,),
        in_specs=[pl.BlockSpec(s, lambda i, n=len(s): (0,) * n) for s in (record.shape, part.shape, waiting.shape, cells.shape, target.shape)]
        + [pl.BlockSpec(memory_space=pl.ANY)],
        out_specs=pl.BlockSpec(blocks, lambda i: (0, depth // 8 - 1, 0)),
        input_output_aliases={5: 0},
        cost_estimate=cost(2 * 2 * 16 * slots * 4 * slots, 1000000),
        name="place_samples",
    )(record, part, waiting, cells, target, placed)
    if not paired:
        placed = placed.reshape(2, depth, tile_count, per_owner).transpose(2, 1, 0, 3)
    arrived = lax.all_to_all(placed, ("ty", "tx"), split_axis=0, concat_axis=0, tiled=True)
    if not paired:
        arrived = arrived.transpose(2, 1, 0, 3).reshape(shape)
    matrix = jnp.zeros((up(SAMPLES, 16), depth), f32)
    matrix = matrix.at[:SAMPLES, :HISTORY].set(filter_matrix[:, :HISTORY])
    matrix = matrix.at[:SAMPLES, depth - 8 : depth - 8 + STEPS].set(filter_matrix[:, HISTORY:])
    return pl.pallas_call(
        functools.partial(filter_kernel, per_owner, paired),
        out_shape=jax.ShapeDtypeStruct((2, SAMPLES, tile_count * per_owner), f32),
        in_specs=whole(2),
        out_specs=whole(1)[0],
        cost_estimate=cost(2 * 3 * 80 * 80 * 8 * slots, 3000000),
        name="filter_series",
    )(matrix, arrived)


def solution(mesh):
    placed = (
        P(None, None, "ty", "tx"),
        P(None, ("ty", "tx")),
        P(None, None, None, ("ty", "tx")),
        P(None, None, ("ty", "tx")),
        P(),
        P(("ty", "tx"), None),
        P(),
    )
    return jax.shard_map(
        per_device,
        mesh=mesh,
        in_specs=placed,
        out_specs=P(None, None, ("ty", "tx")),
        check_vma=False,
    )
```

```python
import functools

import jax
import jax.numpy as jnp
from jax import lax
from jax.experimental import pallas as pl
from jax.experimental.pallas import tpu as pltpu
from jax.sharding import PartitionSpec as P

STEPS = 2
SAMPLES = 73
HISTORY = 71
MOST = 16


drift = 0.2
moves = ((-1, -1), (-1, 0), (-1, 1), (0, -1), (0, 1), (1, -1), (1, 0), (1, 1))
f32 = jnp.float32
bf16 = jnp.bfloat16
LANES = 128


def up(value, to):
    return -(-value // to) * to


def shifted(value, axis, by):
    peers = lax.axis_size(axis)
    return lax.ppermute(value, axis, [(i, (i + by) % peers) for i in range(peers)])


def halves(value):
    high = value.astype(bf16)
    return high, (value - high.astype(f32)).astype(bf16)


def picked(condition):
    return jnp.where(condition, 1.0, 0.0).astype(f32)


def iota(shape, dim):
    return lax.broadcasted_iota(jnp.int32, shape, dim)


def whole(count):
    return [pl.BlockSpec(memory_space=pltpu.VMEM) for _ in range(count)]


def cost(flops, moved):
    return pl.CostEstimate(flops=flops, bytes_accessed=moved, transcendentals=0)


grant = pltpu.CompilerParams(vmem_limit_bytes=16 * 1024 * 1024)


def build_table(table_ref, number, snapshots, weight, velocity_ref, north_ref, south_ref, west_ref, east_ref, columns):
    rows, cols = velocity_ref.shape[2], velocity_ref.shape[3]
    count = velocity_ref.shape[1]
    block = up(rows + 2, 16)
    lane = iota((16, cols), 1)
    sub = iota((16, cols), 0)
    for c in range(2):
        inner = None
        for a in snapshots:
            k = c * count + a
            body = velocity_ref[c, a]
            side = pltpu.roll(columns, (cols - k) % cols, 1)
            top, low = north_ref[c, a : a + 1], south_ref[c, a : a + 1]
            edge = jnp.where(sub == 0, top, jnp.where(sub == 1, low, 0.0))
            north_west, north_east = west_ref[1, c, a : a + 1, cols - 1 :], east_ref[1, c, a : a + 1, 0:1]
            south_west, south_east = west_ref[2, c, a : a + 1, cols - 1 :], east_ref[2, c, a : a + 1, 0:1]
            west = jnp.where(sub == 0, north_west, jnp.where(sub == 1, south_west, 0.0))
            east = jnp.where(sub == 0, north_east, jnp.where(sub == 1, south_east, 0.0))
            corner = jnp.where(lane == 0, west, jnp.where(lane == 8, east, 0.0))
            parts = (body, side, edge, corner)
            inner = parts if inner is None else tuple(p + q for p, q in zip(inner, parts))
        body, side, edge, corner = (weight * p if weight != 1.0 else p for p in inner)
        for split, (b, s, e, n) in enumerate(zip(halves(body), halves(side), halves(edge), halves(corner))):
            at = (split * 2 + c) * block
            table_ref[number, at : at + rows, 0:cols] = b
            table_ref[number, at : at + rows, cols : 2 * cols] = s
            table_ref[number, at + rows : at + block, 0:cols] = e
            table_ref[number, at + rows : at + block, cols : 2 * cols] = n


def read_corners(table_ref, number, cell, rows, cols):
    block = up(rows + 2, 16)
    slots = cell.shape[1]
    cy, cx = cell[0:1], cell[1:2]
    at = iota((2 * cols, slots), 0)
    left = picked(at == jnp.where(cx < 0, cols, cx)).astype(bf16)
    right = picked(at == jnp.where(cx + 1 >= cols, cols + 8, cx + 1)).astype(bf16)
    row = iota((block, slots), 0)
    upper = row == jnp.where(cy < 0, rows, cy)
    lower = row == jnp.where(cy + 1 >= rows, rows + 1, cy + 1)
    table = table_ref[number]
    values = {}
    for side, onehot in enumerate((left, right)):
        product = jnp.dot(table, onehot, preferred_element_type=f32)
        for c in range(2):
            column = product[c * block : (c + 1) * block] + product[(2 + c) * block : (3 + c) * block]
            values[0, side, c] = jnp.sum(jnp.where(upper, column, 0.0), axis=0, keepdims=True)
            values[1, side, c] = jnp.sum(jnp.where(lower, column, 0.0), axis=0, keepdims=True)
    return [[values[v, h, c] for c in range(2)] for v in range(2) for h in range(2)]


def bilinear(corners, point, cell):
    wy = point[0] - cell[0:1].astype(f32)
    wx = point[1] - cell[1:2].astype(f32)
    first, second, third, fourth = corners
    return [
        (1.0 - wy) * ((1.0 - wx) * first[c] + wx * second[c]) + wy * ((1.0 - wx) * third[c] + wx * fourth[c])
        for c in range(2)
    ]


def along(point, factor, speed):
    return [p + factor * s for p, s in zip(point, speed)]


def halo_columns(west_ref, east_ref, cols):
    count = west_ref.shape[1] * west_ref.shape[2]
    zeros = jnp.zeros((8 - count, cols), f32)
    west = [west_ref[0, c, a : a + 1] for c in range(west_ref.shape[1]) for a in range(west_ref.shape[2])]
    east = [east_ref[0, c, a : a + 1] for c in range(east_ref.shape[1]) for a in range(east_ref.shape[2])]
    flat = jnp.concatenate(west + [zeros] + east + [zeros, jnp.zeros((cols - 16, cols), f32)], axis=0)
    return flat.T


def step_kernel(step, following, velocity_ref, north_ref, south_ref, west_ref, east_ref, point_ref, cells_ref, *rest):
    if step > 0:
        first_ref, rest = rest[0], rest[1:]
    if following:
        record_ref, lead_ref, next_ref, table_ref = rest
    else:
        record_ref, lead_ref, table_ref = rest
    rows, cols = velocity_ref.shape[2], velocity_ref.shape[3]
    columns = halo_columns(west_ref, east_ref, cols)
    fields = (velocity_ref, north_ref, south_ref, west_ref, east_ref, columns)
    build_table(table_ref, 0, (step,), 1.0, *fields)
    build_table(table_ref, 1, (step, step + 1), 0.5, *fields)
    build_table(table_ref, 2, (step + 1,), 1.0, *fields)
    sections = [cells_ref[step, s] for s in range(4)]
    if step == 0:
        first = read_corners(table_ref, 0, sections[0], rows, cols)
    else:
        first = [[first_ref[2 * i + c : 2 * i + c + 1] for c in range(2)] for i in range(4)]
    second = read_corners(table_ref, 1, sections[1], rows, cols)
    third = read_corners(table_ref, 1, sections[2], rows, cols)
    fourth = read_corners(table_ref, 2, sections[3], rows, cols)
    point = [point_ref[0:1], point_ref[1:2]]
    k_one = bilinear(first, point, sections[0])
    k_two = bilinear(second, along(point, 0.5 * drift, k_one), sections[1])
    k_three = bilinear(third, along(point, 0.5 * drift, k_two), sections[2])
    k_four = bilinear(fourth, along(point, drift, k_three), sections[3])
    point = [
        p + drift / 6.0 * (a + 2.0 * b + 2.0 * c + d)
        for p, a, b, c, d in zip(point, k_one, k_two, k_three, k_four)
    ]
    blank = [jnp.zeros_like(point[0])] * 4
    record = jnp.concatenate(point + k_one + blank, axis=0)
    record_ref[...] = record
    band = step * 8 * MOST
    lead_ref[...] = record[:, band : band + 8 * MOST]
    if following:
        ahead = read_corners(table_ref, 2, cells_ref[step + 1, 0], rows, cols)
        next_ref[...] = jnp.concatenate([value for corner in ahead for value in corner], axis=0)


def run_step(step, halo, point, first, cells):
    velocity = halo[0]
    slots = point.shape[1]
    following = step + 1 < STEPS
    cols = velocity.shape[3]
    block = up(velocity.shape[2] + 2, 16)
    operands = (*halo, point, cells) + ((first,) if step > 0 else ())
    shape = jax.ShapeDtypeStruct((8, slots), f32)
    shapes = [shape, jax.ShapeDtypeStruct((8, 8 * MOST), f32)] + ([shape] if following else [])
    return pl.pallas_call(
        functools.partial(step_kernel, step, following),
        out_shape=shapes,
        in_specs=whole(len(operands)),
        out_specs=whole(len(shapes)),
        scratch_shapes=[pltpu.VMEM((3, 4 * block, 2 * cols), bf16)],
        cost_estimate=cost(10 * 4 * block * 2 * cols * slots * 2, 600000),
        compiler_params=grant,
        name="sample_step",
    )(*operands)


def sides_kernel(leavers_ref, sides_ref):
    slot = iota((1, 8 * MOST), 1)
    for step in range(leavers_ref.shape[0]):
        rows = [jnp.zeros((1, 8 * MOST), f32) for _ in range(2)]
        start = 0
        for j in range(8):
            end = start + leavers_ref[step, j]
            inside = (slot >= start) & (slot < end)
            rows = [jnp.where(inside, float(moves[j][axis]), rows[axis]) for axis in range(2)]
            start = end
        sides_ref[step] = jnp.concatenate(rows + [jnp.zeros((6, 8 * MOST), f32)], axis=0)


def find_sides(leavers):
    return pl.pallas_call(
        sides_kernel,
        out_shape=jax.ShapeDtypeStruct((leavers.shape[0], 8, 8 * MOST), f32),
        in_specs=[pl.BlockSpec(memory_space=pltpu.SMEM)],
        out_specs=whole(1)[0],
        compiler_params=grant,
        cost_estimate=cost(100000, 5000),
        name="find_sides",
    )(leavers)


def chosen(side, value, forward, backward):
    return jnp.where(side > 0.0, forward, jnp.where(side < 0.0, backward, value))


def paired_halves(first, second, width):
    lane = iota(first.shape, 1)
    left = jnp.where(lane < width, first, pltpu.roll(second, width, 1))
    right = jnp.where(lane < width, pltpu.roll(first, width, 1), second)
    return left, right


def place_history_kernel(width, paired, history_ref, past_ref, west_ref, east_ref, sides_ref, owner_ref, out_ref, target_ref):
    slots = owner_ref.shape[1]
    total = out_ref.shape[0] * width if paired else out_ref.shape[2]
    rows = up(HISTORY, 8)
    groups = slots // LANES
    moving = 8 * MOST // LANES
    owner_row = owner_ref[...]
    owner = jnp.broadcast_to(owner_row, (LANES, slots)).T[:, 0:1]
    before = iota((slots, slots), 1) < iota((slots, slots), 0)
    rank = jnp.sum(picked((owner == owner_row) & before), axis=1, keepdims=True).astype(jnp.int32)
    target = owner * width + rank
    target_ref[...] = jnp.broadcast_to(target, target_ref.shape)
    side = sides_ref[0, 1:2]
    parts = []
    for c in range(2):
        at = pl.ds(c, HISTORY, stride=2)
        pieces = [chosen(side, past_ref[at, :], west_ref[at, :], east_ref[at, :])]
        pieces += [history_ref[pl.ds(2 * g + c, HISTORY, stride=2 * groups), :] for g in range(moving, groups)]
        parts += [jnp.concatenate(pieces, axis=1), jnp.zeros((rows - HISTORY, slots), f32)]
    high, low = halves(jnp.concatenate(parts, axis=0))
    both = jnp.concatenate([high, low], axis=0)
    chunk = 256
    for start in range(0, total, chunk):
        onehot = picked(target == start + iota((slots, chunk), 1)).astype(bf16)
        product = jnp.dot(both, onehot, preferred_element_type=f32)
        placed = product[: 2 * rows] + product[2 * rows :]
        if paired:
            for at in range(0, chunk, LANES):
                left, right = paired_halves(placed[:rows, at : at + LANES], placed[rows:, at : at + LANES], width)
                number = (start + at) // width
                out_ref[number] = left
                out_ref[number + 1] = right
        else:
            out_ref[0, :, start : start + chunk] = placed[:rows]
            out_ref[1, :, start : start + chunk] = placed[rows:]


def place_samples_kernel(
    width, paired, tile, record_ref, lead_ref, west_ref, east_ref, sides_ref, next_ref, cells_ref, target_ref, placed_ref, out_ref
):
    slots = record_ref.shape[1]
    moved = lead_ref.shape[1]
    total = out_ref.shape[0] * width if paired else out_ref.shape[2]
    rows = up(HISTORY, 8)
    sides = sides_ref[0]
    lead = chosen(sides[1:2], lead_ref[...], west_ref[...], east_ref[...])
    sub = iota(lead.shape, 0)
    lowered = jnp.where(sub == 0, sides[0:1] * tile[0], jnp.where(sub == 1, sides[1:2] * tile[1], 0.0))
    record = jnp.concatenate([lead - lowered, record_ref[:, moved:]], axis=1)
    corners = [[next_ref[2 * i + c : 2 * i + c + 1] for c in range(2)] for i in range(4)]
    last = bilinear(corners, [record[0:1], record[1:2]], cells_ref[STEPS - 1, 0])
    blank = jnp.zeros((6, slots), f32)
    columns = [last[0], blank, record[2:3], last[1], blank, record[3:4]]
    high, low = halves(jnp.concatenate(columns, axis=0))
    both = jnp.concatenate([high, low], axis=0)
    target = target_ref[:, 0:1]
    chunk = 256
    row = iota((8, LANES), 0)
    wide = iota((8, chunk), 0)
    for start in range(0, total, chunk):
        onehot = picked(target == start + iota((slots, chunk), 1)).astype(bf16)
        product = jnp.dot(both, onehot, preferred_element_type=f32)
        values = product[:16] + product[16:]
        if paired:
            for at in range(0, chunk, LANES):
                pair = paired_halves(values[:8, at : at + LANES], values[8:, at : at + LANES], width)
                for i in range(2):
                    number = (start + at) // width + i
                    out_ref[number, 0 : rows - 8] = placed_ref[number, 0 : rows - 8]
                    out_ref[number, rows - 8 : rows] = jnp.where(row == 7, pair[i], placed_ref[number, rows - 8 : rows])
                    out_ref[number, rows : rows + 8] = jnp.where(row == 0, pair[i], 0.0)
        else:
            span = slice(start, start + chunk)
            for c in range(2):
                value = values[8 * c : 8 * c + 8]
                out_ref[c, 0 : rows - 8, span] = placed_ref[c, 0 : rows - 8, span]
                out_ref[c, rows - 8 : rows, span] = jnp.where(wide == 7, value, placed_ref[c, rows - 8 : rows, span])
                out_ref[c, rows : rows + 8, span] = jnp.where(wide == 0, value, 0.0)


def filter_kernel(width, paired, matrix_ref, arrived_ref, out_ref, wide_ref):
    depth = arrived_ref.shape[1]
    samples = matrix_ref.shape[0]
    wide_ref[...] = jnp.zeros_like(wide_ref)
    wide_ref[0:samples, 0:samples] = matrix_ref[...]
    high, low = halves(wide_ref[:, 0:depth])
    left = jnp.concatenate([high, low, high], axis=1)
    groups = out_ref.shape[0] // (2 * samples)
    step = 4
    for first in range(0, groups, step):
        start = first * LANES
        if paired:
            tiles = [
                paired_halves(arrived_ref[at // width], arrived_ref[at // width + 1], width)
                for at in range(start, start + step * LANES, LANES)
            ]
            columns = [jnp.concatenate([t[c] for t in tiles], axis=1) for c in range(2)]
        else:
            columns = [arrived_ref[c, :, start : start + step * LANES] for c in range(2)]
        for c in range(2):
            x_high, x_low = halves(columns[c])
            right = jnp.concatenate([x_high, x_high, x_low], axis=0)
            product = jnp.dot(left, right, preferred_element_type=f32)
            for g in range(step):
                rows = pl.ds(2 * (first + g) + c, samples, stride=2 * groups)
                out_ref[rows, :] = product[:samples, g * LANES : (g + 1) * LANES]


def per_device(velocity, start_position, cells, history, leavers, owner, filter_matrix):
    tile_rows = velocity.shape[2]
    tile_cols = velocity.shape[3]
    slots = start_position.shape[1]
    tile_count = lax.axis_size("ty") * lax.axis_size("tx")
    per_owner = 4 * slots // tile_count
    paired = 2 * per_owner == LANES
    groups = slots // LANES
    north = shifted(velocity[:, :, tile_rows - 1], "ty", 1)
    south = shifted(velocity[:, :, 0], "ty", -1)
    west = shifted(jnp.stack([velocity[:, :, :, tile_cols - 1], north, south]), "tx", 1)
    east = shifted(jnp.stack([velocity[:, :, :, 0], north, south]), "tx", -1)
    halo = (velocity, north, south, west, east)
    sides = find_sides(leavers)
    by_rows = history.reshape(2, HISTORY, groups, LANES).transpose(1, 2, 0, 3)
    past = by_rows[:, 0].reshape(2 * HISTORY, LANES)
    past = chosen(sides[0, 0:1], past, shifted(past, "ty", 1), shifted(past, "ty", -1))
    past_west, past_east = shifted(past, "tx", 1), shifted(past, "tx", -1)
    record, lead, first = run_step(0, halo, start_position, None, cells)
    lead = chosen(sides[0, 0:1], lead, shifted(lead, "ty", 1), shifted(lead, "ty", -1))
    lead_west, lead_east = shifted(lead, "tx", 1), shifted(lead, "tx", -1)
    rows = up(HISTORY, 8)
    shape = (tile_count, rows, LANES) if paired else (2, rows, tile_count * per_owner)
    placed, target = pl.pallas_call(
        functools.partial(place_history_kernel, per_owner, paired),
        out_shape=[jax.ShapeDtypeStruct(shape, f32), jax.ShapeDtypeStruct((slots, LANES), jnp.int32)],
        in_specs=whole(6),
        out_specs=whole(2),
        cost_estimate=cost(2 * 4 * rows * slots * 4 * slots, 3000000),
        compiler_params=grant,
        name="place_history",
    )(by_rows.reshape(2 * groups * HISTORY, LANES), past, past_west, past_east, sides, owner.reshape(1, slots))
    shape = (shape[0], rows + 8, shape[2])
    outgoing = pl.pallas_call(
        functools.partial(place_samples_kernel, per_owner, paired, (float(tile_rows), float(tile_cols))),
        out_shape=jax.ShapeDtypeStruct(shape, f32),
        in_specs=whole(9),
        out_specs=whole(1)[0],
        cost_estimate=cost(2 * 2 * 16 * slots * 4 * slots, 3000000),
        compiler_params=grant,
        name="place_samples",
    )(record, lead, lead_west, lead_east, sides, first, cells, target, placed)
    if not paired:
        outgoing = outgoing.reshape(2, rows + 8, tile_count, per_owner).transpose(2, 1, 0, 3)
    arrived = lax.all_to_all(outgoing, ("ty", "tx"), split_axis=0, concat_axis=0, tiled=True)
    if not paired:
        arrived = arrived.transpose(2, 1, 0, 3).reshape(shape)
    filtered = pl.pallas_call(
        functools.partial(filter_kernel, per_owner, paired),
        out_shape=jax.ShapeDtypeStruct((SAMPLES * 4 * groups * 2, LANES), f32),
        in_specs=whole(2),
        out_specs=whole(1)[0],
        scratch_shapes=[pltpu.VMEM((rows + 8, LANES), f32)],
        cost_estimate=cost(2 * 3 * 80 * 80 * 8 * slots, 3000000),
        compiler_params=grant,
        name="filter_series",
    )(filter_matrix, arrived)
    filtered = filtered.reshape(SAMPLES, 4 * groups, 2, LANES)
    return filtered.transpose(2, 0, 1, 3).reshape(2, SAMPLES, 4 * slots)


def solution(mesh):
    placed = (
        P(None, None, "ty", "tx"),
        P(None, ("ty", "tx")),
        P(None, None, None, ("ty", "tx")),
        P(None, None, ("ty", "tx")),
        P(),
        P(("ty", "tx"), None),
        P(),
    )
    return jax.shard_map(
        per_device,
        mesh=mesh,
        in_specs=placed,
        out_specs=P(None, None, ("ty", "tx")),
        check_vma=False,
    )
```

```python
import functools

import jax
import jax.numpy as jnp
from jax import lax
from jax.experimental import pallas as pl
from jax.experimental.pallas import tpu as pltpu
from jax.sharding import Mesh
from jax.sharding import PartitionSpec as P


STEPS = 2
SAMPLES = 73
HISTORY = 71
MOST = 16


drift = 0.2
moves = ((-1, -1), (-1, 0), (-1, 1), (0, -1), (0, 1), (1, -1), (1, 0), (1, 1))
f32 = jnp.float32
bf16 = jnp.bfloat16
LANES = 128


def up(value, to):
    return -(-value // to) * to


places = {"ty": "ty", "tx": ("half", "within")}


def shifted(value, axis, by):
    peers = lax.axis_size(places[axis])
    return lax.ppermute(value, places[axis], [(i, (i + by) % peers) for i in range(peers)])


def swapped(value):
    return lax.ppermute(value, "half", [(0, 1), (1, 0)])


def halves(value):
    high = value.astype(bf16)
    return high, (value - high.astype(f32)).astype(bf16)


def picked(condition):
    return jnp.where(condition, 1.0, 0.0).astype(f32)


def iota(shape, dim):
    return lax.broadcasted_iota(jnp.int32, shape, dim)


def whole(count):
    return [pl.BlockSpec(memory_space=pltpu.VMEM) for _ in range(count)]


def cost(flops, moved):
    return pl.CostEstimate(flops=flops, bytes_accessed=moved, transcendentals=0)


grant = pltpu.CompilerParams(vmem_limit_bytes=16 * 1024 * 1024)


def build_table(table_ref, number, snapshots, weight, velocity_ref, north_ref, south_ref, west_ref, east_ref, columns):
    rows, cols = velocity_ref.shape[2], velocity_ref.shape[3]
    count = velocity_ref.shape[1]
    base = 2 * HISTORY
    block = up(rows + 2, 16)
    lane = iota((16, cols), 1)
    sub = iota((16, cols), 0)
    for c in range(2):
        inner = None
        for a in snapshots:
            k = c * count + a
            body = velocity_ref[c, a]
            side = pltpu.roll(columns, (cols - k) % cols, 1)
            at = base + k
            top, low = north_ref[at : at + 1], south_ref[at : at + 1]
            edge = jnp.where(sub == 0, top, jnp.where(sub == 1, low, 0.0))
            at += 2 * count
            north_west, north_east = west_ref[at : at + 1, cols - 1 :], east_ref[at : at + 1, 0:1]
            at += 2 * count
            south_west, south_east = west_ref[at : at + 1, cols - 1 :], east_ref[at : at + 1, 0:1]
            west = jnp.where(sub == 0, north_west, jnp.where(sub == 1, south_west, 0.0))
            east = jnp.where(sub == 0, north_east, jnp.where(sub == 1, south_east, 0.0))
            corner = jnp.where(lane == 0, west, jnp.where(lane == 8, east, 0.0))
            parts = (body, side, edge, corner)
            inner = parts if inner is None else tuple(p + q for p, q in zip(inner, parts))
        body, side, edge, corner = (weight * p if weight != 1.0 else p for p in inner)
        for split, (b, s, e, n) in enumerate(zip(halves(body), halves(side), halves(edge), halves(corner))):
            at = (split * 2 + c) * block
            table_ref[number, at : at + rows, 0:cols] = b
            table_ref[number, at : at + rows, cols : 2 * cols] = s
            table_ref[number, at + rows : at + block, 0:cols] = e
            table_ref[number, at + rows : at + block, cols : 2 * cols] = n


def read_corners(table_ref, number, cell, rows, cols):
    block = up(rows + 2, 16)
    slots = cell.shape[1]
    cy, cx = cell[0:1], cell[1:2]
    at = iota((2 * cols, slots), 0)
    left = picked(at == jnp.where(cx < 0, cols, cx)).astype(bf16)
    right = picked(at == jnp.where(cx + 1 >= cols, cols + 8, cx + 1)).astype(bf16)
    row = iota((block, slots), 0)
    upper = row == jnp.where(cy < 0, rows, cy)
    lower = row == jnp.where(cy + 1 >= rows, rows + 1, cy + 1)
    table = table_ref[number]
    values = {}
    for side, onehot in enumerate((left, right)):
        product = jnp.dot(table, onehot, preferred_element_type=f32)
        for c in range(2):
            column = product[c * block : (c + 1) * block] + product[(2 + c) * block : (3 + c) * block]
            values[0, side, c] = jnp.sum(jnp.where(upper, column, 0.0), axis=0, keepdims=True)
            values[1, side, c] = jnp.sum(jnp.where(lower, column, 0.0), axis=0, keepdims=True)
    return [[values[v, h, c] for c in range(2)] for v in range(2) for h in range(2)]


def bilinear(corners, point, cell):
    wy = point[0] - cell[0:1].astype(f32)
    wx = point[1] - cell[1:2].astype(f32)
    first, second, third, fourth = corners
    return [
        (1.0 - wy) * ((1.0 - wx) * first[c] + wx * second[c]) + wy * ((1.0 - wx) * third[c] + wx * fourth[c])
        for c in range(2)
    ]


def along(point, factor, speed):
    return [p + factor * s for p, s in zip(point, speed)]


def halo_columns(west_ref, east_ref, count, cols):
    zeros = jnp.zeros((8 - count, cols), f32)
    base = 2 * HISTORY
    west, east = west_ref[base : base + count], east_ref[base : base + count]
    flat = jnp.concatenate([west, zeros, east, zeros, jnp.zeros((cols - 16, cols), f32)], axis=0)
    return flat.T


def step_kernel(step, following, velocity_ref, north_ref, south_ref, west_ref, east_ref, point_ref, cells_ref, *rest):
    if step > 0:
        first_ref, rest = rest[0], rest[1:]
    if following:
        record_ref, lead_ref, next_ref, table_ref = rest
    else:
        record_ref, lead_ref, table_ref = rest
    rows, cols = velocity_ref.shape[2], velocity_ref.shape[3]
    columns = halo_columns(west_ref, east_ref, 2 * velocity_ref.shape[1], cols)
    fields = (velocity_ref, north_ref, south_ref, west_ref, east_ref, columns)
    build_table(table_ref, 0, (step,), 1.0, *fields)
    build_table(table_ref, 1, (step, step + 1), 0.5, *fields)
    build_table(table_ref, 2, (step + 1,), 1.0, *fields)
    sections = [cells_ref[step, s] for s in range(4)]
    if step == 0:
        first = read_corners(table_ref, 0, sections[0], rows, cols)
    else:
        first = [[first_ref[2 * i + c : 2 * i + c + 1] for c in range(2)] for i in range(4)]
    second = read_corners(table_ref, 1, sections[1], rows, cols)
    third = read_corners(table_ref, 1, sections[2], rows, cols)
    fourth = read_corners(table_ref, 2, sections[3], rows, cols)
    point = [point_ref[0:1], point_ref[1:2]]
    k_one = bilinear(first, point, sections[0])
    k_two = bilinear(second, along(point, 0.5 * drift, k_one), sections[1])
    k_three = bilinear(third, along(point, 0.5 * drift, k_two), sections[2])
    k_four = bilinear(fourth, along(point, drift, k_three), sections[3])
    point = [
        p + drift / 6.0 * (a + 2.0 * b + 2.0 * c + d)
        for p, a, b, c, d in zip(point, k_one, k_two, k_three, k_four)
    ]
    blank = [jnp.zeros_like(point[0])] * 4
    record = jnp.concatenate(point + k_one + blank, axis=0)
    record_ref[...] = record
    band = step * 8 * MOST
    lead_ref[...] = record[:, band : band + 8 * MOST]
    if following:
        ahead = read_corners(table_ref, 2, cells_ref[step + 1, 0], rows, cols)
        next_ref[...] = jnp.concatenate([value for corner in ahead for value in corner], axis=0)


def run_step(step, halo, point, first, cells):
    velocity = halo[0]
    slots = point.shape[1]
    following = step + 1 < STEPS
    cols = velocity.shape[3]
    block = up(velocity.shape[2] + 2, 16)
    operands = (*halo, point, cells) + ((first,) if step > 0 else ())
    shape = jax.ShapeDtypeStruct((8, slots), f32)
    shapes = [shape, jax.ShapeDtypeStruct((8, 8 * MOST), f32)] + ([shape] if following else [])
    return pl.pallas_call(
        functools.partial(step_kernel, step, following),
        out_shape=shapes,
        in_specs=whole(len(operands)),
        out_specs=whole(len(shapes)),
        scratch_shapes=[pltpu.VMEM((3, 4 * block, 2 * cols), bf16)],
        cost_estimate=cost(10 * 4 * block * 2 * cols * slots * 2, 600000),
        compiler_params=grant,
        name="sample_step",
    )(*operands)


def sides_kernel(leavers_ref, sides_ref):
    slot = iota((1, 8 * MOST), 1)
    for step in range(leavers_ref.shape[0]):
        rows = [jnp.zeros((1, 8 * MOST), f32) for _ in range(2)]
        start = 0
        for j in range(8):
            end = start + leavers_ref[step, j]
            inside = (slot >= start) & (slot < end)
            rows = [jnp.where(inside, float(moves[j][axis]), rows[axis]) for axis in range(2)]
            start = end
        sides_ref[step] = jnp.concatenate(rows + [jnp.zeros((6, 8 * MOST), f32)], axis=0)


def find_sides(leavers):
    return pl.pallas_call(
        sides_kernel,
        out_shape=jax.ShapeDtypeStruct((leavers.shape[0], 8, 8 * MOST), f32),
        in_specs=[pl.BlockSpec(memory_space=pltpu.SMEM)],
        out_specs=whole(1)[0],
        compiler_params=grant,
        cost_estimate=cost(100000, 5000),
        name="find_sides",
    )(leavers)


def chosen(side, value, forward, backward):
    return jnp.where(side > 0.0, forward, jnp.where(side < 0.0, backward, value))


def paired_halves(first, second, width):
    lane = iota(first.shape, 1)
    left = jnp.where(lane < width, first, pltpu.roll(second, width, 1))
    right = jnp.where(lane < width, pltpu.roll(first, width, 1), second)
    return left, right


def targets_of(owner_row, half, within, width):
    slots = owner_row.shape[1]
    half = half.astype(f32)
    column = jnp.floor((owner_row + 0.5) / within)
    line = jnp.floor((column + 0.5) * 0.5)
    block = line * within + (owner_row - column * within)
    base = jnp.where(column - 2.0 * line == half, block * width, -1.0e6)
    row = iota((LANES, slots), 0)
    turned = jnp.where(row == 0, owner_row, base).T
    owner, base = turned[:, 0:1], turned[:, 1:2]
    before = iota((slots, slots), 1) < iota((slots, slots), 0)
    rank = jnp.sum(picked((owner == owner_row) & before), axis=1, keepdims=True)
    return (base + rank).astype(jnp.int32)


def place_history_kernel(
    width, paired, within, half_ref, owner_ref, history_ref, past_ref, far_owner_ref, far_history_ref, far_past_ref, out_ref, target_ref
):
    slots = owner_ref.shape[1]
    half = half_ref[0]
    rows = up(HISTORY, 8)
    groups = slots // LANES
    moving = 8 * MOST // LANES
    total = out_ref.shape[0] * width if paired else out_ref.shape[3]
    tiles = ((half, owner_ref, history_ref, past_ref), (1 - half, far_owner_ref, far_history_ref, far_past_ref))
    for order, (number, owners, raw, past) in enumerate(tiles):
        target = targets_of(owners[...], half, within, width)
        target_ref[order] = jnp.broadcast_to(target, (slots, LANES))
        parts = []
        for c in range(2):
            pieces = [past[pl.ds(c, HISTORY, stride=2), :]]
            pieces += [raw[pl.ds(2 * g + c, HISTORY, stride=2 * groups), :] for g in range(moving, groups)]
            parts += [jnp.concatenate(pieces, axis=1), jnp.zeros((rows - HISTORY, slots), f32)]
        joined = jnp.concatenate(halves(jnp.concatenate(parts, axis=0)), axis=0)
        chunk = 256
        base = pl.multiple_of(number * rows, 8)
        for start in range(0, total, chunk):
            onehot = picked(target == start + iota((slots, chunk), 1)).astype(bf16)
            product = jnp.dot(joined, onehot, preferred_element_type=f32)
            placed = product[: 2 * rows] + product[2 * rows :]
            if paired:
                for at in range(0, chunk, LANES):
                    pair = paired_halves(placed[:rows, at : at + LANES], placed[rows:, at : at + LANES], width)
                    for i in range(2):
                        out_ref[(start + at) // width + i, pl.ds(base, rows), :] = pair[i]
            else:
                out_ref[number, 0, :, start : start + chunk] = placed[:rows]
                out_ref[number, 1, :, start : start + chunk] = placed[rows:]


def last_samples_kernel(tile, record_ref, lead_ref, west_ref, east_ref, sides_ref, next_ref, cells_ref, out_ref):
    slots = record_ref.shape[1]
    moved = lead_ref.shape[1]
    sides = sides_ref[0]
    lead = chosen(sides[1:2], lead_ref[...], west_ref[...], east_ref[...])
    sub = iota(lead.shape, 0)
    lowered = jnp.where(sub == 0, sides[0:1] * tile[0], jnp.where(sub == 1, sides[1:2] * tile[1], 0.0))
    record = jnp.concatenate([lead - lowered, record_ref[:, moved:]], axis=1)
    corners = [[next_ref[2 * i + c : 2 * i + c + 1] for c in range(2)] for i in range(4)]
    last = bilinear(corners, [record[0:1], record[1:2]], cells_ref[STEPS - 1, 0])
    blank = jnp.zeros((4, slots), f32)
    out_ref[...] = jnp.concatenate([last[0], record[2:3], last[1], record[3:4], blank], axis=0)


def place_samples_kernel(width, paired, half_ref, samples_ref, far_samples_ref, target_ref, placed_ref, out_ref):
    slots = samples_ref.shape[1]
    half = half_ref[0]
    rows = up(HISTORY, 8)
    total = out_ref.shape[0] * width if paired else out_ref.shape[3]
    chunk = 256
    row = iota((8, LANES), 0)
    wide = iota((8, chunk), 0)
    blank = jnp.zeros((6, slots), f32)
    numbers = (half, 1 - half)
    lefts = []
    for samples in (samples_ref, far_samples_ref):
        columns = []
        for c in range(2):
            columns += [samples[2 * c : 2 * c + 1], blank, samples[2 * c + 1 : 2 * c + 2]]
        lefts.append(jnp.concatenate(halves(jnp.concatenate(columns, axis=0)), axis=0))
    for start in range(0, total, chunk):
        values = []
        for order in range(2):
            onehot = picked(target_ref[order, :, 0:1] == start + iota((slots, chunk), 1)).astype(bf16)
            product = jnp.dot(lefts[order], onehot, preferred_element_type=f32)
            values.append(product[:16] + product[16:])
        if paired:
            for at in range(0, chunk, LANES):
                pairs = [paired_halves(v[:8, at : at + LANES], v[8:, at : at + LANES], width) for v in values]
                for i in range(2):
                    block = (start + at) // width + i
                    out_ref[block, 0 : 2 * rows] = placed_ref[block, 0 : 2 * rows]
                    behind = jnp.zeros((8, LANES), f32)
                    for order in range(2):
                        value = pairs[order][i]
                        place = pl.ds(pl.multiple_of(numbers[order] * rows + rows - 8, 8), 8)
                        out_ref[block, place, :] = jnp.where(row == 7, value, placed_ref[block, place, :])
                        behind = jnp.where(row == numbers[order], value[0:1], behind)
                    out_ref[block, 2 * rows : 2 * rows + 8] = behind
        else:
            span = slice(start, start + chunk)
            for order in range(2):
                for c in range(2):
                    value = values[order][8 * c : 8 * c + 8]
                    old = placed_ref[numbers[order], c, :, span]
                    out_ref[numbers[order], c, 0 : rows - 8, span] = old[0 : rows - 8]
                    out_ref[numbers[order], c, rows - 8 : rows, span] = jnp.where(wide == 7, value, old[rows - 8 : rows])
                    out_ref[numbers[order], c, rows : rows + 8, span] = jnp.where(wide == 0, value, 0.0)


def filter_kernel(width, paired, across, matrix_ref, arrived_ref, out_ref, wide_ref):
    depth = wide_ref.shape[0]
    rows = depth - 8
    samples = matrix_ref.shape[0]
    groups = out_ref.shape[0] // (2 * samples)
    wide_ref[...] = jnp.zeros_like(wide_ref)
    wide_ref[0:samples, 0:samples] = matrix_ref[...]
    wide_ref[0:samples, samples : samples + 1] = matrix_ref[:, samples - 1 : samples]
    high, low = halves(wide_ref[:, 0:depth])
    left = jnp.concatenate([high, low, high], axis=1)
    row = iota((8, LANES), 0)

    def block_of(tile):
        line, column = tile // across, tile % across
        number, column = column // (across // 2), column % (across // 2)
        block = line * (across // 2) + column
        behind = jnp.where(row == number, arrived_ref[block, 2 * rows : 2 * rows + 8], 0.0)
        return jnp.concatenate([arrived_ref[block, number * rows : (number + 1) * rows], behind], axis=0)

    step = 4
    for first in range(0, groups, step):
        start = first * LANES
        if paired:
            tiles = [
                paired_halves(block_of(at // width), block_of(at // width + 1), width)
                for at in range(start, start + step * LANES, LANES)
            ]
            columns = [jnp.concatenate([t[c] for t in tiles], axis=1) for c in range(2)]
        else:
            columns = [arrived_ref[c, :, start : start + step * LANES] for c in range(2)]
        for c in range(2):
            x_high, x_low = halves(columns[c])
            right = jnp.concatenate([x_high, x_high, x_low], axis=0)
            product = jnp.dot(left, right, preferred_element_type=f32)
            for g in range(step):
                target = pl.ds(2 * (first + g) + c, samples, stride=2 * groups)
                out_ref[target, :] = product[:samples, g * LANES : (g + 1) * LANES]


def run(velocity, start_position, cells, history, leavers, owner, filter_matrix):
    tile_rows = velocity.shape[2]
    tile_cols = velocity.shape[3]
    slots = start_position.shape[1]
    within = lax.axis_size("within")
    members = lax.axis_size("ty") * within
    tile_count = 2 * members
    per_owner = 4 * slots // tile_count
    paired = 2 * per_owner == LANES
    groups = slots // LANES
    lines = 2 * HISTORY
    by_rows = history.reshape(2, HISTORY, groups, LANES).transpose(1, 2, 0, 3)
    raw = by_rows.reshape(2 * groups * HISTORY, LANES)
    past = by_rows[:, 0].reshape(lines, LANES)
    sides = find_sides(leavers)

    def joined(*parts):
        return jnp.concatenate([part.reshape(-1, LANES) for part in parts], axis=0)

    north = shifted(joined(past, velocity[:, :, tile_rows - 1]), "ty", 1)
    south = shifted(joined(past, velocity[:, :, 0]), "ty", -1)
    past = chosen(sides[0, 0:1], past, north[:lines], south[:lines])
    west = shifted(joined(past, velocity[:, :, :, tile_cols - 1], north[lines:], south[lines:]), "tx", 1)
    east = shifted(joined(past, velocity[:, :, :, 0], north[lines:], south[lines:]), "tx", -1)
    past = chosen(sides[0, 1:2], past, west[:lines], east[:lines])
    halo = (velocity, north, south, west, east)
    owner = owner.astype(f32)
    past = jnp.concatenate([past, owner.reshape(groups, LANES), jnp.zeros((2, LANES), f32)], axis=0)
    far_raw = swapped(raw)
    far_past = swapped(past)
    far_owner = far_past[2 * HISTORY : 2 * HISTORY + groups].reshape(1, slots)
    half = lax.axis_index("half").reshape(1)
    record, lead, first = run_step(0, halo, start_position, None, cells)
    lead = chosen(sides[0, 0:1], lead, shifted(lead, "ty", 1), shifted(lead, "ty", -1))
    lead_west, lead_east = shifted(lead, "tx", 1), shifted(lead, "tx", -1)
    rows = up(HISTORY, 8)
    scalar = [pl.BlockSpec(memory_space=pltpu.SMEM)]
    shape = (members, 2 * rows, LANES) if paired else (2, 2, rows, members * per_owner)
    placed, target = pl.pallas_call(
        functools.partial(place_history_kernel, per_owner, paired, within),
        out_shape=[jax.ShapeDtypeStruct(shape, f32), jax.ShapeDtypeStruct((2, slots, LANES), jnp.int32)],
        in_specs=scalar + whole(6),
        out_specs=whole(2),
        cost_estimate=cost(2 * 4 * rows * slots * 4 * slots, 3000000),
        compiler_params=grant,
        name="place_history",
    )(half, owner.reshape(1, slots), raw, past, far_owner, far_raw, far_past)
    samples = pl.pallas_call(
        functools.partial(last_samples_kernel, (float(tile_rows), float(tile_cols))),
        out_shape=jax.ShapeDtypeStruct((8, slots), f32),
        in_specs=whole(7),
        out_specs=whole(1)[0],
        cost_estimate=cost(1000000, 100000),
        compiler_params=grant,
        name="last_samples",
    )(record, lead, lead_west, lead_east, sides, first, cells)
    far_samples = swapped(samples)
    shape = (members, 2 * rows + 8, LANES) if paired else (2, 2, rows + 8, members * per_owner)
    outgoing = pl.pallas_call(
        functools.partial(place_samples_kernel, per_owner, paired),
        out_shape=jax.ShapeDtypeStruct(shape, f32),
        in_specs=scalar + whole(4),
        out_specs=whole(1)[0],
        cost_estimate=cost(2 * 2 * 16 * slots * 4 * slots, 3000000),
        compiler_params=grant,
        name="place_samples",
    )(half, samples, far_samples, target, placed)
    if not paired:
        outgoing = outgoing.reshape(2, 2, rows + 8, members, per_owner).transpose(3, 2, 0, 1, 4)
    arrived = lax.all_to_all(outgoing, ("ty", "within"), split_axis=0, concat_axis=0, tiled=True)
    if not paired:
        arrived = arrived.reshape(-1, within, rows + 8, 2, 2, per_owner).transpose(4, 2, 0, 3, 1, 5)
        arrived = arrived.reshape(2, rows + 8, tile_count * per_owner)
    filtered = pl.pallas_call(
        functools.partial(filter_kernel, per_owner, paired, 2 * within),
        out_shape=jax.ShapeDtypeStruct((SAMPLES * 4 * groups * 2, LANES), f32),
        in_specs=whole(2),
        out_specs=whole(1)[0],
        scratch_shapes=[pltpu.VMEM((rows + 8, LANES), f32)],
        cost_estimate=cost(2 * 3 * 80 * 80 * 8 * slots, 3000000),
        compiler_params=grant,
        name="filter_series",
    )(filter_matrix, arrived)
    filtered = filtered.reshape(SAMPLES, 4 * groups, 2, LANES)
    return filtered.transpose(2, 0, 1, 3).reshape(2, SAMPLES, 4 * slots)


def solution(mesh):
    lines, across = mesh.devices.shape
    halved = Mesh(mesh.devices.reshape(lines, 2, across // 2), ("ty", "half", "within"))
    tile = ("ty", "half", "within")
    placed = (
        P(None, None, "ty", ("half", "within")),
        P(None, tile),
        P(None, None, None, tile),
        P(None, None, tile),
        P(),
        P(tile, None),
        P(),
    )
    return jax.shard_map(
        run,
        mesh=halved,
        in_specs=placed,
        out_specs=P(None, None, tile),
        check_vma=False,
    )
```

```python
import functools

import jax
import jax.numpy as jnp
from jax import lax
from jax.experimental import pallas as pl
from jax.experimental.pallas import tpu as pltpu
from jax.sharding import Mesh
from jax.sharding import PartitionSpec as P


STEPS = 2
SAMPLES = 73
HISTORY = 71
MOST = 16


drift = 0.2
moves = ((-1, -1), (-1, 0), (-1, 1), (0, -1), (0, 1), (1, -1), (1, 0), (1, 1))
f32 = jnp.float32
bf16 = jnp.bfloat16
LANES = 128


def up(value, to):
    return -(-value // to) * to


places = {"ty": "ty", "tx": ("half", "within")}


def shifted(value, axis, by):
    peers = lax.axis_size(places[axis])
    return lax.ppermute(value, places[axis], [(i, (i + by) % peers) for i in range(peers)])


def swapped(value):
    return lax.ppermute(value, "half", [(0, 1), (1, 0)])


def halves(value):
    high = value.astype(bf16)
    return high, (value - high.astype(f32)).astype(bf16)


def picked(condition):
    return jnp.where(condition, 1.0, 0.0).astype(f32)


def iota(shape, dim):
    return lax.broadcasted_iota(jnp.int32, shape, dim)


def whole(count):
    return [pl.BlockSpec(memory_space=pltpu.VMEM) for _ in range(count)]


def cost(flops, moved):
    return pl.CostEstimate(flops=flops, bytes_accessed=moved, transcendentals=0)


grant = pltpu.CompilerParams(vmem_limit_bytes=16 * 1024 * 1024)


def build_table(table_ref, number, snapshots, weight, velocity_ref, north_ref, south_ref, west_ref, east_ref, columns):
    rows, cols = velocity_ref.shape[2], velocity_ref.shape[3]
    count = velocity_ref.shape[1]
    base = 2 * HISTORY
    block = up(rows + 2, 16)
    lane = iota((16, cols), 1)
    sub = iota((16, cols), 0)
    for c in range(2):
        inner = None
        for a in snapshots:
            k = c * count + a
            body = velocity_ref[c, a]
            side = pltpu.roll(columns, (cols - k) % cols, 1)
            at = base + k
            top, low = north_ref[at : at + 1], south_ref[at : at + 1]
            edge = jnp.where(sub == 0, top, jnp.where(sub == 1, low, 0.0))
            at += 2 * count
            north_west, north_east = west_ref[at : at + 1, cols - 1 :], east_ref[at : at + 1, 0:1]
            at += 2 * count
            south_west, south_east = west_ref[at : at + 1, cols - 1 :], east_ref[at : at + 1, 0:1]
            west = jnp.where(sub == 0, north_west, jnp.where(sub == 1, south_west, 0.0))
            east = jnp.where(sub == 0, north_east, jnp.where(sub == 1, south_east, 0.0))
            corner = jnp.where(lane == 0, west, jnp.where(lane == 8, east, 0.0))
            parts = (body, side, edge, corner)
            inner = parts if inner is None else tuple(p + q for p, q in zip(inner, parts))
        body, side, edge, corner = (weight * p if weight != 1.0 else p for p in inner)
        for split, (b, s, e, n) in enumerate(zip(halves(body), halves(side), halves(edge), halves(corner))):
            at = (split * 2 + c) * block
            table_ref[number, at : at + rows, 0:cols] = b
            table_ref[number, at : at + rows, cols : 2 * cols] = s
            table_ref[number, at + rows : at + block, 0:cols] = e
            table_ref[number, at + rows : at + block, cols : 2 * cols] = n


def read_corners(table_ref, number, cell, rows, cols):
    block = up(rows + 2, 16)
    slots = cell.shape[1]
    cy, cx = cell[0:1], cell[1:2]
    at = iota((2 * cols, slots), 0)
    left = picked(at == jnp.where(cx < 0, cols, cx)).astype(bf16)
    right = picked(at == jnp.where(cx + 1 >= cols, cols + 8, cx + 1)).astype(bf16)
    row = iota((block, slots), 0)
    upper = row == jnp.where(cy < 0, rows, cy)
    lower = row == jnp.where(cy + 1 >= rows, rows + 1, cy + 1)
    table = table_ref[number]
    values = {}
    for side, onehot in enumerate((left, right)):
        product = jnp.dot(table, onehot, preferred_element_type=f32)
        for c in range(2):
            column = product[c * block : (c + 1) * block] + product[(2 + c) * block : (3 + c) * block]
            values[0, side, c] = jnp.sum(jnp.where(upper, column, 0.0), axis=0, keepdims=True)
            values[1, side, c] = jnp.sum(jnp.where(lower, column, 0.0), axis=0, keepdims=True)
    return [[values[v, h, c] for c in range(2)] for v in range(2) for h in range(2)]


def bilinear(corners, point, cell):
    wy = point[0] - cell[0:1].astype(f32)
    wx = point[1] - cell[1:2].astype(f32)
    first, second, third, fourth = corners
    return [
        (1.0 - wy) * ((1.0 - wx) * first[c] + wx * second[c]) + wy * ((1.0 - wx) * third[c] + wx * fourth[c])
        for c in range(2)
    ]


def along(point, factor, speed):
    return [p + factor * s for p, s in zip(point, speed)]


def halo_columns(west_ref, east_ref, count, cols):
    zeros = jnp.zeros((8 - count, cols), f32)
    base = 2 * HISTORY
    west, east = west_ref[base : base + count], east_ref[base : base + count]
    flat = jnp.concatenate([west, zeros, east, zeros, jnp.zeros((cols - 16, cols), f32)], axis=0)
    return flat.T


def step_kernel(step, following, velocity_ref, north_ref, south_ref, west_ref, east_ref, point_ref, cells_ref, *rest):
    if step > 0:
        first_ref, rest = rest[0], rest[1:]
    if following:
        record_ref, lead_ref, next_ref, table_ref = rest
    else:
        record_ref, lead_ref, table_ref = rest
    rows, cols = velocity_ref.shape[2], velocity_ref.shape[3]
    columns = halo_columns(west_ref, east_ref, 2 * velocity_ref.shape[1], cols)
    fields = (velocity_ref, north_ref, south_ref, west_ref, east_ref, columns)
    build_table(table_ref, 0, (step,), 1.0, *fields)
    build_table(table_ref, 1, (step, step + 1), 0.5, *fields)
    build_table(table_ref, 2, (step + 1,), 1.0, *fields)
    sections = [cells_ref[step, s] for s in range(4)]
    if step == 0:
        first = read_corners(table_ref, 0, sections[0], rows, cols)
    else:
        first = [[first_ref[2 * i + c : 2 * i + c + 1] for c in range(2)] for i in range(4)]
    second = read_corners(table_ref, 1, sections[1], rows, cols)
    third = read_corners(table_ref, 1, sections[2], rows, cols)
    fourth = read_corners(table_ref, 2, sections[3], rows, cols)
    point = [point_ref[0:1], point_ref[1:2]]
    k_one = bilinear(first, point, sections[0])
    k_two = bilinear(second, along(point, 0.5 * drift, k_one), sections[1])
    k_three = bilinear(third, along(point, 0.5 * drift, k_two), sections[2])
    k_four = bilinear(fourth, along(point, drift, k_three), sections[3])
    point = [
        p + drift / 6.0 * (a + 2.0 * b + 2.0 * c + d)
        for p, a, b, c, d in zip(point, k_one, k_two, k_three, k_four)
    ]
    blank = [jnp.zeros_like(point[0])] * 4
    record = jnp.concatenate(point + k_one + blank, axis=0)
    record_ref[...] = record
    band = step * 8 * MOST
    lead_ref[...] = record[:, band : band + 8 * MOST]
    if following:
        ahead = read_corners(table_ref, 2, cells_ref[step + 1, 0], rows, cols)
        next_ref[...] = jnp.concatenate([value for corner in ahead for value in corner], axis=0)


def run_step(step, halo, point, first, cells):
    velocity = halo[0]
    slots = point.shape[1]
    following = step + 1 < STEPS
    cols = velocity.shape[3]
    block = up(velocity.shape[2] + 2, 16)
    operands = (*halo, point, cells) + ((first,) if step > 0 else ())
    shape = jax.ShapeDtypeStruct((8, slots), f32)
    shapes = [shape, jax.ShapeDtypeStruct((8, 8 * MOST), f32)] + ([shape] if following else [])
    return pl.pallas_call(
        functools.partial(step_kernel, step, following),
        out_shape=shapes,
        in_specs=whole(len(operands)),
        out_specs=whole(len(shapes)),
        scratch_shapes=[pltpu.VMEM((3, 4 * block, 2 * cols), bf16)],
        cost_estimate=cost(10 * 4 * block * 2 * cols * slots * 2, 600000),
        compiler_params=grant,
        name="sample_step",
    )(*operands)


def sides_kernel(leavers_ref, sides_ref):
    slot = iota((1, 8 * MOST), 1)
    for step in range(leavers_ref.shape[0]):
        rows = [jnp.zeros((1, 8 * MOST), f32) for _ in range(2)]
        start = 0
        for j in range(8):
            end = start + leavers_ref[step, j]
            inside = (slot >= start) & (slot < end)
            rows = [jnp.where(inside, float(moves[j][axis]), rows[axis]) for axis in range(2)]
            start = end
        sides_ref[step] = jnp.concatenate(rows + [jnp.zeros((6, 8 * MOST), f32)], axis=0)


def find_sides(leavers):
    return pl.pallas_call(
        sides_kernel,
        out_shape=jax.ShapeDtypeStruct((leavers.shape[0], 8, 8 * MOST), f32),
        in_specs=[pl.BlockSpec(memory_space=pltpu.SMEM)],
        out_specs=whole(1)[0],
        compiler_params=grant,
        cost_estimate=cost(100000, 5000),
        name="find_sides",
    )(leavers)


def chosen(side, value, forward, backward):
    return jnp.where(side > 0.0, forward, jnp.where(side < 0.0, backward, value))


def paired_halves(first, second, width):
    lane = iota(first.shape, 1)
    left = jnp.where(lane < width, first, pltpu.roll(second, width, 1))
    right = jnp.where(lane < width, pltpu.roll(first, width, 1), second)
    return left, right


def targets_of(owner_row, half, within, width):
    slots = owner_row.shape[1]
    half = half.astype(f32)
    column = jnp.floor((owner_row + 0.5) / within)
    line = jnp.floor((column + 0.5) * 0.5)
    block = line * within + (owner_row - column * within)
    base = jnp.where(column - 2.0 * line == half, block * width, -1.0e6)
    row = iota((LANES, slots), 0)
    turned = jnp.where(row == 0, owner_row, base).T
    owner, base = turned[:, 0:1], turned[:, 1:2]
    before = iota((slots, slots), 1) < iota((slots, slots), 0)
    rank = jnp.sum(picked((owner == owner_row) & before), axis=1, keepdims=True)
    return (base + rank).astype(jnp.int32)


def place_history_kernel(width, paired, within, skipped, half_ref, owner_ref, history_ref, past_ref, out_ref, onehot_ref):
    slots = owner_ref.shape[1]
    rows = up(HISTORY, 8)
    groups = slots // LANES
    moving = 8 * MOST // LANES
    total = onehot_ref.shape[1]
    target = targets_of(owner_ref[...], half_ref[0], within, width)
    parts = []
    for c in range(2):
        pieces = [past_ref[pl.ds(c, HISTORY, stride=2), :]]
        for g in range(moving, groups):
            pieces.append(history_ref[pl.ds(2 * (g - skipped) + c, HISTORY, stride=2 * (groups - skipped)), :])
        parts += [jnp.concatenate(pieces, axis=1), jnp.zeros((rows - HISTORY, slots), f32)]
    joined = jnp.concatenate(halves(jnp.concatenate(parts, axis=0)), axis=0)
    chunk = 256
    for start in range(0, total, chunk):
        onehot = picked(target == start + iota((slots, chunk), 1)).astype(bf16)
        onehot_ref[:, start : start + chunk] = onehot
        product = jnp.dot(joined, onehot, preferred_element_type=f32)
        placed = product[: 2 * rows] + product[2 * rows :]
        if paired:
            for at in range(0, chunk, LANES):
                pair = paired_halves(placed[:rows, at : at + LANES], placed[rows:, at : at + LANES], width)
                for i in range(2):
                    out_ref[(start + at) // width + i] = pair[i]
        else:
            out_ref[0, :, start : start + chunk] = placed[:rows]
            out_ref[1, :, start : start + chunk] = placed[rows:]


def last_samples_kernel(tile, record_ref, lead_ref, west_ref, east_ref, sides_ref, next_ref, cells_ref, out_ref):
    moved = lead_ref.shape[1]
    sides = sides_ref[0]
    lead = chosen(sides[1:2], lead_ref[...], west_ref[...], east_ref[...])
    sub = iota(lead.shape, 0)
    lowered = jnp.where(sub == 0, sides[0:1] * tile[0], jnp.where(sub == 1, sides[1:2] * tile[1], 0.0))
    record = jnp.concatenate([lead - lowered, record_ref[:, moved:]], axis=1)
    corners = [[next_ref[2 * i + c : 2 * i + c + 1] for c in range(2)] for i in range(4)]
    last = bilinear(corners, [record[0:1], record[1:2]], cells_ref[STEPS - 1, 0])
    out_ref[...] = jnp.concatenate([record[2:3], last[0], record[3:4], last[1]], axis=0)


def place_samples_kernel(
    width, paired, half_ref, samples_ref, far_samples_ref, onehot_ref, far_onehot_ref, placed_ref, far_placed_ref, out_ref
):
    half = half_ref[0]
    rows = up(HISTORY, 8)
    total = onehot_ref.shape[1]
    chunk = 256
    row = iota((8, LANES), 0)
    wide = iota((8, chunk), 0)
    tiles = (
        (half, samples_ref, onehot_ref, placed_ref),
        (1 - half, far_samples_ref, far_onehot_ref, far_placed_ref),
    )
    lefts = []
    for number, samples, _, _ in tiles:
        columns = []
        for c in range(2):
            early, late = samples[2 * c : 2 * c + 1], samples[2 * c + 1 : 2 * c + 2]
            at = iota((8, early.shape[1]), 0)
            columns.append(jnp.where(at == number, early, jnp.where(at == number + 2, late, 0.0)))
        lefts.append(jnp.concatenate(halves(jnp.concatenate(columns, axis=0)), axis=0))
    for start in range(0, total, chunk):
        span = slice(start, start + chunk)
        values = None
        for left, (_, _, onehot, _) in zip(lefts, tiles):
            product = jnp.dot(left, onehot[:, span], preferred_element_type=f32)
            value = product[:16] + product[16:]
            values = value if values is None else values + value
        if paired:
            for at in range(0, chunk, LANES):
                pair = paired_halves(values[:8, at : at + LANES], values[8:, at : at + LANES], width)
                for i in range(2):
                    block = (start + at) // width + i
                    for number, _, _, placed in tiles:
                        out_ref[block, pl.ds(pl.multiple_of(number * rows, 8), rows), :] = placed[block]
                    out_ref[block, 2 * rows : 2 * rows + 8] = pair[i]
        else:
            for c in range(2):
                for number, _, _, placed in tiles:
                    out_ref[c, pl.ds(pl.multiple_of(number * rows, 8), rows), span] = placed[c, :, span]
                out_ref[c, 2 * rows : 2 * rows + 8, span] = values[8 * c : 8 * c + 8]


def filter_kernel(width, paired, across, matrix_ref, arrived_ref, out_ref, wide_ref, ready_ref, sems):
    depth = wide_ref.shape[0]
    rows = depth - 8
    samples = matrix_ref.shape[0]
    groups = out_ref.shape[2] // 2
    row = iota((8, LANES), 0)
    wide_ref[...] = jnp.zeros_like(wide_ref)
    wide_ref[0:samples, 0:HISTORY] = matrix_ref[:, 0:HISTORY]
    for late in range(STEPS):
        for number in range(2):
            at = rows + 2 * late + number
            wide_ref[0:samples, at : at + 1] = matrix_ref[:, HISTORY + late : HISTORY + late + 1]
    high, low = halves(wide_ref[:, 0:depth])
    left = jnp.concatenate([high, low, high], axis=1)

    def block_of(tile):
        line, column = tile // across, tile % across
        number, column = column // (across // 2), column % (across // 2)
        block = line * (across // 2) + column
        behind = jnp.where((row == number) | (row == number + 2), arrived_ref[block, 2 * rows : 2 * rows + 8], 0.0)
        return jnp.concatenate([arrived_ref[block, number * rows : (number + 1) * rows], behind], axis=0)

    copies = []
    for run in range(out_ref.shape[1]):
        start = run * groups * LANES
        if paired:
            spots = range(start // width, (start + groups * LANES) // width, 2)
            tiles = [paired_halves(block_of(at), block_of(at + 1), width) for at in spots]
            columns = [jnp.concatenate([t[c] for t in tiles], axis=1) for c in range(2)]
        else:
            columns = [arrived_ref[c, :, start : start + groups * LANES] for c in range(2)]
        for c in range(2):
            x_high, x_low = halves(columns[c])
            right = jnp.concatenate([x_high, x_high, x_low], axis=0)
            product = jnp.dot(left, right, preferred_element_type=f32)
            for g in range(groups):
                target = pl.ds(2 * g + c, samples, stride=2 * groups)
                ready_ref[run, target, :] = product[:samples, g * LANES : (g + 1) * LANES]
        source = ready_ref.at[run].reshape(samples, 2 * groups, LANES)
        copies.append(pltpu.make_async_copy(source, out_ref.at[:, run], sems.at[run]))
        copies[-1].start()
    for copy in copies:
        copy.wait()


def run(velocity, start_position, cells, history, leavers, owner, filter_matrix):
    tile_rows = velocity.shape[2]
    tile_cols = velocity.shape[3]
    slots = start_position.shape[1]
    within = lax.axis_size("within")
    members = lax.axis_size("ty") * within
    tile_count = 2 * members
    per_owner = 4 * slots // tile_count
    paired = 2 * per_owner == LANES
    groups = slots // LANES
    lines = 2 * HISTORY
    by_rows = history.reshape(2, HISTORY, groups, LANES).transpose(1, 2, 0, 3)
    raw = by_rows.reshape(2 * groups * HISTORY, LANES)
    past = by_rows[:, 0].reshape(lines, LANES)
    sides = find_sides(leavers)

    def joined(*parts):
        return jnp.concatenate([part.reshape(-1, LANES) for part in parts], axis=0)

    north = shifted(joined(past, velocity[:, :, tile_rows - 1]), "ty", 1)
    south = shifted(joined(past, velocity[:, :, 0]), "ty", -1)
    past = chosen(sides[0, 0:1], past, north[:lines], south[:lines])
    west = shifted(joined(past, velocity[:, :, :, tile_cols - 1], north[lines:], south[lines:]), "tx", 1)
    east = shifted(joined(past, velocity[:, :, :, 0], north[lines:], south[lines:]), "tx", -1)
    past = chosen(sides[0, 1:2], past, west[:lines], east[:lines])
    halo = (velocity, north, south, west, east)
    owner = owner.astype(f32)
    past = joined(past, owner, jnp.zeros((2, LANES), f32))
    moving = 8 * MOST // LANES
    far_raw = swapped(by_rows[:, moving:].reshape(2 * (groups - moving) * HISTORY, LANES))
    far_past = swapped(past)
    far_owner = far_past[lines : lines + groups].reshape(1, slots)
    half = lax.axis_index("half").reshape(1)
    record, lead, first = run_step(0, halo, start_position, None, cells)
    lead = chosen(sides[0, 0:1], lead, shifted(lead, "ty", 1), shifted(lead, "ty", -1))
    lead_west, lead_east = shifted(lead, "tx", 1), shifted(lead, "tx", -1)
    rows = up(HISTORY, 8)
    scalar = [pl.BlockSpec(memory_space=pltpu.SMEM)]
    span = members * per_owner
    shape = (members, rows, LANES) if paired else (2, rows, span)

    def place(owner, raw, past, skipped):
        return pl.pallas_call(
            functools.partial(place_history_kernel, per_owner, paired, within, skipped),
            out_shape=[jax.ShapeDtypeStruct(shape, f32), jax.ShapeDtypeStruct((slots, span), bf16)],
            in_specs=scalar + whole(3),
            out_specs=whole(2),
            cost_estimate=cost(2 * 4 * rows * slots * span, 3000000),
            compiler_params=grant,
            name="place_history",
        )(half, owner, raw, past)

    placed, onehot = place(owner.reshape(1, slots), raw, past, 0)
    far_placed, far_onehot = place(far_owner, far_raw, far_past, moving)
    samples = pl.pallas_call(
        functools.partial(last_samples_kernel, (float(tile_rows), float(tile_cols))),
        out_shape=jax.ShapeDtypeStruct((2 * STEPS, slots), f32),
        in_specs=whole(7),
        out_specs=whole(1)[0],
        cost_estimate=cost(1000000, 100000),
        compiler_params=grant,
        name="last_samples",
    )(record, lead, lead_west, lead_east, sides, first, cells)
    far_samples = swapped(samples)
    depth = 2 * rows + 8
    outgoing = pl.pallas_call(
        functools.partial(place_samples_kernel, per_owner, paired),
        out_shape=jax.ShapeDtypeStruct((members, depth, LANES) if paired else (2, depth, span), f32),
        in_specs=scalar + whole(6),
        out_specs=whole(1)[0],
        cost_estimate=cost(2 * 2 * 32 * slots * span, 3000000),
        compiler_params=grant,
        name="place_samples",
    )(half, samples, far_samples, onehot, far_onehot, placed, far_placed)
    if not paired:
        outgoing = outgoing.reshape(2, depth, members, per_owner).transpose(2, 1, 0, 3)
    arrived = lax.all_to_all(outgoing, ("ty", "within"), split_axis=0, concat_axis=0, tiled=True)
    runs = 4 * groups // 4
    if not paired:
        behind = arrived[:, 2 * rows :]
        number = jnp.arange(8)[:, None] % 2 == jnp.arange(2)
        behind = jnp.where(number[None, :, :, None, None], behind[:, :, None], 0.0)
        arrived = arrived[:, : 2 * rows].reshape(members, 2, rows, 2, per_owner).transpose(0, 2, 1, 3, 4)
        arrived = jnp.concatenate([arrived, behind], axis=1)
        arrived = arrived.reshape(-1, within, rows + 8, 2, 2, per_owner).transpose(4, 2, 0, 3, 1, 5)
        arrived = arrived.reshape(2, rows + 8, tile_count * per_owner)
    filtered = pl.pallas_call(
        functools.partial(filter_kernel, per_owner, paired, 2 * within),
        out_shape=jax.ShapeDtypeStruct((SAMPLES, runs, 8, LANES), f32),
        in_specs=whole(2),
        out_specs=pl.BlockSpec(memory_space=pltpu.HBM),
        scratch_shapes=[
            pltpu.VMEM((rows + 8, LANES), f32),
            pltpu.VMEM((runs, SAMPLES * 8, LANES), f32),
            pltpu.SemaphoreType.DMA((runs,)),
        ],
        cost_estimate=cost(2 * 3 * 80 * 80 * 8 * slots, 3000000),
        compiler_params=grant,
        name="filter_series",
    )(filter_matrix, arrived)
    filtered = filtered.reshape(SAMPLES, 4 * groups, 2, LANES)
    return filtered.transpose(2, 0, 1, 3).reshape(2, SAMPLES, 4 * slots)


def solution(mesh):
    lines, across = mesh.devices.shape
    halved = Mesh(mesh.devices.reshape(lines, 2, across // 2), ("ty", "half", "within"))
    tile = ("ty", "half", "within")
    placed = (
        P(None, None, "ty", ("half", "within")),
        P(None, tile),
        P(None, None, None, tile),
        P(None, None, tile),
        P(),
        P(tile, None),
        P(),
    )
    return jax.shard_map(
        run,
        mesh=halved,
        in_specs=placed,
        out_specs=P(None, None, tile),
        check_vma=False,
    )
```

```python
import functools

import jax
import jax.numpy as jnp
from jax import lax
from jax.experimental import pallas as pl
from jax.experimental.pallas import tpu as pltpu
from jax.sharding import Mesh
from jax.sharding import PartitionSpec as P


STEPS = 2
SAMPLES = 73
HISTORY = 71
MOST = 16


drift = 0.2
moves = ((-1, -1), (-1, 0), (-1, 1), (0, -1), (0, 1), (1, -1), (1, 0), (1, 1))
f32 = jnp.float32
bf16 = jnp.bfloat16
LANES = 128


def up(value, to):
    return -(-value // to) * to


places = {"ty": "ty", "tx": ("half", "within")}


def exchanged(up, down, axis):
    peers = lax.axis_size(places[axis])
    even = lax.axis_index(places[axis]) % 2 == 0
    near = [(i, i ^ 1) for i in range(peers)]
    far = [(i, (i - 1 if i % 2 == 0 else i + 1) % peers) for i in range(peers)]
    first = lax.ppermute(up if up is down else jnp.where(even, up, down), places[axis], near)
    second = lax.ppermute(up if up is down else jnp.where(even, down, up), places[axis], far)
    return jnp.where(even, second, first), jnp.where(even, first, second)


def swapped(value):
    return lax.ppermute(value, "half", [(0, 1), (1, 0)])


def halves(value):
    high = value.astype(bf16)
    return high, (value - high.astype(f32)).astype(bf16)


def picked(condition):
    return jnp.where(condition, 1.0, 0.0).astype(f32)


def iota(shape, dim):
    return lax.broadcasted_iota(jnp.int32, shape, dim)


def whole(count):
    return [pl.BlockSpec(memory_space=pltpu.VMEM) for _ in range(count)]


def cost(flops, moved):
    return pl.CostEstimate(flops=flops, bytes_accessed=moved, transcendentals=0)


grant = pltpu.CompilerParams(vmem_limit_bytes=16 * 1024 * 1024)


def sections_of(step, following):
    own = [(step, 0, 0)] if step == 0 else []
    own += [(step, 1, 1), (step, 2, 1), (step, 3, 2)]
    return own + ([(step + 1, 0, 2)] if following else [])


def at_time(read, step, table):
    if table == 1:
        return 0.5 * (read(step) + read(step + 1))
    return read(step + table // 2)


def side_by_side(value):
    return jnp.concatenate(halves(value), axis=1)


def doubled(value):
    return jnp.concatenate([value, value], axis=0)


def inner_kernel(step, following, velocity_ref, cells_ref, part_ref, cols_ref, rows_ref, table_ref):
    rows, cols = velocity_ref.shape[2], velocity_ref.shape[3]
    slots = cells_ref.shape[3]
    for table in range(3):
        for c in range(2):
            value = at_time(lambda a: velocity_ref[c, a], step, table)
            table_ref[table, c * rows : (c + 1) * rows] = side_by_side(value)
    col = iota((cols, slots), 0)
    row = iota((rows, slots), 0)
    for number, (k, section, table) in enumerate(sections_of(step, following)):
        cy, cx = cells_ref[k, section, 0:1], cells_ref[k, section, 1:2]
        across = [picked(row == cy), picked(row == cy + 1)]
        for v in range(2):
            rows_ref[number, v] = across[v].astype(bf16)
        values = {}
        for h in range(2):
            onehot = picked(col == cx + h).astype(bf16)
            cols_ref[number, h] = onehot
            product = jnp.dot(table_ref[table], doubled(onehot), preferred_element_type=f32)
            for c in range(2):
                for v in range(2):
                    kept = across[v] * product[c * rows : (c + 1) * rows]
                    values[v, h, c] = jnp.sum(kept, axis=0, keepdims=True)
        corners = [values[v, h, c] for v in range(2) for h in range(2) for c in range(2)]
        part_ref[number] = jnp.concatenate(corners, axis=0)


def bilinear(corners, point, cell):
    wy = point[0] - cell[0:1].astype(f32)
    wx = point[1] - cell[1:2].astype(f32)
    first, second, third, fourth = corners
    return [
        (1.0 - wy) * ((1.0 - wx) * first[c] + wx * second[c]) + wy * ((1.0 - wx) * third[c] + wx * fourth[c])
        for c in range(2)
    ]


def along(point, factor, speed):
    return [p + factor * s for p, s in zip(point, speed)]


def step_kernel(
    step, following, velocity_shape, part_ref, cols_ref, rows_ref, north_ref, south_ref, west_ref, east_ref, point_ref, cells_ref, *rest
):
    if step > 0:
        first_ref, rest = rest[0], rest[1:]
    if following:
        record_ref, lead_ref, next_ref = rest
    else:
        record_ref, lead_ref = rest
    count, rows, cols = velocity_shape
    ends = ((north_ref, south_ref), (west_ref, east_ref))
    tables = []
    for pair in ends:
        lines = []
        for table in range(3):
            for c in range(2):
                for ref in pair:
                    lines.append(at_time(lambda a: ref[c * count + a : c * count + a + 1], step, table))
        lines.append(jnp.zeros((4, cols), f32))
        tables.append(side_by_side(jnp.concatenate(lines, axis=0)))

    def tip(table, c, v, h):
        ref, at = ends[1][h], (1 + v) * 2 * count + c * count
        lane = slice(cols - 1, cols) if h == 0 else slice(0, 1)
        return at_time(lambda a: ref[at + a : at + a + 1, lane], step, table)

    def corners_of(number):
        k, section, table = sections_of(step, following)[number]
        cy, cx = cells_ref[k, section, 0:1], cells_ref[k, section, 1:2]
        outside = ((cy < 0, cy + 1 >= rows), (cx < 0, cx + 1 >= cols))
        ends_of = [
            jnp.dot(tables[0], doubled(cols_ref[number, i]), preferred_element_type=f32) for i in range(2)
        ], [jnp.dot(tables[1], doubled(rows_ref[number, i]), preferred_element_type=f32) for i in range(2)]
        result = []
        for v in range(2):
            for h in range(2):
                pair = []
                for c in range(2):
                    value = part_ref[number, 4 * v + 2 * h + c : 4 * v + 2 * h + c + 1]
                    at = 4 * table + 2 * c
                    value += jnp.where(outside[0][v], ends_of[0][h][at + v : at + v + 1], 0.0)
                    value += jnp.where(outside[1][h], ends_of[1][v][at + h : at + h + 1], 0.0)
                    value += jnp.where(outside[0][v] & outside[1][h], tip(table, c, v, h), 0.0)
                    pair.append(value)
                result.append(pair)
        return result

    corners = [corners_of(number) for number in range(len(sections_of(step, following)))]
    sections = [cells_ref[step, s] for s in range(4)]
    if step > 0:
        given = [[first_ref[2 * i + c : 2 * i + c + 1] for c in range(2)] for i in range(4)]
        corners = [given] + corners
    point = [point_ref[0:1], point_ref[1:2]]
    k_one = bilinear(corners[0], point, sections[0])
    k_two = bilinear(corners[1], along(point, 0.5 * drift, k_one), sections[1])
    k_three = bilinear(corners[2], along(point, 0.5 * drift, k_two), sections[2])
    k_four = bilinear(corners[3], along(point, drift, k_three), sections[3])
    point = [
        p + drift / 6.0 * (a + 2.0 * b + 2.0 * c + d)
        for p, a, b, c, d in zip(point, k_one, k_two, k_three, k_four)
    ]
    blank = [jnp.zeros_like(point[0])] * 4
    record = jnp.concatenate(point + k_one + blank, axis=0)
    record_ref[...] = record
    band = step * 8 * MOST
    lead_ref[...] = record[:, band : band + 8 * MOST]
    if following:
        next_ref[...] = jnp.concatenate([value for corner in corners[4] for value in corner], axis=0)


def run_step(step, halo, point, first, cells):
    velocity, *ends = halo
    slots = point.shape[1]
    following = step + 1 < STEPS
    rows, cols = velocity.shape[2:]
    number = len(sections_of(step, following))
    inner = pl.pallas_call(
        functools.partial(inner_kernel, step, following),
        out_shape=[
            jax.ShapeDtypeStruct((number, 8, slots), f32),
            jax.ShapeDtypeStruct((number, 2, cols, slots), bf16),
            jax.ShapeDtypeStruct((number, 2, rows, slots), bf16),
        ],
        in_specs=whole(2),
        out_specs=whole(3),
        scratch_shapes=[pltpu.VMEM((3, 2 * rows, 2 * cols), bf16)],
        cost_estimate=cost(number * 2 * 2 * rows * 2 * cols * slots * 2, 600000),
        compiler_params=grant,
        name="sample_inner",
    )(velocity, cells)
    operands = (*inner, *ends, point, cells) + ((first,) if step > 0 else ())
    shape = jax.ShapeDtypeStruct((8, slots), f32)
    shapes = [shape, jax.ShapeDtypeStruct((8, 8 * MOST), f32)] + ([shape] if following else [])
    return pl.pallas_call(
        functools.partial(step_kernel, step, following, velocity.shape[1:]),
        out_shape=shapes,
        in_specs=whole(len(operands)),
        out_specs=whole(len(shapes)),
        cost_estimate=cost(number * 2 * 4 * 16 * 2 * cols * slots, 600000),
        compiler_params=grant,
        name="sample_step",
    )(*operands)


def sides_kernel(leavers_ref, sides_ref):
    slot = iota((1, 8 * MOST), 1)
    for step in range(leavers_ref.shape[0]):
        rows = [jnp.zeros((1, 8 * MOST), f32) for _ in range(2)]
        start = 0
        for j in range(8):
            end = start + leavers_ref[step, j]
            inside = (slot >= start) & (slot < end)
            rows = [jnp.where(inside, float(moves[j][axis]), rows[axis]) for axis in range(2)]
            start = end
        sides_ref[step] = jnp.concatenate(rows + [jnp.zeros((6, 8 * MOST), f32)], axis=0)


def find_sides(leavers):
    return pl.pallas_call(
        sides_kernel,
        out_shape=jax.ShapeDtypeStruct((leavers.shape[0], 8, 8 * MOST), f32),
        in_specs=[pl.BlockSpec(memory_space=pltpu.SMEM)],
        out_specs=whole(1)[0],
        compiler_params=grant,
        cost_estimate=cost(100000, 5000),
        name="find_sides",
    )(leavers)


def chosen(side, value, forward, backward):
    return jnp.where(side > 0.0, forward, jnp.where(side < 0.0, backward, value))


def paired_halves(first, second, width):
    lane = iota(first.shape, 1)
    left = jnp.where(lane < width, first, pltpu.roll(second, width, 1))
    right = jnp.where(lane < width, pltpu.roll(first, width, 1), second)
    return left, right


def targets_of(owner_row, half, within, width):
    slots = owner_row.shape[1]
    half = half.astype(f32)
    column = jnp.floor((owner_row + 0.5) / within)
    line = jnp.floor((column + 0.5) * 0.5)
    block = line * within + (owner_row - column * within)
    base = jnp.where(column - 2.0 * line == half, block * width, -1.0e6)
    row = iota((LANES, slots), 0)
    turned = jnp.where(row == 0, owner_row, base).T
    owner, base = turned[:, 0:1], turned[:, 1:2]
    before = iota((slots, slots), 1) < iota((slots, slots), 0)
    rank = jnp.sum(picked((owner == owner_row) & before), axis=1, keepdims=True)
    return (base + rank).astype(jnp.int32)


def place_history_kernel(width, paired, within, skipped, half_ref, owner_ref, history_ref, past_ref, out_ref, onehot_ref):
    slots = owner_ref.shape[1]
    rows = up(HISTORY, 8)
    groups = slots // LANES
    moving = 8 * MOST // LANES
    total = onehot_ref.shape[1]
    target = targets_of(owner_ref[...], half_ref[0], within, width)
    parts = []
    for c in range(2):
        pieces = [past_ref[pl.ds(c, HISTORY, stride=2), :]]
        for g in range(moving, groups):
            pieces.append(history_ref[pl.ds(2 * (g - skipped) + c, HISTORY, stride=2 * (groups - skipped)), :])
        parts += [jnp.concatenate(pieces, axis=1), jnp.zeros((rows - HISTORY, slots), f32)]
    joined = jnp.concatenate(halves(jnp.concatenate(parts, axis=0)), axis=0)
    chunk = 256
    for start in range(0, total, chunk):
        onehot = picked(target == start + iota((slots, chunk), 1)).astype(bf16)
        onehot_ref[:, start : start + chunk] = onehot
        product = jnp.dot(joined, onehot, preferred_element_type=f32)
        placed = product[: 2 * rows] + product[2 * rows :]
        if paired:
            for at in range(0, chunk, LANES):
                pair = paired_halves(placed[:rows, at : at + LANES], placed[rows:, at : at + LANES], width)
                for i in range(2):
                    out_ref[(start + at) // width + i] = pair[i]
        else:
            out_ref[0, :, start : start + chunk] = placed[:rows]
            out_ref[1, :, start : start + chunk] = placed[rows:]


def last_samples_kernel(tile, record_ref, lead_ref, west_ref, east_ref, sides_ref, next_ref, cells_ref, out_ref, point_ref):
    moved = lead_ref.shape[1]
    sides = sides_ref[0]
    lead = chosen(sides[1:2], lead_ref[...], west_ref[...], east_ref[...])
    sub = iota(lead.shape, 0)
    lowered = jnp.where(sub == 0, sides[0:1] * tile[0], jnp.where(sub == 1, sides[1:2] * tile[1], 0.0))
    record = jnp.concatenate([lead - lowered, record_ref[:, moved:]], axis=1)
    corners = [[next_ref[2 * i + c : 2 * i + c + 1] for c in range(2)] for i in range(4)]
    last = bilinear(corners, [record[0:1], record[1:2]], cells_ref[STEPS - 1, 0])
    out_ref[...] = jnp.concatenate([record[2:3], last[0], record[3:4], last[1]], axis=0)
    point_ref[...] = record[0:2]


def place_samples_kernel(
    width, paired, half_ref, samples_ref, far_samples_ref, onehot_ref, far_onehot_ref, placed_ref, far_placed_ref, out_ref
):
    half = half_ref[0]
    rows = up(HISTORY, 8)
    total = onehot_ref.shape[1]
    chunk = 256
    row = iota((8, LANES), 0)
    wide = iota((8, chunk), 0)
    tiles = (
        (half, samples_ref, onehot_ref, placed_ref),
        (1 - half, far_samples_ref, far_onehot_ref, far_placed_ref),
    )
    lefts = []
    for number, samples, _, _ in tiles:
        columns = []
        for c in range(2):
            early, late = samples[2 * c : 2 * c + 1], samples[2 * c + 1 : 2 * c + 2]
            at = iota((8, early.shape[1]), 0)
            columns.append(jnp.where(at == number, early, jnp.where(at == number + 2, late, 0.0)))
        lefts.append(jnp.concatenate(halves(jnp.concatenate(columns, axis=0)), axis=0))
    for start in range(0, total, chunk):
        span = slice(start, start + chunk)
        values = None
        for left, (_, _, onehot, _) in zip(lefts, tiles):
            product = jnp.dot(left, onehot[:, span], preferred_element_type=f32)
            value = product[:16] + product[16:]
            values = value if values is None else values + value
        if paired:
            for at in range(0, chunk, LANES):
                pair = paired_halves(values[:8, at : at + LANES], values[8:, at : at + LANES], width)
                for i in range(2):
                    block = (start + at) // width + i
                    for number, _, _, placed in tiles:
                        out_ref[block, pl.ds(pl.multiple_of(number * rows, 8), rows), :] = placed[block]
                    out_ref[block, 2 * rows : 2 * rows + 8] = pair[i]
        else:
            for c in range(2):
                for number, _, _, placed in tiles:
                    out_ref[c, pl.ds(pl.multiple_of(number * rows, 8), rows), span] = placed[c, :, span]
                out_ref[c, 2 * rows : 2 * rows + 8, span] = values[8 * c : 8 * c + 8]


def filter_kernel(width, paired, across, matrix_ref, arrived_ref, out_ref, wide_ref, ready_ref, sems):
    depth = wide_ref.shape[0]
    rows = depth - 8
    samples = matrix_ref.shape[0]
    groups = out_ref.shape[2] // 2
    row = iota((8, LANES), 0)
    wide_ref[...] = jnp.zeros_like(wide_ref)
    wide_ref[0:samples, 0:HISTORY] = matrix_ref[:, 0:HISTORY]
    for late in range(STEPS):
        for number in range(2):
            at = rows + 2 * late + number
            wide_ref[0:samples, at : at + 1] = matrix_ref[:, HISTORY + late : HISTORY + late + 1]
    high, low = halves(wide_ref[:, 0:depth])
    left = jnp.concatenate([high, low, high], axis=1)

    def block_of(tile):
        line, column = tile // across, tile % across
        number, column = column // (across // 2), column % (across // 2)
        block = line * (across // 2) + column
        behind = jnp.where((row == number) | (row == number + 2), arrived_ref[block, 2 * rows : 2 * rows + 8], 0.0)
        return jnp.concatenate([arrived_ref[block, number * rows : (number + 1) * rows], behind], axis=0)

    copies = []
    for run in range(out_ref.shape[1]):
        start = run * groups * LANES
        if paired:
            spots = range(start // width, (start + groups * LANES) // width, 2)
            tiles = [paired_halves(block_of(at), block_of(at + 1), width) for at in spots]
            columns = [jnp.concatenate([t[c] for t in tiles], axis=1) for c in range(2)]
        else:
            columns = [arrived_ref[c, :, start : start + groups * LANES] for c in range(2)]
        for c in range(2):
            x_high, x_low = halves(columns[c])
            right = jnp.concatenate([x_high, x_high, x_low], axis=0)
            product = jnp.dot(left, right, preferred_element_type=f32)
            for g in range(groups):
                target = pl.ds(2 * g + c, samples, stride=2 * groups)
                ready_ref[run, target, :] = product[:samples, g * LANES : (g + 1) * LANES]
        source = ready_ref.at[run].reshape(samples, 2 * groups, LANES)
        copies.append(pltpu.make_async_copy(source, out_ref.at[:, run], sems.at[run]))
        copies[-1].start()
    for copy in copies:
        copy.wait()


def run(velocity, start_position, cells, history, leavers, owner, filter_matrix):
    tile_rows = velocity.shape[2]
    tile_cols = velocity.shape[3]
    slots = start_position.shape[1]
    within = lax.axis_size("within")
    members = lax.axis_size("ty") * within
    tile_count = 2 * members
    per_owner = 4 * slots // tile_count
    paired = 2 * per_owner == LANES
    groups = slots // LANES

    def joined(*parts):
        return jnp.concatenate([part.reshape(-1, LANES) for part in parts], axis=0)

    lines = 2 * HISTORY
    north, south = exchanged(joined(velocity[:, :, tile_rows - 1]), joined(velocity[:, :, 0]), "ty")
    west, east = exchanged(
        joined(velocity[:, :, :, tile_cols - 1], north, south), joined(velocity[:, :, :, 0], north, south), "tx"
    )
    by_rows = history.reshape(2, HISTORY, groups, LANES).transpose(1, 2, 0, 3)
    raw = by_rows.reshape(2 * groups * HISTORY, LANES)
    sides = find_sides(leavers)
    past = by_rows[:, 0].reshape(lines, LANES)
    past = chosen(sides[0, 0:1], past, *exchanged(past, past, "ty"))
    past = chosen(sides[0, 1:2], past, *exchanged(past, past, "tx"))
    halo = (velocity, north, south, west, east)
    owner = owner.astype(f32)
    past = joined(past, owner, jnp.zeros((2, LANES), f32))
    moving = 8 * MOST // LANES
    far_raw = swapped(by_rows[:, moving:].reshape(2 * (groups - moving) * HISTORY, LANES))
    far_past = swapped(past)
    far_owner = far_past[lines : lines + groups].reshape(1, slots)
    half = lax.axis_index("half").reshape(1)
    record, lead, first = run_step(0, halo, start_position, None, cells)
    lead = chosen(sides[0, 0:1], lead, *exchanged(lead, lead, "ty"))
    lead_west, lead_east = exchanged(lead, lead, "tx")
    rows = up(HISTORY, 8)
    scalar = [pl.BlockSpec(memory_space=pltpu.SMEM)]
    span = members * per_owner
    shape = (members, rows, LANES) if paired else (2, rows, span)

    def place(owner, raw, past, skipped):
        return pl.pallas_call(
            functools.partial(place_history_kernel, per_owner, paired, within, skipped),
            out_shape=[jax.ShapeDtypeStruct(shape, f32), jax.ShapeDtypeStruct((slots, span), bf16)],
            in_specs=scalar + whole(3),
            out_specs=whole(2),
            cost_estimate=cost(2 * 4 * rows * slots * span, 3000000),
            compiler_params=grant,
            name="place_history",
        )(half, owner, raw, past)

    placed, onehot = place(owner.reshape(1, slots), raw, past, 0)
    far_placed, far_onehot = place(far_owner, far_raw, far_past, moving)
    samples, point = pl.pallas_call(
        functools.partial(last_samples_kernel, (float(tile_rows), float(tile_cols))),
        out_shape=[jax.ShapeDtypeStruct((2 * STEPS, slots), f32), jax.ShapeDtypeStruct((2, slots), f32)],
        in_specs=whole(7),
        out_specs=whole(2),
        cost_estimate=cost(1000000, 100000),
        compiler_params=grant,
        name="last_samples",
    )(record, lead, lead_west, lead_east, sides, first, cells)
    run_step(STEPS - 1, halo, point, first, cells)
    far_samples = swapped(samples)
    depth = 2 * rows + 8
    outgoing = pl.pallas_call(
        functools.partial(place_samples_kernel, per_owner, paired),
        out_shape=jax.ShapeDtypeStruct((members, depth, LANES) if paired else (2, depth, span), f32),
        in_specs=scalar + whole(6),
        out_specs=whole(1)[0],
        cost_estimate=cost(2 * 2 * 32 * slots * span, 3000000),
        compiler_params=grant,
        name="place_samples",
    )(half, samples, far_samples, onehot, far_onehot, placed, far_placed)
    if not paired:
        outgoing = outgoing.reshape(2, depth, members, per_owner).transpose(2, 1, 0, 3)
    arrived = lax.all_to_all(outgoing, ("ty", "within"), split_axis=0, concat_axis=0, tiled=True)
    runs = 4 * groups // 4
    if not paired:
        behind = arrived[:, 2 * rows :]
        number = jnp.arange(8)[:, None] % 2 == jnp.arange(2)
        behind = jnp.where(number[None, :, :, None, None], behind[:, :, None], 0.0)
        arrived = arrived[:, : 2 * rows].reshape(members, 2, rows, 2, per_owner).transpose(0, 2, 1, 3, 4)
        arrived = jnp.concatenate([arrived, behind], axis=1)
        arrived = arrived.reshape(-1, within, rows + 8, 2, 2, per_owner).transpose(4, 2, 0, 3, 1, 5)
        arrived = arrived.reshape(2, rows + 8, tile_count * per_owner)
    filtered = pl.pallas_call(
        functools.partial(filter_kernel, per_owner, paired, 2 * within),
        out_shape=jax.ShapeDtypeStruct((SAMPLES, runs, 8, LANES), f32),
        in_specs=whole(2),
        out_specs=pl.BlockSpec(memory_space=pltpu.HBM),
        scratch_shapes=[
            pltpu.VMEM((rows + 8, LANES), f32),
            pltpu.VMEM((runs, SAMPLES * 8, LANES), f32),
            pltpu.SemaphoreType.DMA((runs,)),
        ],
        cost_estimate=cost(2 * 3 * 80 * 80 * 8 * slots, 3000000),
        compiler_params=grant,
        name="filter_series",
    )(filter_matrix, arrived)
    filtered = filtered.reshape(SAMPLES, 4 * groups, 2, LANES)
    return filtered.transpose(2, 0, 1, 3).reshape(2, SAMPLES, 4 * slots)


def solution(mesh):
    lines, across = mesh.devices.shape
    halved = Mesh(mesh.devices.reshape(lines, 2, across // 2), ("ty", "half", "within"))
    tile = ("ty", "half", "within")
    placed = (
        P(None, None, "ty", ("half", "within")),
        P(None, tile),
        P(None, None, None, tile),
        P(None, None, tile),
        P(),
        P(tile, None),
        P(),
    )
    return jax.shard_map(
        run,
        mesh=halved,
        in_specs=placed,
        out_specs=P(None, None, tile),
        check_vma=False,
    )
```

```python
import functools

import jax
import jax.numpy as jnp
from jax import lax
from jax.experimental import pallas as pl
from jax.experimental.pallas import tpu as pltpu
from jax.sharding import Mesh
from jax.sharding import PartitionSpec as P


STEPS = 2
SAMPLES = 73
HISTORY = 71
MOST = 16


drift = 0.2
moves = ((-1, -1), (-1, 0), (-1, 1), (0, -1), (0, 1), (1, -1), (1, 0), (1, 1))
f32 = jnp.float32
bf16 = jnp.bfloat16
LANES = 128


def up(value, to):
    return -(-value // to) * to


places = {"ty": "ty", "tx": ("half", "within")}


def exchanged(up, down, axis):
    peers = lax.axis_size(places[axis])
    even = lax.axis_index(places[axis]) % 2 == 0
    near = [(i, i ^ 1) for i in range(peers)]
    far = [(i, (i - 1 if i % 2 == 0 else i + 1) % peers) for i in range(peers)]
    first = lax.ppermute(up if up is down else jnp.where(even, up, down), places[axis], near)
    second = lax.ppermute(up if up is down else jnp.where(even, down, up), places[axis], far)
    return jnp.where(even, second, first), jnp.where(even, first, second)


def swapped(value):
    return lax.ppermute(value, "half", [(0, 1), (1, 0)])


def halves(value):
    high = value.astype(bf16)
    return high, (value - high.astype(f32)).astype(bf16)


def picked(condition):
    return jnp.where(condition, 1.0, 0.0).astype(f32)


def iota(shape, dim):
    return lax.broadcasted_iota(jnp.int32, shape, dim)


def whole(count):
    return [pl.BlockSpec(memory_space=pltpu.VMEM) for _ in range(count)]


def cost(flops, moved):
    return pl.CostEstimate(flops=flops, bytes_accessed=moved, transcendentals=0)


grant = pltpu.CompilerParams(vmem_limit_bytes=16 * 1024 * 1024)


def sections_of(step, following):
    own = [(step, 0, 0)] if step == 0 else []
    own += [(step, 1, 1), (step, 2, 1), (step, 3, 2)]
    return own + ([(step + 1, 0, 2)] if following else [])


def at_time(read, step, table):
    if table == 1:
        return 0.5 * (read(step) + read(step + 1))
    return read(step + table // 2)


def side_by_side(value):
    return jnp.concatenate(halves(value), axis=1)


def doubled(value):
    return jnp.concatenate([value, value], axis=0)


def inner_kernel(step, following, velocity_ref, cells_ref, part_ref, cols_ref, rows_ref, table_ref):
    rows, cols = velocity_ref.shape[2], velocity_ref.shape[3]
    slots = cells_ref.shape[3]
    for table in range(3):
        for c in range(2):
            value = at_time(lambda a: velocity_ref[c, a], step, table)
            table_ref[table, c * rows : (c + 1) * rows] = side_by_side(value)
    col = iota((cols, slots), 0)
    row = iota((rows, slots), 0)
    for number, (k, section, table) in enumerate(sections_of(step, following)):
        cy, cx = cells_ref[k, section, 0:1], cells_ref[k, section, 1:2]
        across = [picked(row == cy), picked(row == cy + 1)]
        for v in range(2):
            rows_ref[number, v] = across[v].astype(bf16)
        values = {}
        for h in range(2):
            onehot = picked(col == cx + h).astype(bf16)
            cols_ref[number, h] = onehot
            product = jnp.dot(table_ref[table], doubled(onehot), preferred_element_type=f32)
            for c in range(2):
                for v in range(2):
                    kept = across[v] * product[c * rows : (c + 1) * rows]
                    values[v, h, c] = jnp.sum(kept, axis=0, keepdims=True)
        corners = [values[v, h, c] for v in range(2) for h in range(2) for c in range(2)]
        part_ref[number] = jnp.concatenate(corners, axis=0)


def bilinear(corners, point, cell):
    wy = point[0] - cell[0:1].astype(f32)
    wx = point[1] - cell[1:2].astype(f32)
    first, second, third, fourth = corners
    return [
        (1.0 - wy) * ((1.0 - wx) * first[c] + wx * second[c]) + wy * ((1.0 - wx) * third[c] + wx * fourth[c])
        for c in range(2)
    ]


def along(point, factor, speed):
    return [p + factor * s for p, s in zip(point, speed)]


def step_kernel(
    step, following, velocity_shape, part_ref, cols_ref, rows_ref, north_ref, south_ref, west_ref, east_ref, point_ref, cells_ref, *rest
):
    if step > 0:
        first_ref, rest = rest[0], rest[1:]
    if following:
        record_ref, lead_ref, next_ref = rest
    else:
        record_ref, lead_ref = rest
    count, rows, cols = velocity_shape
    base = 2 * HISTORY
    ends = ((north_ref, south_ref), (west_ref, east_ref))
    tables = []
    for pair in ends:
        lines = []
        for table in range(3):
            for c in range(2):
                for ref in pair:
                    lines.append(at_time(lambda a: ref[base + c * count + a : base + c * count + a + 1], step, table))
        lines.append(jnp.zeros((4, cols), f32))
        tables.append(side_by_side(jnp.concatenate(lines, axis=0)))

    def tip(table, c, v, h):
        ref, at = ends[1][h], base + (1 + v) * 2 * count + c * count
        lane = slice(cols - 1, cols) if h == 0 else slice(0, 1)
        return at_time(lambda a: ref[at + a : at + a + 1, lane], step, table)

    def corners_of(number):
        k, section, table = sections_of(step, following)[number]
        cy, cx = cells_ref[k, section, 0:1], cells_ref[k, section, 1:2]
        outside = ((cy < 0, cy + 1 >= rows), (cx < 0, cx + 1 >= cols))
        ends_of = [
            jnp.dot(tables[0], doubled(cols_ref[number, i]), preferred_element_type=f32) for i in range(2)
        ], [jnp.dot(tables[1], doubled(rows_ref[number, i]), preferred_element_type=f32) for i in range(2)]
        result = []
        for v in range(2):
            for h in range(2):
                pair = []
                for c in range(2):
                    value = part_ref[number, 4 * v + 2 * h + c : 4 * v + 2 * h + c + 1]
                    at = 4 * table + 2 * c
                    value += jnp.where(outside[0][v], ends_of[0][h][at + v : at + v + 1], 0.0)
                    value += jnp.where(outside[1][h], ends_of[1][v][at + h : at + h + 1], 0.0)
                    value += jnp.where(outside[0][v] & outside[1][h], tip(table, c, v, h), 0.0)
                    pair.append(value)
                result.append(pair)
        return result

    corners = [corners_of(number) for number in range(len(sections_of(step, following)))]
    sections = [cells_ref[step, s] for s in range(4)]
    if step > 0:
        given = [[first_ref[2 * i + c : 2 * i + c + 1] for c in range(2)] for i in range(4)]
        corners = [given] + corners
    point = [point_ref[0:1], point_ref[1:2]]
    k_one = bilinear(corners[0], point, sections[0])
    k_two = bilinear(corners[1], along(point, 0.5 * drift, k_one), sections[1])
    k_three = bilinear(corners[2], along(point, 0.5 * drift, k_two), sections[2])
    k_four = bilinear(corners[3], along(point, drift, k_three), sections[3])
    point = [
        p + drift / 6.0 * (a + 2.0 * b + 2.0 * c + d)
        for p, a, b, c, d in zip(point, k_one, k_two, k_three, k_four)
    ]
    blank = [jnp.zeros_like(point[0])] * 4
    record = jnp.concatenate(point + k_one + blank, axis=0)
    record_ref[...] = record
    band = step * 8 * MOST
    lead_ref[...] = record[:, band : band + 8 * MOST]
    if following:
        next_ref[...] = jnp.concatenate([value for corner in corners[4] for value in corner], axis=0)


def run_step(step, halo, point, first, cells):
    velocity, *ends = halo
    slots = point.shape[1]
    following = step + 1 < STEPS
    rows, cols = velocity.shape[2:]
    number = len(sections_of(step, following))
    inner = pl.pallas_call(
        functools.partial(inner_kernel, step, following),
        out_shape=[
            jax.ShapeDtypeStruct((number, 8, slots), f32),
            jax.ShapeDtypeStruct((number, 2, cols, slots), bf16),
            jax.ShapeDtypeStruct((number, 2, rows, slots), bf16),
        ],
        in_specs=whole(2),
        out_specs=whole(3),
        scratch_shapes=[pltpu.VMEM((3, 2 * rows, 2 * cols), bf16)],
        cost_estimate=cost(number * 2 * 2 * rows * 2 * cols * slots * 2, 600000),
        compiler_params=grant,
        name="sample_inner",
    )(velocity, cells)
    operands = (*inner, *ends, point, cells) + ((first,) if step > 0 else ())
    shape = jax.ShapeDtypeStruct((8, slots), f32)
    shapes = [shape, jax.ShapeDtypeStruct((8, 8 * MOST), f32)] + ([shape] if following else [])
    return pl.pallas_call(
        functools.partial(step_kernel, step, following, velocity.shape[1:]),
        out_shape=shapes,
        in_specs=whole(len(operands)),
        out_specs=whole(len(shapes)),
        cost_estimate=cost(number * 2 * 4 * 16 * 2 * cols * slots, 600000),
        compiler_params=grant,
        name="sample_step",
    )(*operands)


def sides_kernel(leavers_ref, sides_ref):
    slot = iota((1, 8 * MOST), 1)
    for step in range(leavers_ref.shape[0]):
        rows = [jnp.zeros((1, 8 * MOST), f32) for _ in range(2)]
        start = 0
        for j in range(8):
            end = start + leavers_ref[step, j]
            inside = (slot >= start) & (slot < end)
            rows = [jnp.where(inside, float(moves[j][axis]), rows[axis]) for axis in range(2)]
            start = end
        sides_ref[step] = jnp.concatenate(rows + [jnp.zeros((6, 8 * MOST), f32)], axis=0)


def find_sides(leavers):
    return pl.pallas_call(
        sides_kernel,
        out_shape=jax.ShapeDtypeStruct((leavers.shape[0], 8, 8 * MOST), f32),
        in_specs=[pl.BlockSpec(memory_space=pltpu.SMEM)],
        out_specs=whole(1)[0],
        compiler_params=grant,
        cost_estimate=cost(100000, 5000),
        name="find_sides",
    )(leavers)


def chosen(side, value, forward, backward):
    return jnp.where(side > 0.0, forward, jnp.where(side < 0.0, backward, value))


def paired_halves(first, second, width):
    lane = iota(first.shape, 1)
    left = jnp.where(lane < width, first, pltpu.roll(second, width, 1))
    right = jnp.where(lane < width, pltpu.roll(first, width, 1), second)
    return left, right


def targets_of(owner_row, half, within, width):
    slots = owner_row.shape[1]
    half = half.astype(f32)
    column = jnp.floor((owner_row + 0.5) / within)
    line = jnp.floor((column + 0.5) * 0.5)
    block = line * within + (owner_row - column * within)
    base = jnp.where(column - 2.0 * line == half, block * width, -1.0e6)
    row = iota((LANES, slots), 0)
    turned = jnp.where(row == 0, owner_row, base).T
    owner, base = turned[:, 0:1], turned[:, 1:2]
    before = iota((slots, slots), 1) < iota((slots, slots), 0)
    rank = jnp.sum(picked((owner == owner_row) & before), axis=1, keepdims=True)
    return (base + rank).astype(jnp.int32)


def place_history_kernel(width, paired, within, skipped, half_ref, owner_ref, history_ref, past_ref, out_ref, onehot_ref):
    slots = owner_ref.shape[1]
    rows = up(HISTORY, 8)
    groups = slots // LANES
    moving = 8 * MOST // LANES
    total = onehot_ref.shape[1]
    target = targets_of(owner_ref[...], half_ref[0], within, width)
    parts = []
    for c in range(2):
        pieces = [past_ref[pl.ds(c, HISTORY, stride=2), :]]
        for g in range(moving, groups):
            pieces.append(history_ref[pl.ds(2 * (g - skipped) + c, HISTORY, stride=2 * (groups - skipped)), :])
        parts += [jnp.concatenate(pieces, axis=1), jnp.zeros((rows - HISTORY, slots), f32)]
    joined = jnp.concatenate(halves(jnp.concatenate(parts, axis=0)), axis=0)
    chunk = 256
    for start in range(0, total, chunk):
        onehot = picked(target == start + iota((slots, chunk), 1)).astype(bf16)
        onehot_ref[:, start : start + chunk] = onehot
        product = jnp.dot(joined, onehot, preferred_element_type=f32)
        placed = product[: 2 * rows] + product[2 * rows :]
        if paired:
            for at in range(0, chunk, LANES):
                pair = paired_halves(placed[:rows, at : at + LANES], placed[rows:, at : at + LANES], width)
                for i in range(2):
                    out_ref[(start + at) // width + i] = pair[i]
        else:
            out_ref[0, :, start : start + chunk] = placed[:rows]
            out_ref[1, :, start : start + chunk] = placed[rows:]


def place_samples_kernel(
    width, paired, half_ref, samples_ref, far_samples_ref, onehot_ref, far_onehot_ref, placed_ref, far_placed_ref, out_ref
):
    half = half_ref[0]
    rows = up(HISTORY, 8)
    total = onehot_ref.shape[1]
    chunk = 256
    row = iota((8, LANES), 0)
    wide = iota((8, chunk), 0)
    tiles = (
        (half, samples_ref, onehot_ref, placed_ref),
        (1 - half, far_samples_ref, far_onehot_ref, far_placed_ref),
    )
    lefts = []
    for number, samples, _, _ in tiles:
        columns = []
        for c in range(2):
            early, late = samples[2 * c : 2 * c + 1], samples[2 * c + 1 : 2 * c + 2]
            at = iota((8, early.shape[1]), 0)
            columns.append(jnp.where(at == number, early, jnp.where(at == number + 2, late, 0.0)))
        lefts.append(jnp.concatenate(halves(jnp.concatenate(columns, axis=0)), axis=0))
    for start in range(0, total, chunk):
        span = slice(start, start + chunk)
        values = None
        for left, (_, _, onehot, _) in zip(lefts, tiles):
            product = jnp.dot(left, onehot[:, span], preferred_element_type=f32)
            value = product[:16] + product[16:]
            values = value if values is None else values + value
        if paired:
            for at in range(0, chunk, LANES):
                pair = paired_halves(values[:8, at : at + LANES], values[8:, at : at + LANES], width)
                for i in range(2):
                    block = (start + at) // width + i
                    for number, _, _, placed in tiles:
                        out_ref[block, pl.ds(pl.multiple_of(number * rows, 8), rows), :] = placed[block]
                    out_ref[block, 2 * rows : 2 * rows + 8] = pair[i]
        else:
            for c in range(2):
                for number, _, _, placed in tiles:
                    out_ref[c, pl.ds(pl.multiple_of(number * rows, 8), rows), span] = placed[c, :, span]
                out_ref[c, 2 * rows : 2 * rows + 8, span] = values[8 * c : 8 * c + 8]


def filter_kernel(width, paired, across, matrix_ref, arrived_ref, out_ref, wide_ref, ready_ref, sems):
    depth = wide_ref.shape[0]
    rows = depth - 8
    samples = matrix_ref.shape[0]
    groups = out_ref.shape[2] // 2
    row = iota((8, LANES), 0)
    wide_ref[...] = jnp.zeros_like(wide_ref)
    wide_ref[0:samples, 0:HISTORY] = matrix_ref[:, 0:HISTORY]
    for late in range(STEPS):
        for number in range(2):
            at = rows + 2 * late + number
            wide_ref[0:samples, at : at + 1] = matrix_ref[:, HISTORY + late : HISTORY + late + 1]
    high, low = halves(wide_ref[:, 0:depth])
    left = jnp.concatenate([high, low, high], axis=1)

    def block_of(tile):
        line, column = tile // across, tile % across
        number, column = column // (across // 2), column % (across // 2)
        block = line * (across // 2) + column
        behind = jnp.where((row == number) | (row == number + 2), arrived_ref[block, 2 * rows : 2 * rows + 8], 0.0)
        return jnp.concatenate([arrived_ref[block, number * rows : (number + 1) * rows], behind], axis=0)

    copies = []
    for run in range(out_ref.shape[1]):
        start = run * groups * LANES
        if paired:
            spots = range(start // width, (start + groups * LANES) // width, 2)
            tiles = [paired_halves(block_of(at), block_of(at + 1), width) for at in spots]
            columns = [jnp.concatenate([t[c] for t in tiles], axis=1) for c in range(2)]
        else:
            columns = [arrived_ref[c, :, start : start + groups * LANES] for c in range(2)]
        for c in range(2):
            x_high, x_low = halves(columns[c])
            right = jnp.concatenate([x_high, x_high, x_low], axis=0)
            product = jnp.dot(left, right, preferred_element_type=f32)
            for g in range(groups):
                target = pl.ds(2 * g + c, samples, stride=2 * groups)
                ready_ref[run, target, :] = product[:samples, g * LANES : (g + 1) * LANES]
        source = ready_ref.at[run].reshape(samples, 2 * groups, LANES)
        copies.append(pltpu.make_async_copy(source, out_ref.at[:, run], sems.at[run]))
        copies[-1].start()
    for copy in copies:
        copy.wait()


def run(velocity, start_position, cells, history, leavers, owner, filter_matrix):
    tile_rows = velocity.shape[2]
    tile_cols = velocity.shape[3]
    slots = start_position.shape[1]
    within = lax.axis_size("within")
    members = lax.axis_size("ty") * within
    tile_count = 2 * members
    per_owner = 4 * slots // tile_count
    paired = 2 * per_owner == LANES
    groups = slots // LANES
    lines = 2 * HISTORY
    by_rows = history.reshape(2, HISTORY, groups, LANES).transpose(1, 2, 0, 3)
    raw = by_rows.reshape(2 * groups * HISTORY, LANES)
    past = by_rows[:, 0].reshape(lines, LANES)
    sides = find_sides(leavers)

    def joined(*parts):
        return jnp.concatenate([part.reshape(-1, LANES) for part in parts], axis=0)

    north, south = exchanged(joined(past, velocity[:, :, tile_rows - 1]), joined(past, velocity[:, :, 0]), "ty")
    past = chosen(sides[0, 0:1], past, north[:lines], south[:lines])
    west, east = exchanged(
        joined(past, velocity[:, :, :, tile_cols - 1], north[lines:], south[lines:]),
        joined(past, velocity[:, :, :, 0], north[lines:], south[lines:]),
        "tx",
    )
    past = chosen(sides[0, 1:2], past, west[:lines], east[:lines])
    halo = (velocity, north, south, west, east)
    owner = owner.astype(f32)
    past = joined(past, owner, jnp.zeros((2, LANES), f32))
    moving = 8 * MOST // LANES
    far_raw = swapped(by_rows[:, moving:].reshape(2 * (groups - moving) * HISTORY, LANES))
    far_past = swapped(past)
    far_owner = far_past[lines : lines + groups].reshape(1, slots)
    half = lax.axis_index("half").reshape(1)
    record, lead, first = run_step(0, halo, start_position, None, cells)
    lead = chosen(sides[0, 0:1], lead, *exchanged(lead, lead, "ty"))
    lead_west, lead_east = exchanged(lead, lead, "tx")
    rows = up(HISTORY, 8)
    scalar = [pl.BlockSpec(memory_space=pltpu.SMEM)]
    span = members * per_owner
    shape = (members, rows, LANES) if paired else (2, rows, span)

    def place(owner, raw, past, skipped):
        return pl.pallas_call(
            functools.partial(place_history_kernel, per_owner, paired, within, skipped),
            out_shape=[jax.ShapeDtypeStruct(shape, f32), jax.ShapeDtypeStruct((slots, span), bf16)],
            in_specs=scalar + whole(3),
            out_specs=whole(2),
            cost_estimate=cost(2 * 4 * rows * slots * span, 3000000),
            compiler_params=grant,
            name="place_history",
        )(half, owner, raw, past)

    placed, onehot = place(owner.reshape(1, slots), raw, past, 0)
    far_placed, far_onehot = place(far_owner, far_raw, far_past, moving)
    lead = chosen(sides[0, 1:2], lead, lead_west, lead_east)
    lowered = [sides[0, 0:1] * tile_rows, sides[0, 1:2] * tile_cols, jnp.zeros((6, 8 * MOST), f32)]
    record = jnp.concatenate([lead - jnp.concatenate(lowered, axis=0), record[:, 8 * MOST :]], axis=1)
    point = record[0:2]
    corners = [[first[2 * i + c : 2 * i + c + 1] for c in range(2)] for i in range(4)]
    last = bilinear(corners, [record[0:1], record[1:2]], cells[STEPS - 1, 0])
    samples = jnp.concatenate([record[2:3], last[0], record[3:4], last[1]], axis=0)
    run_step(STEPS - 1, halo, point, first, cells)
    far_samples = swapped(samples)
    depth = 2 * rows + 8
    outgoing = pl.pallas_call(
        functools.partial(place_samples_kernel, per_owner, paired),
        out_shape=jax.ShapeDtypeStruct((members, depth, LANES) if paired else (2, depth, span), f32),
        in_specs=scalar + whole(6),
        out_specs=whole(1)[0],
        cost_estimate=cost(2 * 2 * 32 * slots * span, 3000000),
        compiler_params=grant,
        name="place_samples",
    )(half, samples, far_samples, onehot, far_onehot, placed, far_placed)
    if not paired:
        outgoing = outgoing.reshape(2, depth, members, per_owner).transpose(2, 1, 0, 3)
    arrived = lax.all_to_all(outgoing, ("ty", "within"), split_axis=0, concat_axis=0, tiled=True)
    runs = 4 * groups // 4
    if not paired:
        behind = arrived[:, 2 * rows :]
        number = jnp.arange(8)[:, None] % 2 == jnp.arange(2)
        behind = jnp.where(number[None, :, :, None, None], behind[:, :, None], 0.0)
        arrived = arrived[:, : 2 * rows].reshape(members, 2, rows, 2, per_owner).transpose(0, 2, 1, 3, 4)
        arrived = jnp.concatenate([arrived, behind], axis=1)
        arrived = arrived.reshape(-1, within, rows + 8, 2, 2, per_owner).transpose(4, 2, 0, 3, 1, 5)
        arrived = arrived.reshape(2, rows + 8, tile_count * per_owner)
    filtered = pl.pallas_call(
        functools.partial(filter_kernel, per_owner, paired, 2 * within),
        out_shape=jax.ShapeDtypeStruct((SAMPLES, runs, 8, LANES), f32),
        in_specs=whole(2),
        out_specs=pl.BlockSpec(memory_space=pltpu.HBM),
        scratch_shapes=[
            pltpu.VMEM((rows + 8, LANES), f32),
            pltpu.VMEM((runs, SAMPLES * 8, LANES), f32),
            pltpu.SemaphoreType.DMA((runs,)),
        ],
        cost_estimate=cost(2 * 3 * 80 * 80 * 8 * slots, 3000000),
        compiler_params=grant,
        name="filter_series",
    )(filter_matrix, arrived)
    filtered = filtered.reshape(SAMPLES, 4 * groups, 2, LANES)
    return filtered.transpose(2, 0, 1, 3).reshape(2, SAMPLES, 4 * slots)


def solution(mesh):
    lines, across = mesh.devices.shape
    halved = Mesh(mesh.devices.reshape(lines, 2, across // 2), ("ty", "half", "within"))
    tile = ("ty", "half", "within")
    placed = (
        P(None, None, "ty", ("half", "within")),
        P(None, tile),
        P(None, None, None, tile),
        P(None, None, tile),
        P(),
        P(tile, None),
        P(),
    )
    return jax.shard_map(
        run,
        mesh=halved,
        in_specs=placed,
        out_specs=P(None, None, tile),
        check_vma=False,
    )
```

```python
import functools

import jax
import jax.numpy as jnp
from jax import lax
from jax.experimental import pallas as pl
from jax.experimental.pallas import tpu as pltpu
from jax.sharding import Mesh
from jax.sharding import PartitionSpec as P


STEPS = 2
SAMPLES = 73
HISTORY = 71
MOST = 16


drift = 0.2
moves = ((-1, -1), (-1, 0), (-1, 1), (0, -1), (0, 1), (1, -1), (1, 0), (1, 1))
f32 = jnp.float32
bf16 = jnp.bfloat16
LANES = 128


def up(value, to):
    return -(-value // to) * to


places = {"ty": "ty", "tx": ("half", "within")}


def exchanged(up, down, axis):
    peers = lax.axis_size(places[axis])
    even = lax.axis_index(places[axis]) % 2 == 0
    near = [(i, i ^ 1) for i in range(peers)]
    far = [(i, (i - 1 if i % 2 == 0 else i + 1) % peers) for i in range(peers)]
    first = lax.ppermute(up if up is down else jnp.where(even, up, down), places[axis], near)
    second = lax.ppermute(up if up is down else jnp.where(even, down, up), places[axis], far)
    return jnp.where(even, second, first), jnp.where(even, first, second)


def swapped(value):
    return lax.ppermute(value, "half", [(0, 1), (1, 0)])


def halves(value):
    high = value.astype(bf16)
    return high, (value - high.astype(f32)).astype(bf16)


def picked(condition):
    return jnp.where(condition, 1.0, 0.0).astype(f32)


def iota(shape, dim):
    return lax.broadcasted_iota(jnp.int32, shape, dim)


def whole(count):
    return [pl.BlockSpec(memory_space=pltpu.VMEM) for _ in range(count)]


def cost(flops, moved):
    return pl.CostEstimate(flops=flops, bytes_accessed=moved, transcendentals=0)


grant = pltpu.CompilerParams(vmem_limit_bytes=16 * 1024 * 1024)


def sections_of(step, following):
    own = [(step, 0, 0)] if step == 0 else []
    own += [(step, 1, 1), (step, 2, 1), (step, 3, 2)]
    return own + ([(step + 1, 0, 2)] if following else [])


def at_time(read, step, table):
    if table == 1:
        return 0.5 * (read(step) + read(step + 1))
    return read(step + table // 2)


def side_by_side(value):
    return jnp.concatenate(halves(value), axis=1)


def doubled(value):
    return jnp.concatenate([value, value], axis=0)


def inner_kernel(step, following, velocity_ref, cells_ref, part_ref, cols_ref, rows_ref, table_ref):
    rows, cols = velocity_ref.shape[2], velocity_ref.shape[3]
    slots = cells_ref.shape[3]
    for table in range(3):
        for c in range(2):
            value = at_time(lambda a: velocity_ref[c, a], step, table)
            table_ref[table, c * rows : (c + 1) * rows] = side_by_side(value)
    col = iota((cols, slots), 0)
    row = iota((rows, slots), 0)
    for number, (k, section, table) in enumerate(sections_of(step, following)):
        cy, cx = cells_ref[k, section, 0:1], cells_ref[k, section, 1:2]
        across = [picked(row == cy), picked(row == cy + 1)]
        for v in range(2):
            rows_ref[number, v] = across[v].astype(bf16)
        values = {}
        for h in range(2):
            onehot = picked(col == cx + h).astype(bf16)
            cols_ref[number, h] = onehot
            product = jnp.dot(table_ref[table], doubled(onehot), preferred_element_type=f32)
            for c in range(2):
                for v in range(2):
                    kept = across[v] * product[c * rows : (c + 1) * rows]
                    values[v, h, c] = jnp.sum(kept, axis=0, keepdims=True)
        corners = [values[v, h, c] for v in range(2) for h in range(2) for c in range(2)]
        part_ref[number] = jnp.concatenate(corners, axis=0)


def bilinear(corners, point, cell):
    wy = point[0] - cell[0:1].astype(f32)
    wx = point[1] - cell[1:2].astype(f32)
    first, second, third, fourth = corners
    return [
        (1.0 - wy) * ((1.0 - wx) * first[c] + wx * second[c]) + wy * ((1.0 - wx) * third[c] + wx * fourth[c])
        for c in range(2)
    ]


def along(point, factor, speed):
    return [p + factor * s for p, s in zip(point, speed)]


def step_kernel(
    step, following, velocity_shape, part_ref, cols_ref, rows_ref, north_ref, south_ref, west_ref, east_ref, point_ref, cells_ref, *rest
):
    if step > 0:
        first_ref, rest = rest[0], rest[1:]
    if following:
        record_ref, lead_ref, next_ref = rest
    else:
        record_ref, lead_ref = rest
    count, rows, cols = velocity_shape
    base = 2 * HISTORY
    ends = ((north_ref, south_ref), (west_ref, east_ref))
    tables = []
    for pair in ends:
        lines = []
        for table in range(3):
            for c in range(2):
                for ref in pair:
                    lines.append(at_time(lambda a: ref[base + c * count + a : base + c * count + a + 1], step, table))
        lines.append(jnp.zeros((4, cols), f32))
        tables.append(side_by_side(jnp.concatenate(lines, axis=0)))

    def tip(table, c, v, h):
        ref, at = ends[1][h], base + (1 + v) * 2 * count + c * count
        lane = slice(cols - 1, cols) if h == 0 else slice(0, 1)
        return at_time(lambda a: ref[at + a : at + a + 1, lane], step, table)

    def corners_of(number):
        k, section, table = sections_of(step, following)[number]
        cy, cx = cells_ref[k, section, 0:1], cells_ref[k, section, 1:2]
        outside = ((cy < 0, cy + 1 >= rows), (cx < 0, cx + 1 >= cols))
        ends_of = [
            jnp.dot(tables[0], doubled(cols_ref[number, i]), preferred_element_type=f32) for i in range(2)
        ], [jnp.dot(tables[1], doubled(rows_ref[number, i]), preferred_element_type=f32) for i in range(2)]
        result = []
        for v in range(2):
            for h in range(2):
                pair = []
                for c in range(2):
                    value = part_ref[number, 4 * v + 2 * h + c : 4 * v + 2 * h + c + 1]
                    at = 4 * table + 2 * c
                    value += jnp.where(outside[0][v], ends_of[0][h][at + v : at + v + 1], 0.0)
                    value += jnp.where(outside[1][h], ends_of[1][v][at + h : at + h + 1], 0.0)
                    value += jnp.where(outside[0][v] & outside[1][h], tip(table, c, v, h), 0.0)
                    pair.append(value)
                result.append(pair)
        return result

    corners = [corners_of(number) for number in range(len(sections_of(step, following)))]
    sections = [cells_ref[step, s] for s in range(4)]
    if step > 0:
        given = [[first_ref[2 * i + c : 2 * i + c + 1] for c in range(2)] for i in range(4)]
        corners = [given] + corners
    point = [point_ref[0:1], point_ref[1:2]]
    k_one = bilinear(corners[0], point, sections[0])
    k_two = bilinear(corners[1], along(point, 0.5 * drift, k_one), sections[1])
    k_three = bilinear(corners[2], along(point, 0.5 * drift, k_two), sections[2])
    k_four = bilinear(corners[3], along(point, drift, k_three), sections[3])
    point = [
        p + drift / 6.0 * (a + 2.0 * b + 2.0 * c + d)
        for p, a, b, c, d in zip(point, k_one, k_two, k_three, k_four)
    ]
    blank = [jnp.zeros_like(point[0])] * 4
    record = jnp.concatenate(point + k_one + blank, axis=0)
    record_ref[...] = record
    band = step * 8 * MOST
    lead_ref[...] = record[:, band : band + 8 * MOST]
    if following:
        next_ref[...] = jnp.concatenate([value for corner in corners[4] for value in corner], axis=0)


def run_step(step, halo, point, first, cells):
    velocity, *ends = halo
    slots = point.shape[1]
    following = step + 1 < STEPS
    rows, cols = velocity.shape[2:]
    number = len(sections_of(step, following))
    inner = pl.pallas_call(
        functools.partial(inner_kernel, step, following),
        out_shape=[
            jax.ShapeDtypeStruct((number, 8, slots), f32),
            jax.ShapeDtypeStruct((number, 2, cols, slots), bf16),
            jax.ShapeDtypeStruct((number, 2, rows, slots), bf16),
        ],
        in_specs=whole(2),
        out_specs=whole(3),
        scratch_shapes=[pltpu.VMEM((3, 2 * rows, 2 * cols), bf16)],
        cost_estimate=cost(number * 2 * 2 * rows * 2 * cols * slots * 2, 600000),
        compiler_params=grant,
        name="sample_inner",
    )(velocity, cells)
    operands = (*inner, *ends, point, cells) + ((first,) if step > 0 else ())
    shape = jax.ShapeDtypeStruct((8, slots), f32)
    shapes = [shape, jax.ShapeDtypeStruct((8, 8 * MOST), f32)] + ([shape] if following else [])
    return pl.pallas_call(
        functools.partial(step_kernel, step, following, velocity.shape[1:]),
        out_shape=shapes,
        in_specs=whole(len(operands)),
        out_specs=whole(len(shapes)),
        cost_estimate=cost(number * 2 * 4 * 16 * 2 * cols * slots, 600000),
        compiler_params=grant,
        name="sample_step",
    )(*operands)


def sides_kernel(leavers_ref, sides_ref):
    slot = iota((1, 8 * MOST), 1)
    for step in range(leavers_ref.shape[0]):
        rows = [jnp.zeros((1, 8 * MOST), f32) for _ in range(2)]
        start = 0
        for j in range(8):
            end = start + leavers_ref[step, j]
            inside = (slot >= start) & (slot < end)
            rows = [jnp.where(inside, float(moves[j][axis]), rows[axis]) for axis in range(2)]
            start = end
        sides_ref[step] = jnp.concatenate(rows + [jnp.zeros((6, 8 * MOST), f32)], axis=0)


def find_sides(leavers):
    return pl.pallas_call(
        sides_kernel,
        out_shape=jax.ShapeDtypeStruct((leavers.shape[0], 8, 8 * MOST), f32),
        in_specs=[pl.BlockSpec(memory_space=pltpu.SMEM)],
        out_specs=whole(1)[0],
        compiler_params=grant,
        cost_estimate=cost(100000, 5000),
        name="find_sides",
    )(leavers)


def chosen(side, value, forward, backward):
    return jnp.where(side > 0.0, forward, jnp.where(side < 0.0, backward, value))


def paired_halves(first, second, width):
    lane = iota(first.shape, 1)
    left = jnp.where(lane < width, first, pltpu.roll(second, width, 1))
    right = jnp.where(lane < width, pltpu.roll(first, width, 1), second)
    return left, right


def columns_kernel(width, owner_ref, out_ref):
    owner_row = owner_ref[...]
    slots = owner_row.shape[1]
    owner = jnp.broadcast_to(owner_row, (LANES, slots)).T[:, 0:1]
    before = iota((slots, slots), 0) < iota((slots, slots), 1)
    rank = jnp.sum(picked((owner == owner_row) & before), axis=0, keepdims=True)
    out_ref[...] = owner_row * width + rank


def targets_of(columns, half, within, width):
    slots = columns.shape[1]
    half = half.astype(f32)
    owner = jnp.floor((columns + 0.5) / width)
    column = jnp.floor((owner + 0.5) / within)
    line = jnp.floor((column + 0.5) * 0.5)
    block = line * within + (owner - column * within)
    target = jnp.where(column - 2.0 * line == half, block * width + (columns - owner * width), -1.0)
    return jnp.broadcast_to(target, (LANES, slots)).T[:, 0:1].astype(jnp.int32)


def place_history_kernel(width, paired, within, skipped, half_ref, owner_ref, history_ref, past_ref, out_ref, onehot_ref):
    slots = owner_ref.shape[1]
    rows = up(HISTORY, 8)
    groups = slots // LANES
    moving = 8 * MOST // LANES
    total = onehot_ref.shape[1]
    target = targets_of(owner_ref[...], half_ref[0], within, width)
    parts = []
    for c in range(2):
        pieces = [past_ref[pl.ds(c, HISTORY, stride=2), :]]
        for g in range(moving, groups):
            pieces.append(history_ref[pl.ds(2 * (g - skipped) + c, HISTORY, stride=2 * (groups - skipped)), :])
        parts += [jnp.concatenate(pieces, axis=1), jnp.zeros((rows - HISTORY, slots), f32)]
    joined = jnp.concatenate(halves(jnp.concatenate(parts, axis=0)), axis=0)
    chunk = 256
    for start in range(0, total, chunk):
        onehot = picked(target == start + iota((slots, chunk), 1)).astype(bf16)
        onehot_ref[:, start : start + chunk] = onehot
        product = jnp.dot(joined, onehot, preferred_element_type=f32)
        placed = product[: 2 * rows] + product[2 * rows :]
        if paired:
            for at in range(0, chunk, LANES):
                pair = paired_halves(placed[:rows, at : at + LANES], placed[rows:, at : at + LANES], width)
                for i in range(2):
                    out_ref[(start + at) // width + i] = pair[i]
        else:
            out_ref[0, :, start : start + chunk] = placed[:rows]
            out_ref[1, :, start : start + chunk] = placed[rows:]


def place_samples_kernel(
    width, paired, half_ref, samples_ref, far_samples_ref, onehot_ref, far_onehot_ref, placed_ref, far_placed_ref, out_ref
):
    half = half_ref[0]
    rows = up(HISTORY, 8)
    total = onehot_ref.shape[1]
    chunk = 256
    row = iota((8, LANES), 0)
    wide = iota((8, chunk), 0)
    tiles = (
        (half, samples_ref, onehot_ref, placed_ref),
        (1 - half, far_samples_ref, far_onehot_ref, far_placed_ref),
    )
    lefts = []
    for number, samples, _, _ in tiles:
        columns = []
        for c in range(2):
            early, late = samples[2 * c : 2 * c + 1], samples[2 * c + 1 : 2 * c + 2]
            at = iota((8, early.shape[1]), 0)
            columns.append(jnp.where(at == number, early, jnp.where(at == number + 2, late, 0.0)))
        lefts.append(jnp.concatenate(halves(jnp.concatenate(columns, axis=0)), axis=0))
    for start in range(0, total, chunk):
        span = slice(start, start + chunk)
        values = None
        for left, (_, _, onehot, _) in zip(lefts, tiles):
            product = jnp.dot(left, onehot[:, span], preferred_element_type=f32)
            value = product[:16] + product[16:]
            values = value if values is None else values + value
        if paired:
            for at in range(0, chunk, LANES):
                pair = paired_halves(values[:8, at : at + LANES], values[8:, at : at + LANES], width)
                for i in range(2):
                    block = (start + at) // width + i
                    for number, _, _, placed in tiles:
                        out_ref[block, pl.ds(pl.multiple_of(number * rows, 8), rows), :] = placed[block]
                    out_ref[block, 2 * rows : 2 * rows + 8] = pair[i]
        else:
            for c in range(2):
                for number, _, _, placed in tiles:
                    out_ref[c, pl.ds(pl.multiple_of(number * rows, 8), rows), span] = placed[c, :, span]
                out_ref[c, 2 * rows : 2 * rows + 8, span] = values[8 * c : 8 * c + 8]


def filter_kernel(width, paired, across, matrix_ref, arrived_ref, out_ref, wide_ref, ready_ref, sems):
    depth = wide_ref.shape[0]
    rows = depth - 8
    samples = matrix_ref.shape[0]
    groups = out_ref.shape[2] // 2
    row = iota((8, LANES), 0)
    wide_ref[...] = jnp.zeros_like(wide_ref)
    wide_ref[0:samples, 0:HISTORY] = matrix_ref[:, 0:HISTORY]
    for late in range(STEPS):
        for number in range(2):
            at = rows + 2 * late + number
            wide_ref[0:samples, at : at + 1] = matrix_ref[:, HISTORY + late : HISTORY + late + 1]
    high, low = halves(wide_ref[:, 0:depth])
    left = jnp.concatenate([high, low, high], axis=1)

    def block_of(tile):
        line, column = tile // across, tile % across
        number, column = column // (across // 2), column % (across // 2)
        block = line * (across // 2) + column
        behind = jnp.where((row == number) | (row == number + 2), arrived_ref[block, 2 * rows : 2 * rows + 8], 0.0)
        return jnp.concatenate([arrived_ref[block, number * rows : (number + 1) * rows], behind], axis=0)

    copies = []
    for run in range(out_ref.shape[1]):
        start = run * groups * LANES
        if paired:
            spots = range(start // width, (start + groups * LANES) // width, 2)
            tiles = [paired_halves(block_of(at), block_of(at + 1), width) for at in spots]
            columns = [jnp.concatenate([t[c] for t in tiles], axis=1) for c in range(2)]
        else:
            columns = [arrived_ref[c, :, start : start + groups * LANES] for c in range(2)]
        for c in range(2):
            x_high, x_low = halves(columns[c])
            right = jnp.concatenate([x_high, x_high, x_low], axis=0)
            product = jnp.dot(left, right, preferred_element_type=f32)
            for g in range(groups):
                target = pl.ds(2 * g + c, samples, stride=2 * groups)
                ready_ref[run, target, :] = product[:samples, g * LANES : (g + 1) * LANES]
        source = ready_ref.at[run].reshape(samples, 2 * groups, LANES)
        copies.append(pltpu.make_async_copy(source, out_ref.at[:, run], sems.at[run]))
        copies[-1].start()
    for copy in copies:
        copy.wait()


def run(velocity, start_position, cells, history, leavers, owner, filter_matrix):
    tile_rows = velocity.shape[2]
    tile_cols = velocity.shape[3]
    slots = start_position.shape[1]
    within = lax.axis_size("within")
    members = lax.axis_size("ty") * within
    tile_count = 2 * members
    per_owner = 4 * slots // tile_count
    paired = 2 * per_owner == LANES
    groups = slots // LANES
    lines = 2 * HISTORY
    by_rows = history.reshape(2, HISTORY, groups, LANES).transpose(1, 2, 0, 3)
    raw = by_rows.reshape(2 * groups * HISTORY, LANES)
    past = by_rows[:, 0].reshape(lines, LANES)
    sides = find_sides(leavers)

    def joined(*parts):
        return jnp.concatenate([part.reshape(-1, LANES) for part in parts], axis=0)

    north, south = exchanged(joined(past, velocity[:, :, tile_rows - 1]), joined(past, velocity[:, :, 0]), "ty")
    past = chosen(sides[0, 0:1], past, north[:lines], south[:lines])
    west, east = exchanged(
        joined(past, velocity[:, :, :, tile_cols - 1], north[lines:], south[lines:]),
        joined(past, velocity[:, :, :, 0], north[lines:], south[lines:]),
        "tx",
    )
    past = chosen(sides[0, 1:2], past, west[:lines], east[:lines])
    halo = (velocity, north, south, west, east)
    owner = pl.pallas_call(
        functools.partial(columns_kernel, per_owner),
        out_shape=jax.ShapeDtypeStruct((1, slots), f32),
        in_specs=whole(1),
        out_specs=whole(1)[0],
        cost_estimate=cost(1000000, 10000),
        compiler_params=grant,
        name="find_columns",
    )(owner.astype(f32).reshape(1, slots))
    past = joined(past, owner, jnp.zeros((2, LANES), f32))
    moving = 8 * MOST // LANES
    far_raw = swapped(by_rows[:, moving:].reshape(2 * (groups - moving) * HISTORY, LANES))
    far_past = swapped(past)
    far_owner = far_past[lines : lines + groups].reshape(1, slots)
    half = lax.axis_index("half").reshape(1)
    record, lead, first = run_step(0, halo, start_position, None, cells)
    lead = chosen(sides[0, 0:1], lead, *exchanged(lead, lead, "ty"))
    lead_west, lead_east = exchanged(lead, lead, "tx")
    rows = up(HISTORY, 8)
    scalar = [pl.BlockSpec(memory_space=pltpu.SMEM)]
    span = members * per_owner
    shape = (members, rows, LANES) if paired else (2, rows, span)

    def place(owner, raw, past, skipped):
        return pl.pallas_call(
            functools.partial(place_history_kernel, per_owner, paired, within, skipped),
            out_shape=[jax.ShapeDtypeStruct(shape, f32), jax.ShapeDtypeStruct((slots, span), bf16)],
            in_specs=scalar + whole(3),
            out_specs=whole(2),
            cost_estimate=cost(2 * 4 * rows * slots * span, 3000000),
            compiler_params=grant,
            name="place_history",
        )(half, owner, raw, past)

    placed, onehot = place(owner.reshape(1, slots), raw, past, 0)
    far_placed, far_onehot = place(far_owner, far_raw, far_past, moving)
    lead = chosen(sides[0, 1:2], lead, lead_west, lead_east)
    lowered = [sides[0, 0:1] * tile_rows, sides[0, 1:2] * tile_cols, jnp.zeros((6, 8 * MOST), f32)]
    record = jnp.concatenate([lead - jnp.concatenate(lowered, axis=0), record[:, 8 * MOST :]], axis=1)
    point = record[0:2]
    corners = [[first[2 * i + c : 2 * i + c + 1] for c in range(2)] for i in range(4)]
    last = bilinear(corners, [record[0:1], record[1:2]], cells[STEPS - 1, 0])
    samples = jnp.concatenate([record[2:3], last[0], record[3:4], last[1]], axis=0)
    run_step(STEPS - 1, halo, point, first, cells)
    far_samples = swapped(samples)
    depth = 2 * rows + 8
    outgoing = pl.pallas_call(
        functools.partial(place_samples_kernel, per_owner, paired),
        out_shape=jax.ShapeDtypeStruct((members, depth, LANES) if paired else (2, depth, span), f32),
        in_specs=scalar + whole(6),
        out_specs=whole(1)[0],
        cost_estimate=cost(2 * 2 * 32 * slots * span, 3000000),
        compiler_params=grant,
        name="place_samples",
    )(half, samples, far_samples, onehot, far_onehot, placed, far_placed)
    if not paired:
        outgoing = outgoing.reshape(2, depth, members, per_owner).transpose(2, 1, 0, 3)
    arrived = lax.all_to_all(outgoing, ("ty", "within"), split_axis=0, concat_axis=0, tiled=True)
    runs = 4 * groups // 4
    if not paired:
        behind = arrived[:, 2 * rows :]
        number = jnp.arange(8)[:, None] % 2 == jnp.arange(2)
        behind = jnp.where(number[None, :, :, None, None], behind[:, :, None], 0.0)
        arrived = arrived[:, : 2 * rows].reshape(members, 2, rows, 2, per_owner).transpose(0, 2, 1, 3, 4)
        arrived = jnp.concatenate([arrived, behind], axis=1)
        arrived = arrived.reshape(-1, within, rows + 8, 2, 2, per_owner).transpose(4, 2, 0, 3, 1, 5)
        arrived = arrived.reshape(2, rows + 8, tile_count * per_owner)
    filtered = pl.pallas_call(
        functools.partial(filter_kernel, per_owner, paired, 2 * within),
        out_shape=jax.ShapeDtypeStruct((SAMPLES, runs, 8, LANES), f32),
        in_specs=whole(2),
        out_specs=pl.BlockSpec(memory_space=pltpu.HBM),
        scratch_shapes=[
            pltpu.VMEM((rows + 8, LANES), f32),
            pltpu.VMEM((runs, SAMPLES * 8, LANES), f32),
            pltpu.SemaphoreType.DMA((runs,)),
        ],
        cost_estimate=cost(2 * 3 * 80 * 80 * 8 * slots, 3000000),
        compiler_params=grant,
        name="filter_series",
    )(filter_matrix, arrived)
    filtered = filtered.reshape(SAMPLES, 4 * groups, 2, LANES)
    return filtered.transpose(2, 0, 1, 3).reshape(2, SAMPLES, 4 * slots)


def solution(mesh):
    lines, across = mesh.devices.shape
    halved = Mesh(mesh.devices.reshape(lines, 2, across // 2), ("ty", "half", "within"))
    tile = ("ty", "half", "within")
    placed = (
        P(None, None, "ty", ("half", "within")),
        P(None, tile),
        P(None, None, None, tile),
        P(None, None, tile),
        P(),
        P(tile, None),
        P(),
    )
    return jax.shard_map(
        run,
        mesh=halved,
        in_specs=placed,
        out_specs=P(None, None, tile),
        check_vma=False,
    )
```

```python
import functools

import jax
import jax.numpy as jnp
from jax import lax
from jax.experimental import pallas as pl
from jax.experimental.pallas import tpu as pltpu
from jax.sharding import Mesh
from jax.sharding import PartitionSpec as P


STEPS = 2
SAMPLES = 73
HISTORY = 71
MOST = 16


drift = 0.2
moves = ((-1, -1), (-1, 0), (-1, 1), (0, -1), (0, 1), (1, -1), (1, 0), (1, 1))
f32 = jnp.float32
bf16 = jnp.bfloat16
LANES = 128


def up(value, to):
    return -(-value // to) * to


places = {"ty": "ty", "tx": ("half", "within")}


def exchanged(up, down, axis):
    peers = lax.axis_size(places[axis])
    even = lax.axis_index(places[axis]) % 2 == 0
    near = [(i, i ^ 1) for i in range(peers)]
    far = [(i, (i - 1 if i % 2 == 0 else i + 1) % peers) for i in range(peers)]
    first = lax.ppermute(up if up is down else jnp.where(even, up, down), places[axis], near)
    second = lax.ppermute(up if up is down else jnp.where(even, down, up), places[axis], far)
    return jnp.where(even, second, first), jnp.where(even, first, second)


def swapped(value):
    return lax.ppermute(value, "half", [(0, 1), (1, 0)])


def halves(value):
    high = value.astype(bf16)
    return high, (value - high.astype(f32)).astype(bf16)


def picked(condition):
    return jnp.where(condition, 1.0, 0.0).astype(f32)


def iota(shape, dim):
    return lax.broadcasted_iota(jnp.int32, shape, dim)


def whole(count):
    return [pl.BlockSpec(memory_space=pltpu.VMEM) for _ in range(count)]


def cost(flops, moved):
    return pl.CostEstimate(flops=flops, bytes_accessed=moved, transcendentals=0)


grant = pltpu.CompilerParams(vmem_limit_bytes=16 * 1024 * 1024)


def sections_of(step, following):
    own = [(step, 0, 0)] if step == 0 else []
    own += [(step, 1, 1), (step, 2, 1), (step, 3, 2)]
    return own + ([(step + 1, 0, 2)] if following else [])


def at_time(read, step, table):
    if table == 1:
        return 0.5 * (read(step) + read(step + 1))
    return read(step + table // 2)


def side_by_side(value):
    return jnp.concatenate(halves(value), axis=1)


def doubled(value):
    return jnp.concatenate([value, value], axis=0)


def inner_kernel(step, following, velocity_ref, cells_ref, part_ref, cols_ref, rows_ref, table_ref):
    rows, cols = velocity_ref.shape[2], velocity_ref.shape[3]
    slots = cells_ref.shape[3]
    for table in range(3):
        for c in range(2):
            value = at_time(lambda a: velocity_ref[c, a], step, table)
            table_ref[table, c * rows : (c + 1) * rows] = side_by_side(value)
    col = iota((cols, slots), 0)
    row = iota((rows, slots), 0)
    for number, (k, section, table) in enumerate(sections_of(step, following)):
        cy, cx = cells_ref[k, section, 0:1], cells_ref[k, section, 1:2]
        across = [picked(row == cy), picked(row == cy + 1)]
        for v in range(2):
            rows_ref[number, v] = across[v].astype(bf16)
        values = {}
        for h in range(2):
            onehot = picked(col == cx + h).astype(bf16)
            cols_ref[number, h] = onehot
            product = jnp.dot(table_ref[table], doubled(onehot), preferred_element_type=f32)
            for c in range(2):
                for v in range(2):
                    kept = across[v] * product[c * rows : (c + 1) * rows]
                    values[v, h, c] = jnp.sum(kept, axis=0, keepdims=True)
        corners = [values[v, h, c] for v in range(2) for h in range(2) for c in range(2)]
        part_ref[number] = jnp.concatenate(corners, axis=0)


def bilinear(corners, point, cell):
    wy = point[0] - cell[0:1].astype(f32)
    wx = point[1] - cell[1:2].astype(f32)
    first, second, third, fourth = corners
    return [
        (1.0 - wy) * ((1.0 - wx) * first[c] + wx * second[c]) + wy * ((1.0 - wx) * third[c] + wx * fourth[c])
        for c in range(2)
    ]


def along(point, factor, speed):
    return [p + factor * s for p, s in zip(point, speed)]


def step_kernel(
    step, following, velocity_shape, part_ref, cols_ref, rows_ref, north_ref, south_ref, west_ref, east_ref, point_ref, cells_ref, *rest
):
    if step > 0:
        first_ref, rest = rest[0], rest[1:]
    if following:
        record_ref, lead_ref, next_ref = rest
    else:
        record_ref, lead_ref = rest
    count, rows, cols = velocity_shape
    base = 2 * HISTORY
    ends = ((north_ref, south_ref), (west_ref, east_ref))
    tables = []
    for pair in ends:
        lines = []
        for table in range(3):
            for c in range(2):
                for ref in pair:
                    lines.append(at_time(lambda a: ref[base + c * count + a : base + c * count + a + 1], step, table))
        lines.append(jnp.zeros((4, cols), f32))
        tables.append(side_by_side(jnp.concatenate(lines, axis=0)))

    def tip(table, c, v, h):
        ref, at = ends[1][h], base + (1 + v) * 2 * count + c * count
        lane = slice(cols - 1, cols) if h == 0 else slice(0, 1)
        return at_time(lambda a: ref[at + a : at + a + 1, lane], step, table)

    def corners_of(number):
        k, section, table = sections_of(step, following)[number]
        cy, cx = cells_ref[k, section, 0:1], cells_ref[k, section, 1:2]
        outside = ((cy < 0, cy + 1 >= rows), (cx < 0, cx + 1 >= cols))
        ends_of = [
            jnp.dot(tables[0], doubled(cols_ref[number, i]), preferred_element_type=f32) for i in range(2)
        ], [jnp.dot(tables[1], doubled(rows_ref[number, i]), preferred_element_type=f32) for i in range(2)]
        result = []
        for v in range(2):
            for h in range(2):
                pair = []
                for c in range(2):
                    value = part_ref[number, 4 * v + 2 * h + c : 4 * v + 2 * h + c + 1]
                    at = 4 * table + 2 * c
                    value += jnp.where(outside[0][v], ends_of[0][h][at + v : at + v + 1], 0.0)
                    value += jnp.where(outside[1][h], ends_of[1][v][at + h : at + h + 1], 0.0)
                    value += jnp.where(outside[0][v] & outside[1][h], tip(table, c, v, h), 0.0)
                    pair.append(value)
                result.append(pair)
        return result

    corners = [corners_of(number) for number in range(len(sections_of(step, following)))]
    sections = [cells_ref[step, s] for s in range(4)]
    if step > 0:
        given = [[first_ref[2 * i + c : 2 * i + c + 1] for c in range(2)] for i in range(4)]
        corners = [given] + corners
    point = [point_ref[0:1], point_ref[1:2]]
    k_one = bilinear(corners[0], point, sections[0])
    k_two = bilinear(corners[1], along(point, 0.5 * drift, k_one), sections[1])
    k_three = bilinear(corners[2], along(point, 0.5 * drift, k_two), sections[2])
    k_four = bilinear(corners[3], along(point, drift, k_three), sections[3])
    point = [
        p + drift / 6.0 * (a + 2.0 * b + 2.0 * c + d)
        for p, a, b, c, d in zip(point, k_one, k_two, k_three, k_four)
    ]
    blank = [jnp.zeros_like(point[0])] * 4
    record = jnp.concatenate(point + k_one + blank, axis=0)
    record_ref[...] = record
    band = step * 8 * MOST
    lead_ref[...] = record[:, band : band + 8 * MOST]
    if following:
        next_ref[...] = jnp.concatenate([value for corner in corners[4] for value in corner], axis=0)


def run_step(step, halo, point, first, cells):
    velocity, *ends = halo
    slots = point.shape[1]
    following = step + 1 < STEPS
    rows, cols = velocity.shape[2:]
    number = len(sections_of(step, following))
    inner = pl.pallas_call(
        functools.partial(inner_kernel, step, following),
        out_shape=[
            jax.ShapeDtypeStruct((number, 8, slots), f32),
            jax.ShapeDtypeStruct((number, 2, cols, slots), bf16),
            jax.ShapeDtypeStruct((number, 2, rows, slots), bf16),
        ],
        in_specs=whole(2),
        out_specs=whole(3),
        scratch_shapes=[pltpu.VMEM((3, 2 * rows, 2 * cols), bf16)],
        cost_estimate=cost(number * 2 * 2 * rows * 2 * cols * slots * 2, 600000),
        compiler_params=grant,
        name="sample_inner",
    )(velocity, cells)
    operands = (*inner, *ends, point, cells) + ((first,) if step > 0 else ())
    shape = jax.ShapeDtypeStruct((8, slots), f32)
    shapes = [shape, jax.ShapeDtypeStruct((8, 8 * MOST), f32)] + ([shape] if following else [])
    return pl.pallas_call(
        functools.partial(step_kernel, step, following, velocity.shape[1:]),
        out_shape=shapes,
        in_specs=whole(len(operands)),
        out_specs=whole(len(shapes)),
        cost_estimate=cost(number * 2 * 4 * 16 * 2 * cols * slots, 600000),
        compiler_params=grant,
        name="sample_step",
    )(*operands)


def sides_kernel(leavers_ref, sides_ref):
    slot = iota((1, 8 * MOST), 1)
    for step in range(leavers_ref.shape[0]):
        rows = [jnp.zeros((1, 8 * MOST), f32) for _ in range(2)]
        start = 0
        for j in range(8):
            end = start + leavers_ref[step, j]
            inside = (slot >= start) & (slot < end)
            rows = [jnp.where(inside, float(moves[j][axis]), rows[axis]) for axis in range(2)]
            start = end
        sides_ref[step] = jnp.concatenate(rows + [jnp.zeros((6, 8 * MOST), f32)], axis=0)


def find_sides(leavers):
    return pl.pallas_call(
        sides_kernel,
        out_shape=jax.ShapeDtypeStruct((leavers.shape[0], 8, 8 * MOST), f32),
        in_specs=[pl.BlockSpec(memory_space=pltpu.SMEM)],
        out_specs=whole(1)[0],
        compiler_params=grant,
        cost_estimate=cost(100000, 5000),
        name="find_sides",
    )(leavers)


def chosen(side, value, forward, backward):
    return jnp.where(side > 0.0, forward, jnp.where(side < 0.0, backward, value))


def paired_halves(first, second, width):
    lane = iota(first.shape, 1)
    left = jnp.where(lane < width, first, pltpu.roll(second, width, 1))
    right = jnp.where(lane < width, pltpu.roll(first, width, 1), second)
    return left, right


def columns_kernel(width, owner_ref, out_ref):
    owner_row = owner_ref[...]
    slots = owner_row.shape[1]
    owner = jnp.broadcast_to(owner_row, (LANES, slots)).T[:, 0:1]
    before = iota((slots, slots), 0) < iota((slots, slots), 1)
    rank = jnp.sum(picked((owner == owner_row) & before), axis=0, keepdims=True)
    out_ref[...] = owner_row * width + rank


def targets_of(columns, half, within, width):
    slots = columns.shape[1]
    half = half.astype(f32)
    owner = jnp.floor((columns + 0.5) / width)
    column = jnp.floor((owner + 0.5) / within)
    line = jnp.floor((column + 0.5) * 0.5)
    block = line * within + (owner - column * within)
    target = jnp.where(column - 2.0 * line == half, block * width + (columns - owner * width), -1.0)
    return jnp.broadcast_to(target, (LANES, slots)).T[:, 0:1].astype(jnp.int32)


def place_history_kernel(width, paired, within, skipped, half_ref, owner_ref, history_ref, past_ref, out_ref, onehot_ref):
    slots = owner_ref.shape[1]
    rows = up(HISTORY, 8)
    groups = slots // LANES
    moving = 8 * MOST // LANES
    total = onehot_ref.shape[1]
    target = targets_of(owner_ref[...], half_ref[0], within, width)
    parts = []
    for c in range(2):
        pieces = [past_ref[pl.ds(c, HISTORY, stride=2), :]]
        for g in range(moving, groups):
            pieces.append(history_ref[pl.ds(2 * (g - skipped) + c, HISTORY, stride=2 * (groups - skipped)), :])
        parts += [jnp.concatenate(pieces, axis=1), jnp.zeros((rows - HISTORY, slots), f32)]
    joined = jnp.concatenate(halves(jnp.concatenate(parts, axis=0)), axis=0)
    chunk = 256
    for start in range(0, total, chunk):
        onehot = picked(target == start + iota((slots, chunk), 1)).astype(bf16)
        onehot_ref[:, start : start + chunk] = onehot
        product = jnp.dot(joined, onehot, preferred_element_type=f32)
        placed = product[: 2 * rows] + product[2 * rows :]
        if paired:
            for at in range(0, chunk, LANES):
                pair = paired_halves(placed[:rows, at : at + LANES], placed[rows:, at : at + LANES], width)
                for i in range(2):
                    out_ref[(start + at) // width + i] = pair[i]
        else:
            out_ref[0, :, start : start + chunk] = placed[:rows]
            out_ref[1, :, start : start + chunk] = placed[rows:]


def place_samples_kernel(
    width, paired, half_ref, samples_ref, far_samples_ref, onehot_ref, far_onehot_ref, placed_ref, far_placed_ref, out_ref
):
    half = half_ref[0]
    rows = up(HISTORY, 8)
    total = onehot_ref.shape[1]
    chunk = 256
    row = iota((8, LANES), 0)
    wide = iota((8, chunk), 0)
    tiles = (
        (half, samples_ref, onehot_ref, placed_ref),
        (1 - half, far_samples_ref, far_onehot_ref, far_placed_ref),
    )
    lefts = []
    for number, samples, _, _ in tiles:
        columns = []
        for c in range(2):
            early, late = samples[2 * c : 2 * c + 1], samples[2 * c + 1 : 2 * c + 2]
            at = iota((8, early.shape[1]), 0)
            columns.append(jnp.where(at == number, early, jnp.where(at == number + 2, late, 0.0)))
        lefts.append(jnp.concatenate(halves(jnp.concatenate(columns, axis=0)), axis=0))
    for start in range(0, total, chunk):
        span = slice(start, start + chunk)
        values = None
        for left, (_, _, onehot, _) in zip(lefts, tiles):
            product = jnp.dot(left, onehot[:, span], preferred_element_type=f32)
            value = product[:16] + product[16:]
            values = value if values is None else values + value
        if paired:
            for at in range(0, chunk, LANES):
                pair = paired_halves(values[:8, at : at + LANES], values[8:, at : at + LANES], width)
                for i in range(2):
                    block = (start + at) // width + i
                    for number, _, _, placed in tiles:
                        out_ref[block, pl.ds(pl.multiple_of(number * rows, 8), rows), :] = placed[block]
                    out_ref[block, 2 * rows : 2 * rows + 8] = pair[i]
        else:
            for c in range(2):
                for number, _, _, placed in tiles:
                    out_ref[c, pl.ds(pl.multiple_of(number * rows, 8), rows), span] = placed[c, :, span]
                out_ref[c, 2 * rows : 2 * rows + 8, span] = values[8 * c : 8 * c + 8]


def split_matrix_kernel(rows, matrix_ref, out_ref, wide_ref):
    samples = matrix_ref.shape[0]
    wide_ref[...] = jnp.zeros_like(wide_ref)
    wide_ref[0:samples, 0:HISTORY] = matrix_ref[:, 0:HISTORY]
    for late in range(STEPS):
        for number in range(2):
            at = rows + 2 * late + number
            wide_ref[0:samples, at : at + 1] = matrix_ref[:, HISTORY + late : HISTORY + late + 1]
    high, low = halves(wide_ref[:, 0 : rows + 8])
    out_ref[...] = jnp.concatenate([high, low, high], axis=1)


def filter_kernel(width, paired, across, matrix_ref, arrived_ref, out_ref, ready_ref, sems):
    rows = matrix_ref.shape[0] - 8
    samples = out_ref.shape[0]
    groups = out_ref.shape[2] // 2
    row = iota((8, LANES), 0)
    left = matrix_ref[...]

    def block_of(tile):
        line, column = tile // across, tile % across
        number, column = column // (across // 2), column % (across // 2)
        block = line * (across // 2) + column
        behind = jnp.where((row == number) | (row == number + 2), arrived_ref[block, 2 * rows : 2 * rows + 8], 0.0)
        return jnp.concatenate([arrived_ref[block, number * rows : (number + 1) * rows], behind], axis=0)

    copies = []
    for run in range(out_ref.shape[1]):
        start = run * groups * LANES
        if paired:
            spots = range(start // width, (start + groups * LANES) // width, 2)
            tiles = [paired_halves(block_of(at), block_of(at + 1), width) for at in spots]
            columns = [jnp.concatenate([t[c] for t in tiles], axis=1) for c in range(2)]
        else:
            columns = [arrived_ref[c, :, start : start + groups * LANES] for c in range(2)]
        for c in range(2):
            x_high, x_low = halves(columns[c])
            right = jnp.concatenate([x_high, x_high, x_low], axis=0)
            product = jnp.dot(left, right, preferred_element_type=f32)
            for g in range(groups):
                target = pl.ds(2 * g + c, samples, stride=2 * groups)
                ready_ref[run, target, :] = product[:samples, g * LANES : (g + 1) * LANES]
        source = ready_ref.at[run].reshape(samples, 2 * groups, LANES)
        copies.append(pltpu.make_async_copy(source, out_ref.at[:, run], sems.at[run]))
        copies[-1].start()
    for copy in copies:
        copy.wait()


def run(velocity, start_position, cells, history, leavers, owner, filter_matrix):
    tile_rows = velocity.shape[2]
    tile_cols = velocity.shape[3]
    slots = start_position.shape[1]
    within = lax.axis_size("within")
    members = lax.axis_size("ty") * within
    tile_count = 2 * members
    per_owner = 4 * slots // tile_count
    paired = 2 * per_owner == LANES
    groups = slots // LANES
    lines = 2 * HISTORY
    by_rows = history.reshape(2, HISTORY, groups, LANES).transpose(1, 2, 0, 3)
    raw = by_rows.reshape(2 * groups * HISTORY, LANES)
    past = by_rows[:, 0].reshape(lines, LANES)
    sides = find_sides(leavers)

    def joined(*parts):
        return jnp.concatenate([part.reshape(-1, LANES) for part in parts], axis=0)

    north, south = exchanged(joined(past, velocity[:, :, tile_rows - 1]), joined(past, velocity[:, :, 0]), "ty")
    past = chosen(sides[0, 0:1], past, north[:lines], south[:lines])
    west, east = exchanged(
        joined(past, velocity[:, :, :, tile_cols - 1], north[lines:], south[lines:]),
        joined(past, velocity[:, :, :, 0], north[lines:], south[lines:]),
        "tx",
    )
    past = chosen(sides[0, 1:2], past, west[:lines], east[:lines])
    halo = (velocity, north, south, west, east)
    owner = pl.pallas_call(
        functools.partial(columns_kernel, per_owner),
        out_shape=jax.ShapeDtypeStruct((1, slots), f32),
        in_specs=whole(1),
        out_specs=whole(1)[0],
        cost_estimate=cost(1000000, 10000),
        compiler_params=grant,
        name="find_columns",
    )(owner.astype(f32).reshape(1, slots))
    past = joined(past, owner, jnp.zeros((2, LANES), f32))
    moving = 8 * MOST // LANES
    far_raw = swapped(by_rows[:, moving:].reshape(2 * (groups - moving) * HISTORY, LANES))
    far_past = swapped(past)
    far_owner = far_past[lines : lines + groups].reshape(1, slots)
    half = lax.axis_index("half").reshape(1)
    record, lead, first = run_step(0, halo, start_position, None, cells)
    lead = chosen(sides[0, 0:1], lead, *exchanged(lead, lead, "ty"))
    lead_west, lead_east = exchanged(lead, lead, "tx")
    rows = up(HISTORY, 8)
    scalar = [pl.BlockSpec(memory_space=pltpu.SMEM)]
    span = members * per_owner
    shape = (members, rows, LANES) if paired else (2, rows, span)

    def place(owner, raw, past, skipped):
        return pl.pallas_call(
            functools.partial(place_history_kernel, per_owner, paired, within, skipped),
            out_shape=[jax.ShapeDtypeStruct(shape, f32), jax.ShapeDtypeStruct((slots, span), bf16)],
            in_specs=scalar + whole(3),
            out_specs=whole(2),
            cost_estimate=cost(2 * 4 * rows * slots * span, 3000000),
            compiler_params=grant,
            name="place_history",
        )(half, owner, raw, past)

    placed, onehot = place(owner.reshape(1, slots), raw, past, 0)
    far_placed, far_onehot = place(far_owner, far_raw, far_past, moving)
    lead = chosen(sides[0, 1:2], lead, lead_west, lead_east)
    lowered = [sides[0, 0:1] * tile_rows, sides[0, 1:2] * tile_cols, jnp.zeros((6, 8 * MOST), f32)]
    record = jnp.concatenate([lead - jnp.concatenate(lowered, axis=0), record[:, 8 * MOST :]], axis=1)
    point = record[0:2]
    corners = [[first[2 * i + c : 2 * i + c + 1] for c in range(2)] for i in range(4)]
    last = bilinear(corners, [record[0:1], record[1:2]], cells[STEPS - 1, 0])
    samples = jnp.concatenate([record[2:3], last[0], record[3:4], last[1]], axis=0)
    run_step(STEPS - 1, halo, point, first, cells)
    far_samples = swapped(samples)
    depth = 2 * rows + 8
    outgoing = pl.pallas_call(
        functools.partial(place_samples_kernel, per_owner, paired),
        out_shape=jax.ShapeDtypeStruct((members, depth, LANES) if paired else (2, depth, span), f32),
        in_specs=scalar + whole(6),
        out_specs=whole(1)[0],
        cost_estimate=cost(2 * 2 * 32 * slots * span, 3000000),
        compiler_params=grant,
        name="place_samples",
    )(half, samples, far_samples, onehot, far_onehot, placed, far_placed)
    matrix = pl.pallas_call(
        functools.partial(split_matrix_kernel, rows),
        out_shape=jax.ShapeDtypeStruct((rows + 8, 3 * (rows + 8)), bf16),
        in_specs=whole(1),
        out_specs=whole(1)[0],
        scratch_shapes=[pltpu.VMEM((rows + 8, LANES), f32)],
        cost_estimate=cost(1000000, 60000),
        compiler_params=grant,
        name="split_matrix",
    )(filter_matrix)
    matrix, outgoing = lax.optimization_barrier((matrix, outgoing))
    if not paired:
        outgoing = outgoing.reshape(2, depth, members, per_owner).transpose(2, 1, 0, 3)
    arrived = lax.all_to_all(outgoing, ("ty", "within"), split_axis=0, concat_axis=0, tiled=True)
    runs = 4 * groups // 4
    if not paired:
        behind = arrived[:, 2 * rows :]
        number = jnp.arange(8)[:, None] % 2 == jnp.arange(2)
        behind = jnp.where(number[None, :, :, None, None], behind[:, :, None], 0.0)
        arrived = arrived[:, : 2 * rows].reshape(members, 2, rows, 2, per_owner).transpose(0, 2, 1, 3, 4)
        arrived = jnp.concatenate([arrived, behind], axis=1)
        arrived = arrived.reshape(-1, within, rows + 8, 2, 2, per_owner).transpose(4, 2, 0, 3, 1, 5)
        arrived = arrived.reshape(2, rows + 8, tile_count * per_owner)
    filtered = pl.pallas_call(
        functools.partial(filter_kernel, per_owner, paired, 2 * within),
        out_shape=jax.ShapeDtypeStruct((SAMPLES, runs, 8, LANES), f32),
        in_specs=whole(2),
        out_specs=pl.BlockSpec(memory_space=pltpu.HBM),
        scratch_shapes=[
            pltpu.VMEM((runs, SAMPLES * 8, LANES), f32),
            pltpu.SemaphoreType.DMA((runs,)),
        ],
        cost_estimate=cost(2 * 3 * 80 * 80 * 8 * slots, 3000000),
        compiler_params=grant,
        name="filter_series",
    )(matrix, arrived)
    filtered = filtered.reshape(SAMPLES, 4 * groups, 2, LANES)
    return filtered.transpose(2, 0, 1, 3).reshape(2, SAMPLES, 4 * slots)


def solution(mesh):
    lines, across = mesh.devices.shape
    halved = Mesh(mesh.devices.reshape(lines, 2, across // 2), ("ty", "half", "within"))
    tile = ("ty", "half", "within")
    placed = (
        P(None, None, "ty", ("half", "within")),
        P(None, tile),
        P(None, None, None, tile),
        P(None, None, tile),
        P(),
        P(tile, None),
        P(),
    )
    return jax.shard_map(
        run,
        mesh=halved,
        in_specs=placed,
        out_specs=P(None, None, tile),
        check_vma=False,
    )
```

```python
import functools

import jax
import jax.numpy as jnp
from jax import lax
from jax.experimental import pallas as pl
from jax.experimental.pallas import tpu as pltpu
from jax.sharding import Mesh
from jax.sharding import PartitionSpec as P


STEPS = 2
SAMPLES = 73
HISTORY = 71
MOST = 16


drift = 0.2
moves = ((-1, -1), (-1, 0), (-1, 1), (0, -1), (0, 1), (1, -1), (1, 0), (1, 1))
f32 = jnp.float32
bf16 = jnp.bfloat16
LANES = 128


def up(value, to):
    return -(-value // to) * to


places = {"ty": "ty", "tx": ("half", "within")}


def exchanged(up, down, axis):
    peers = lax.axis_size(places[axis])
    even = lax.axis_index(places[axis]) % 2 == 0
    near = [(i, i ^ 1) for i in range(peers)]
    far = [(i, (i - 1 if i % 2 == 0 else i + 1) % peers) for i in range(peers)]
    first = lax.ppermute(up if up is down else jnp.where(even, up, down), places[axis], near)
    second = lax.ppermute(up if up is down else jnp.where(even, down, up), places[axis], far)
    return jnp.where(even, second, first), jnp.where(even, first, second)


def swapped(value):
    return lax.ppermute(value, "half", [(0, 1), (1, 0)])


def halves(value):
    high = value.astype(bf16)
    return high, (value - high.astype(f32)).astype(bf16)


def picked(condition):
    return jnp.where(condition, 1.0, 0.0).astype(f32)


def iota(shape, dim):
    return lax.broadcasted_iota(jnp.int32, shape, dim)


def whole(count):
    return [pl.BlockSpec(memory_space=pltpu.VMEM) for _ in range(count)]


def cost(flops, moved):
    return pl.CostEstimate(flops=flops, bytes_accessed=moved, transcendentals=0)


grant = pltpu.CompilerParams(vmem_limit_bytes=16 * 1024 * 1024)


def sections_of(step, following):
    own = [(step, 0, 0)] if step == 0 else []
    own += [(step, 1, 1), (step, 2, 1), (step, 3, 2)]
    return own + ([(step + 1, 0, 2)] if following else [])


def at_time(read, step, table):
    if table == 1:
        return 0.5 * (read(step) + read(step + 1))
    return read(step + table // 2)


def side_by_side(value):
    return jnp.concatenate(halves(value), axis=1)


def doubled(value):
    return jnp.concatenate([value, value], axis=0)


def inner_kernel(step, following, velocity_ref, cells_ref, part_ref, cols_ref, rows_ref, table_ref):
    rows, cols = velocity_ref.shape[2], velocity_ref.shape[3]
    slots = cells_ref.shape[3]
    for table in range(3):
        for c in range(2):
            value = at_time(lambda a: velocity_ref[c, a], step, table)
            table_ref[table, c * rows : (c + 1) * rows] = side_by_side(value)
    col = iota((cols, slots), 0)
    row = iota((rows, slots), 0)
    for number, (k, section, table) in enumerate(sections_of(step, following)):
        cy, cx = cells_ref[k, section, 0:1], cells_ref[k, section, 1:2]
        across = [picked(row == cy), picked(row == cy + 1)]
        for v in range(2):
            rows_ref[number, v] = across[v].astype(bf16)
        values = {}
        for h in range(2):
            onehot = picked(col == cx + h).astype(bf16)
            cols_ref[number, h] = onehot
            product = jnp.dot(table_ref[table], doubled(onehot), preferred_element_type=f32)
            for c in range(2):
                for v in range(2):
                    kept = across[v] * product[c * rows : (c + 1) * rows]
                    values[v, h, c] = jnp.sum(kept, axis=0, keepdims=True)
        corners = [values[v, h, c] for v in range(2) for h in range(2) for c in range(2)]
        part_ref[number] = jnp.concatenate(corners, axis=0)


def bilinear(corners, point, cell):
    wy = point[0] - cell[0:1].astype(f32)
    wx = point[1] - cell[1:2].astype(f32)
    first, second, third, fourth = corners
    return [
        (1.0 - wy) * ((1.0 - wx) * first[c] + wx * second[c]) + wy * ((1.0 - wx) * third[c] + wx * fourth[c])
        for c in range(2)
    ]


def along(point, factor, speed):
    return [p + factor * s for p, s in zip(point, speed)]


def step_kernel(
    step, following, velocity_shape, part_ref, cols_ref, rows_ref, north_ref, south_ref, west_ref, east_ref, point_ref, cells_ref, *rest
):
    if step > 0:
        first_ref, rest = rest[0], rest[1:]
    if following:
        record_ref, lead_ref, next_ref = rest
    else:
        record_ref, lead_ref = rest
    count, rows, cols = velocity_shape
    base = 2 * HISTORY
    ends = ((north_ref, south_ref), (west_ref, east_ref))
    tables = []
    for pair in ends:
        lines = []
        for table in range(3):
            for c in range(2):
                for ref in pair:
                    lines.append(at_time(lambda a: ref[base + c * count + a : base + c * count + a + 1], step, table))
        lines.append(jnp.zeros((4, cols), f32))
        tables.append(side_by_side(jnp.concatenate(lines, axis=0)))

    def tip(table, c, v, h):
        ref, at = ends[1][h], base + (1 + v) * 2 * count + c * count
        lane = slice(cols - 1, cols) if h == 0 else slice(0, 1)
        return at_time(lambda a: ref[at + a : at + a + 1, lane], step, table)

    def corners_of(number):
        k, section, table = sections_of(step, following)[number]
        cy, cx = cells_ref[k, section, 0:1], cells_ref[k, section, 1:2]
        outside = ((cy < 0, cy + 1 >= rows), (cx < 0, cx + 1 >= cols))
        ends_of = [
            jnp.dot(tables[0], doubled(cols_ref[number, i]), preferred_element_type=f32) for i in range(2)
        ], [jnp.dot(tables[1], doubled(rows_ref[number, i]), preferred_element_type=f32) for i in range(2)]
        result = []
        for v in range(2):
            for h in range(2):
                pair = []
                for c in range(2):
                    value = part_ref[number, 4 * v + 2 * h + c : 4 * v + 2 * h + c + 1]
                    at = 4 * table + 2 * c
                    value += jnp.where(outside[0][v], ends_of[0][h][at + v : at + v + 1], 0.0)
                    value += jnp.where(outside[1][h], ends_of[1][v][at + h : at + h + 1], 0.0)
                    value += jnp.where(outside[0][v] & outside[1][h], tip(table, c, v, h), 0.0)
                    pair.append(value)
                result.append(pair)
        return result

    corners = [corners_of(number) for number in range(len(sections_of(step, following)))]
    sections = [cells_ref[step, s] for s in range(4)]
    if step > 0:
        given = [[first_ref[2 * i + c : 2 * i + c + 1] for c in range(2)] for i in range(4)]
        corners = [given] + corners
    point = [point_ref[0:1], point_ref[1:2]]
    k_one = bilinear(corners[0], point, sections[0])
    k_two = bilinear(corners[1], along(point, 0.5 * drift, k_one), sections[1])
    k_three = bilinear(corners[2], along(point, 0.5 * drift, k_two), sections[2])
    k_four = bilinear(corners[3], along(point, drift, k_three), sections[3])
    point = [
        p + drift / 6.0 * (a + 2.0 * b + 2.0 * c + d)
        for p, a, b, c, d in zip(point, k_one, k_two, k_three, k_four)
    ]
    blank = [jnp.zeros_like(point[0])] * 4
    record = jnp.concatenate(point + k_one + blank, axis=0)
    record_ref[...] = record
    band = step * 8 * MOST
    lead_ref[...] = record[0:4, band : band + 8 * MOST]
    if following:
        next_ref[...] = jnp.concatenate([value for corner in corners[4] for value in corner], axis=0)


def run_step(step, halo, point, first, cells):
    velocity, *ends = halo
    slots = point.shape[1]
    following = step + 1 < STEPS
    rows, cols = velocity.shape[2:]
    number = len(sections_of(step, following))
    inner = pl.pallas_call(
        functools.partial(inner_kernel, step, following),
        out_shape=[
            jax.ShapeDtypeStruct((number, 8, slots), f32),
            jax.ShapeDtypeStruct((number, 2, cols, slots), bf16),
            jax.ShapeDtypeStruct((number, 2, rows, slots), bf16),
        ],
        in_specs=whole(2),
        out_specs=whole(3),
        scratch_shapes=[pltpu.VMEM((3, 2 * rows, 2 * cols), bf16)],
        cost_estimate=cost(number * 2 * 2 * rows * 2 * cols * slots * 2, 600000),
        compiler_params=grant,
        name="sample_inner",
    )(velocity, cells)
    operands = (*inner, *ends, point, cells) + ((first,) if step > 0 else ())
    shape = jax.ShapeDtypeStruct((8, slots), f32)
    shapes = [shape, jax.ShapeDtypeStruct((4, 8 * MOST), f32)] + ([shape] if following else [])
    return pl.pallas_call(
        functools.partial(step_kernel, step, following, velocity.shape[1:]),
        out_shape=shapes,
        in_specs=whole(len(operands)),
        out_specs=whole(len(shapes)),
        cost_estimate=cost(number * 2 * 4 * 16 * 2 * cols * slots, 600000),
        compiler_params=grant,
        name="sample_step",
    )(*operands)


def sides_kernel(leavers_ref, sides_ref):
    slot = iota((1, 8 * MOST), 1)
    for step in range(leavers_ref.shape[0]):
        rows = [jnp.zeros((1, 8 * MOST), f32) for _ in range(2)]
        start = 0
        for j in range(8):
            end = start + leavers_ref[step, j]
            inside = (slot >= start) & (slot < end)
            rows = [jnp.where(inside, float(moves[j][axis]), rows[axis]) for axis in range(2)]
            start = end
        sides_ref[step] = jnp.concatenate(rows + [jnp.zeros((6, 8 * MOST), f32)], axis=0)


def find_sides(leavers):
    return pl.pallas_call(
        sides_kernel,
        out_shape=jax.ShapeDtypeStruct((leavers.shape[0], 8, 8 * MOST), f32),
        in_specs=[pl.BlockSpec(memory_space=pltpu.SMEM)],
        out_specs=whole(1)[0],
        compiler_params=grant,
        cost_estimate=cost(100000, 5000),
        name="find_sides",
    )(leavers)


def chosen(side, value, forward, backward):
    return jnp.where(side > 0.0, forward, jnp.where(side < 0.0, backward, value))


def paired_halves(first, second, width):
    lane = iota(first.shape, 1)
    left = jnp.where(lane < width, first, pltpu.roll(second, width, 1))
    right = jnp.where(lane < width, pltpu.roll(first, width, 1), second)
    return left, right


def columns_kernel(width, owner_ref, out_ref):
    owner_row = owner_ref[...]
    slots = owner_row.shape[1]
    owner = jnp.broadcast_to(owner_row, (LANES, slots)).T[:, 0:1]
    before = iota((slots, slots), 0) < iota((slots, slots), 1)
    rank = jnp.sum(picked((owner == owner_row) & before), axis=0, keepdims=True)
    out_ref[...] = owner_row * width + rank


def targets_of(columns, half, within, width):
    slots = columns.shape[1]
    half = half.astype(f32)
    owner = jnp.floor((columns + 0.5) / width)
    column = jnp.floor((owner + 0.5) / within)
    line = jnp.floor((column + 0.5) * 0.5)
    block = line * within + (owner - column * within)
    target = jnp.where(column - 2.0 * line == half, block * width + (columns - owner * width), -1.0)
    return jnp.broadcast_to(target, (LANES, slots)).T[:, 0:1].astype(jnp.int32)


def place_history_kernel(width, paired, within, skipped, half_ref, owner_ref, history_ref, past_ref, out_ref, onehot_ref):
    slots = owner_ref.shape[1]
    rows = up(HISTORY, 8)
    groups = slots // LANES
    moving = 8 * MOST // LANES
    total = onehot_ref.shape[1]
    target = targets_of(owner_ref[...], half_ref[0], within, width)
    parts = []
    for c in range(2):
        pieces = [past_ref[pl.ds(c, HISTORY, stride=2), :]]
        for g in range(moving, groups):
            pieces.append(history_ref[pl.ds(2 * (g - skipped) + c, HISTORY, stride=2 * (groups - skipped)), :])
        parts += [jnp.concatenate(pieces, axis=1), jnp.zeros((rows - HISTORY, slots), f32)]
    joined = jnp.concatenate(halves(jnp.concatenate(parts, axis=0)), axis=0)
    chunk = 256
    for start in range(0, total, chunk):
        onehot = picked(target == start + iota((slots, chunk), 1)).astype(bf16)
        onehot_ref[:, start : start + chunk] = onehot
        product = jnp.dot(joined, onehot, preferred_element_type=f32)
        placed = product[: 2 * rows] + product[2 * rows :]
        if paired:
            for at in range(0, chunk, LANES):
                pair = paired_halves(placed[:rows, at : at + LANES], placed[rows:, at : at + LANES], width)
                for i in range(2):
                    out_ref[(start + at) // width + i] = pair[i]
        else:
            out_ref[0, :, start : start + chunk] = placed[:rows]
            out_ref[1, :, start : start + chunk] = placed[rows:]


def place_samples_kernel(
    width, paired, half_ref, samples_ref, far_samples_ref, onehot_ref, far_onehot_ref, placed_ref, far_placed_ref, out_ref
):
    half = half_ref[0]
    rows = up(HISTORY, 8)
    total = onehot_ref.shape[1]
    chunk = 256
    row = iota((8, LANES), 0)
    wide = iota((8, chunk), 0)
    tiles = (
        (half, samples_ref, onehot_ref, placed_ref),
        (1 - half, far_samples_ref, far_onehot_ref, far_placed_ref),
    )
    lefts = []
    for number, samples, _, _ in tiles:
        columns = []
        for c in range(2):
            early, late = samples[2 * c : 2 * c + 1], samples[2 * c + 1 : 2 * c + 2]
            at = iota((8, early.shape[1]), 0)
            columns.append(jnp.where(at == number, early, jnp.where(at == number + 2, late, 0.0)))
        lefts.append(jnp.concatenate(halves(jnp.concatenate(columns, axis=0)), axis=0))
    for start in range(0, total, chunk):
        span = slice(start, start + chunk)
        values = None
        for left, (_, _, onehot, _) in zip(lefts, tiles):
            product = jnp.dot(left, onehot[:, span], preferred_element_type=f32)
            value = product[:16] + product[16:]
            values = value if values is None else values + value
        if paired:
            for at in range(0, chunk, LANES):
                pair = paired_halves(values[:8, at : at + LANES], values[8:, at : at + LANES], width)
                for i in range(2):
                    block = (start + at) // width + i
                    for number, _, _, placed in tiles:
                        out_ref[block, pl.ds(pl.multiple_of(number * rows, 8), rows), :] = placed[block]
                    out_ref[block, 2 * rows : 2 * rows + 8] = pair[i]
        else:
            for c in range(2):
                for number, _, _, placed in tiles:
                    out_ref[c, pl.ds(pl.multiple_of(number * rows, 8), rows), span] = placed[c, :, span]
                out_ref[c, 2 * rows : 2 * rows + 8, span] = values[8 * c : 8 * c + 8]


def split_matrix_kernel(rows, matrix_ref, out_ref, wide_ref):
    samples = matrix_ref.shape[0]
    wide_ref[...] = jnp.zeros_like(wide_ref)
    wide_ref[0:samples, 0:HISTORY] = matrix_ref[:, 0:HISTORY]
    for late in range(STEPS):
        for number in range(2):
            at = rows + 2 * late + number
            wide_ref[0:samples, at : at + 1] = matrix_ref[:, HISTORY + late : HISTORY + late + 1]
    high, low = halves(wide_ref[:, 0 : rows + 8])
    out_ref[...] = jnp.concatenate([high, low, high], axis=1)


def filter_kernel(width, paired, across, matrix_ref, arrived_ref, out_ref, ready_ref, sems):
    rows = matrix_ref.shape[0] - 8
    samples = out_ref.shape[0]
    groups = out_ref.shape[2] // 2
    row = iota((8, LANES), 0)
    left = matrix_ref[...]

    def block_of(tile):
        line, column = tile // across, tile % across
        number, column = column // (across // 2), column % (across // 2)
        block = line * (across // 2) + column
        behind = jnp.where((row == number) | (row == number + 2), arrived_ref[block, 2 * rows : 2 * rows + 8], 0.0)
        return jnp.concatenate([arrived_ref[block, number * rows : (number + 1) * rows], behind], axis=0)

    copies = []
    for run in range(out_ref.shape[1]):
        start = run * groups * LANES
        if paired:
            spots = range(start // width, (start + groups * LANES) // width, 2)
            tiles = [paired_halves(block_of(at), block_of(at + 1), width) for at in spots]
            columns = [jnp.concatenate([t[c] for t in tiles], axis=1) for c in range(2)]
        else:
            columns = [arrived_ref[c, :, start : start + groups * LANES] for c in range(2)]
        for c in range(2):
            x_high, x_low = halves(columns[c])
            right = jnp.concatenate([x_high, x_high, x_low], axis=0)
            product = jnp.dot(left, right, preferred_element_type=f32)
            for g in range(groups):
                target = pl.ds(2 * g + c, samples, stride=2 * groups)
                ready_ref[run, target, :] = product[:samples, g * LANES : (g + 1) * LANES]
        source = ready_ref.at[run].reshape(samples, 2 * groups, LANES)
        copies.append(pltpu.make_async_copy(source, out_ref.at[:, run], sems.at[run]))
        copies[-1].start()
    for copy in copies:
        copy.wait()


def run(velocity, start_position, cells, history, leavers, owner, filter_matrix):
    tile_rows = velocity.shape[2]
    tile_cols = velocity.shape[3]
    slots = start_position.shape[1]
    within = lax.axis_size("within")
    members = lax.axis_size("ty") * within
    tile_count = 2 * members
    per_owner = 4 * slots // tile_count
    paired = 2 * per_owner == LANES
    groups = slots // LANES
    lines = 2 * HISTORY
    by_rows = history.reshape(2, HISTORY, groups, LANES).transpose(1, 2, 0, 3)
    raw = by_rows.reshape(2 * groups * HISTORY, LANES)
    past = by_rows[:, 0].reshape(lines, LANES)
    sides = find_sides(leavers)

    def joined(*parts):
        return jnp.concatenate([part.reshape(-1, LANES) for part in parts], axis=0)

    north, south = exchanged(joined(past, velocity[:, :, tile_rows - 1]), joined(past, velocity[:, :, 0]), "ty")
    past = chosen(sides[0, 0:1], past, north[:lines], south[:lines])
    west, east = exchanged(
        joined(past, velocity[:, :, :, tile_cols - 1], north[lines:], south[lines:]),
        joined(past, velocity[:, :, :, 0], north[lines:], south[lines:]),
        "tx",
    )
    past = chosen(sides[0, 1:2], past, west[:lines], east[:lines])
    halo = (velocity, north, south, west, east)
    owner = pl.pallas_call(
        functools.partial(columns_kernel, per_owner),
        out_shape=jax.ShapeDtypeStruct((1, slots), f32),
        in_specs=whole(1),
        out_specs=whole(1)[0],
        cost_estimate=cost(1000000, 10000),
        compiler_params=grant,
        name="find_columns",
    )(owner.astype(f32).reshape(1, slots))
    past = joined(past, owner, jnp.zeros((2, LANES), f32))
    moving = 8 * MOST // LANES
    far_raw = swapped(by_rows[:, moving:].reshape(2 * (groups - moving) * HISTORY, LANES))
    far_past = swapped(past)
    far_owner = far_past[lines : lines + groups].reshape(1, slots)
    half = lax.axis_index("half").reshape(1)
    record, lead, first = run_step(0, halo, start_position, None, cells)
    lead = chosen(sides[0, 0:1], lead, *exchanged(lead, lead, "ty"))
    lead_west, lead_east = exchanged(lead, lead, "tx")
    rows = up(HISTORY, 8)
    scalar = [pl.BlockSpec(memory_space=pltpu.SMEM)]
    span = members * per_owner
    shape = (members, rows, LANES) if paired else (2, rows, span)

    def place(owner, raw, past, skipped):
        return pl.pallas_call(
            functools.partial(place_history_kernel, per_owner, paired, within, skipped),
            out_shape=[jax.ShapeDtypeStruct(shape, f32), jax.ShapeDtypeStruct((slots, span), bf16)],
            in_specs=scalar + whole(3),
            out_specs=whole(2),
            cost_estimate=cost(2 * 4 * rows * slots * span, 3000000),
            compiler_params=grant,
            name="place_history",
        )(half, owner, raw, past)

    placed, onehot = place(owner.reshape(1, slots), raw, past, 0)
    far_placed, far_onehot = place(far_owner, far_raw, far_past, moving)
    lead = chosen(sides[0, 1:2], lead, lead_west, lead_east)
    lowered = [sides[0, 0:1] * tile_rows, sides[0, 1:2] * tile_cols, jnp.zeros((2, 8 * MOST), f32)]
    record = jnp.concatenate([lead - jnp.concatenate(lowered, axis=0), record[0:4, 8 * MOST :]], axis=1)
    point = record[0:2]
    corners = [[first[2 * i + c : 2 * i + c + 1] for c in range(2)] for i in range(4)]
    last = bilinear(corners, [record[0:1], record[1:2]], cells[STEPS - 1, 0])
    samples = jnp.concatenate([record[2:3], last[0], record[3:4], last[1]], axis=0)
    run_step(STEPS - 1, halo, point, first, cells)
    far_samples = swapped(samples)
    depth = 2 * rows + 8
    outgoing = pl.pallas_call(
        functools.partial(place_samples_kernel, per_owner, paired),
        out_shape=jax.ShapeDtypeStruct((members, depth, LANES) if paired else (2, depth, span), f32),
        in_specs=scalar + whole(6),
        out_specs=whole(1)[0],
        cost_estimate=cost(2 * 2 * 32 * slots * span, 3000000),
        compiler_params=grant,
        name="place_samples",
    )(half, samples, far_samples, onehot, far_onehot, placed, far_placed)
    matrix = pl.pallas_call(
        functools.partial(split_matrix_kernel, rows),
        out_shape=jax.ShapeDtypeStruct((rows + 8, 3 * (rows + 8)), bf16),
        in_specs=whole(1),
        out_specs=whole(1)[0],
        scratch_shapes=[pltpu.VMEM((rows + 8, LANES), f32)],
        cost_estimate=cost(1000000, 60000),
        compiler_params=grant,
        name="split_matrix",
    )(filter_matrix)
    matrix, outgoing = lax.optimization_barrier((matrix, outgoing))
    if not paired:
        outgoing = outgoing.reshape(2, depth, members, per_owner).transpose(2, 1, 0, 3)
    arrived = lax.all_to_all(outgoing, ("ty", "within"), split_axis=0, concat_axis=0, tiled=True)
    runs = 4 * groups // 4
    if not paired:
        behind = arrived[:, 2 * rows :]
        number = jnp.arange(8)[:, None] % 2 == jnp.arange(2)
        behind = jnp.where(number[None, :, :, None, None], behind[:, :, None], 0.0)
        arrived = arrived[:, : 2 * rows].reshape(members, 2, rows, 2, per_owner).transpose(0, 2, 1, 3, 4)
        arrived = jnp.concatenate([arrived, behind], axis=1)
        arrived = arrived.reshape(-1, within, rows + 8, 2, 2, per_owner).transpose(4, 2, 0, 3, 1, 5)
        arrived = arrived.reshape(2, rows + 8, tile_count * per_owner)
    filtered = pl.pallas_call(
        functools.partial(filter_kernel, per_owner, paired, 2 * within),
        out_shape=jax.ShapeDtypeStruct((SAMPLES, runs, 8, LANES), f32),
        in_specs=whole(2),
        out_specs=pl.BlockSpec(memory_space=pltpu.HBM),
        scratch_shapes=[
            pltpu.VMEM((runs, SAMPLES * 8, LANES), f32),
            pltpu.SemaphoreType.DMA((runs,)),
        ],
        cost_estimate=cost(2 * 3 * 80 * 80 * 8 * slots, 3000000),
        compiler_params=grant,
        name="filter_series",
    )(matrix, arrived)
    filtered = filtered.reshape(SAMPLES, 4 * groups, 2, LANES)
    return filtered.transpose(2, 0, 1, 3).reshape(2, SAMPLES, 4 * slots)


def solution(mesh):
    lines, across = mesh.devices.shape
    halved = Mesh(mesh.devices.reshape(lines, 2, across // 2), ("ty", "half", "within"))
    tile = ("ty", "half", "within")
    placed = (
        P(None, None, "ty", ("half", "within")),
        P(None, tile),
        P(None, None, None, tile),
        P(None, None, tile),
        P(),
        P(tile, None),
        P(),
    )
    return jax.shard_map(
        run,
        mesh=halved,
        in_specs=placed,
        out_specs=P(None, None, tile),
        check_vma=False,
    )
```
